8 devices in a mesh: task: 1 (over z), row: 8 (over y, x, core).
Axes of the slice: x: 2, y: 2, z: 1, core: 2. Of those that a mesh axis runs over, the one named last changes fastest.
Arguments:
- points: bfloat16 [24576, 768], P(('task', 'row'))
- vectors: bfloat16 [24576, 32], P(('task', 'row'))
- length_scale: float32 [1], P('task')
- out_scale: float32 [1], P('task')
Outputs:
- output: float32 [24576, 32], P(('task', 'row'))
All inputs are finite; a program needn't handle non-finite values.
Results may differ from the reference program's by a relative error of at most 0.001.
Values are sent between devices in bfloat16 or wider.
A program may use at most 1 GiB of HBM per device.

```python
import jax
import jax.numpy as jnp
from jax import lax

ROWS_DEV = 3072
GROUP = 8
FEAT = 768
COLS = 32
N_POINTS = GROUP * ROWS_DEV


def setup_inputs(seed: int = 0, part: int = 0) -> dict:
    base_key = jax.random.fold_in(jax.random.key(seed), part)
    key_x, key_o, key_m, key_v, key_l, key_s = jax.random.split(base_key, 6)
    base_pts = jax.random.normal(key_x, (GROUP, ROWS_DEV, FEAT), jnp.float32)
    offset = 1.6 * jax.random.normal(key_o, (GROUP, 1, FEAT), jnp.float32)
    points = (base_pts + offset).reshape(N_POINTS, FEAT).astype(jnp.bfloat16)
    block_mean = jax.random.normal(key_m, (GROUP, 1, COLS), jnp.float32)
    block_mean = block_mean - jnp.mean(block_mean, axis=0, keepdims=True)
    noise_val = 0.5 * jax.random.normal(key_v, (GROUP, ROWS_DEV, COLS), jnp.float32)
    vectors = (block_mean + noise_val).reshape(N_POINTS, COLS).astype(jnp.bfloat16)
    ell_ratio = jax.random.uniform(key_l, (1,), jnp.float32, 0.8, 1.25)
    length_scale = jnp.sqrt(2.0 * FEAT * ell_ratio)
    out_scale = jax.random.uniform(key_s, (1,), jnp.float32, 1.0, 2.0) / ROWS_DEV
    return {"points": points, "vectors": vectors, "length_scale": length_scale, "out_scale": out_scale}


def kernel_tile(x_rows, x_cols, length_scale, out_scale):
    norm_rows = jnp.sum(jnp.square(x_rows.astype(jnp.float32)), axis=1)
    norm_cols = jnp.sum(jnp.square(x_cols.astype(jnp.float32)), axis=1)
    gram_mat = jnp.dot(x_rows, x_cols.T, preferred_element_type=jnp.float32)
    sq_dist = jnp.maximum(norm_rows[:, None] + norm_cols[None, :] - 2.0 * gram_mat, 0.0)
    return (out_scale * jnp.exp(-sq_dist / (2.0 * length_scale * length_scale))).astype(jnp.bfloat16)


def kernel_apply(points, vectors, length_scale, out_scale):
    x_blocks = points.reshape(GROUP, ROWS_DEV, FEAT)
    v_blocks = vectors.reshape(GROUP, ROWS_DEV, COLS)

    def row_block(x_rows):
        def col_step(running, col_pair):
            x_cols, v_cols = col_pair
            kern_tile = kernel_tile(x_rows, x_cols, length_scale, out_scale)
            return running + jnp.dot(kern_tile, v_cols, preferred_element_type=jnp.float32), None

        running, _ = lax.scan(col_step, jnp.zeros((ROWS_DEV, COLS), jnp.float32), (x_blocks, v_blocks))
        return running

    return lax.map(row_block, x_blocks).reshape(N_POINTS, COLS)


def reference(points, vectors, length_scale, out_scale):
    first_pass = kernel_apply(points, vectors, length_scale, out_scale).astype(jnp.bfloat16)
    return kernel_apply(points, first_pass, length_scale, out_scale)
```

```python
import functools

import jax
import jax.numpy as jnp
from jax import lax
from jax.experimental import pallas as pl
from jax.experimental.pallas import tpu as pltpu
from jax.sharding import PartitionSpec as P

MESH = pl.DeviceIdType.MESH
F32, BF16 = jnp.float32, jnp.bfloat16
LOG2E = 1.4426950408889634

ROWS = 3072
STRIP = 256
CHUNK = 512
N_STRIP = ROWS // STRIP
N_CHUNK = ROWS // CHUNK
UNITS = 3
OWN, XNB, YNB, PAR, TRASH = 0, 1, 2, 3, 4

PRE = 7
FILL = (0, 4, 4, 2, 2, 0, 0, 4, 4, 2, 2, 0)
TILES = tuple(12 + 2 * (n // 2) + 2 * (n % 2) for n in range(N_STRIP))
STEPS = tuple((TILES[n] + FILL[n]) // 6 for n in range(N_STRIP))
N_STEP = PRE + sum(STEPS) + 2
TAIL0 = PRE + sum(STEPS[:11])
LEFT0 = TAIL0 + STEPS[11]


def table(values, n):
    out = jnp.int32(values[0])
    for i in range(1, len(values)):
        if values[i] != values[i - 1]:
            out = out + (values[i] - values[i - 1]) * (n >= i).astype(jnp.int32)
    return out


def cumulative(values):
    out = [0]
    for v in values:
        out.append(out[-1] + v)
    return tuple(out[:-1])


FILL_BASE = tuple(PRE * 6 + c for c in cumulative(FILL))
STEP_BASE = tuple(PRE + c for c in cumulative(STEPS))


def pick(cond, a, b):
    return tuple(jnp.where(cond, x, y) for x, y in zip(a, b))


def i32(*xs):
    return tuple(jnp.int32(x) for x in xs)


def own_tile(w, core):
    e = w - 24
    a = e // 3
    par = (jnp.int32(OWN), a, jnp.int32(PAR), 2 * (e % 3) + (a // 2 + core) % 2, jnp.int32(PAR))
    v = jnp.where(w < 24, w, w - 36)
    d, rem = v // 12, v % 12
    i = rem // 2
    own = (jnp.int32(OWN), 2 * i + rem % 2, jnp.int32(OWN), (i + d) % N_CHUNK, jnp.where(d == 0, TRASH, OWN))
    return pick(jnp.logical_and(w >= 24, w < 60), par, own)


def strip_tile(n, idx, core):
    m = n // 2
    t = (jnp.int32(XNB), n, jnp.int32(OWN), idx, jnp.int32(OWN))
    t = pick(idx < 6, t, (jnp.int32(YNB), n, jnp.int32(OWN), idx - 6, jnp.int32(OWN)))
    t = pick(idx < 12, t, (jnp.int32(XNB), n, jnp.int32(YNB), idx - 12, jnp.int32(YNB)))
    t = pick(idx < 12 + m, t, (jnp.int32(YNB), n, jnp.int32(XNB), idx - 12 - m, jnp.int32(XNB)))
    t = pick(idx < 12 + 2 * m, t, (jnp.int32(XNB), n - 1 + (idx - 12 - 2 * m), jnp.int32(YNB), m, jnp.int32(YNB)))
    end = 12 + 2 * m + 2 * (n % 2)
    w = table(FILL_BASE, n) + idx - end
    return pick(idx < end, t, own_tile(w, core))


def last_tile(idx):
    c = idx // 2
    n = jnp.int32(N_STRIP - 1)
    odd = idx % 2 == 1
    t = pick(odd, (jnp.int32(XNB), n, jnp.int32(YNB), c, jnp.int32(YNB)), (jnp.int32(YNB), n, jnp.int32(XNB), c, jnp.int32(XNB)))
    t = pick(idx < 10, t, (jnp.int32(XNB), idx, jnp.int32(YNB), jnp.int32(5), jnp.int32(YNB)))
    j = idx - 12
    return pick(idx < 12, t, (jnp.where(j < 6, XNB, YNB), n, jnp.int32(OWN), j % 6, jnp.int32(OWN)))


def step_tile(step, j, core):
    n = jnp.int32(0)
    for i in range(1, N_STRIP):
        n = n + (step >= STEP_BASE[i]).astype(jnp.int32)
    idx = (step - table(STEP_BASE, n)) * 6 + j
    t = pick(n < N_STRIP - 1, strip_tile(n, idx, core), last_tile(idx))
    w = jnp.where(step < PRE, step * 6, 66 + (step - LEFT0) * 6) + j
    return pick(jnp.logical_or(step < PRE, step >= LEFT0), own_tile(w, core), t)


def rows_of(a):
    return pl.ds(pl.multiple_of(a * STRIP, STRIP), STRIP)


def sums_of(c):
    return pl.ds(pl.multiple_of(STRIP + c * CHUNK, STRIP), CHUNK)


def cols_of(b):
    return pl.ds(pl.multiple_of(b * CHUNK, CHUNK), CHUNK)


def body(
    x_hbm, v_hbm, ell_ref, amp_ref, out_ref, k_hbm,
    X, V0, VT, YV, NA, NB, CR, YR, YT, SB, RB, SB2, RB2, kr0, kr1, KB,
    sx_sem, rx_sem, sv_sem, rv_sem, sn_sem, rn_sem, sp_sem, rp_sem, loc_sem, ko_sem, ki_sem,
    s1_sem, r1_sem, sy_sem, ry_sem, s2_sem, r2_sem,
):
    me = lax.axis_index("row")
    core, cx, cy = me % 2, (me // 2) % 2, me // 4

    def dev(px, py, pc):
        return {"row": (py * 2 + px) * 2 + pc}

    tx = dev(1 - cx, cy, (core + 1 + cx) % 2)
    ty = dev(cx, 1 - cy, (core + 1 + cx + cy) % 2)
    sx = dev(1 - cx, cy, (core + cx) % 2)
    sy = dev(cx, 1 - cy, (core + cx + cy) % 2)
    pt = dev(cx, cy, 1 - core)

    def remote(src, dst, ss, rs, to):
        return pltpu.make_async_remote_copy(src_ref=src, dst_ref=dst, send_sem=ss, recv_sem=rs, device_id=to, device_id_type=MESH)

    def x_copy(j, n):
        return remote(x_hbm.at[rows_of(n)], X.at[1 + j, rows_of(n)], sx_sem.at[j, n], rx_sem.at[j, n], (tx, ty)[j])

    p_copy = remote(x_hbm, X.at[PAR], sp_sem, rp_sem, pt)
    v_copies = [remote(VT.at[OWN], VT.at[1 + j], sv_sem.at[j], rv_sem.at[j], d) for j, d in enumerate((tx, ty, pt))]
    n_copies = [remote(NB.at[OWN], NB.at[1 + j], sn_sem.at[j], rn_sem.at[j], d) for j, d in enumerate((tx, ty, pt))]

    x_loc = pltpu.make_async_copy(x_hbm, X.at[OWN], loc_sem.at[0])
    v_loc = pltpu.make_async_copy(v_hbm, V0, loc_sem.at[1])
    v_loc.start()
    x_loc.start()

    barrier = pltpu.get_barrier_semaphore()
    for d in (tx, ty, sx, sy, pt):
        pl.semaphore_signal(barrier, inc=1, device_id=d, device_id_type=MESH)
    pl.semaphore_wait(barrier, 5)

    for j in range(2):
        x_copy(j, 0).start()
    p_copy.start()

    ell = jnp.full((1, CHUNK), ell_ref[0], F32)
    half = LOG2E / (2.0 * ell * ell)
    top = jnp.log2(jnp.full((1, CHUNK), amp_ref[0], F32))
    CR[0:1, :] = 2.0 * half
    CR[1:2, :] = top
    h1, l1 = half[:, 0:128], top[:, 0:128]

    for s in range(3):
        YR[s] = jnp.zeros((STRIP + ROWS, 32), F32)
    for t in range(5):
        YT[t] = jnp.zeros((32, ROWS), F32)
    kr0[...] = jnp.zeros_like(kr0)
    kr1[...] = jnp.zeros_like(kr1)

    eye = (lax.broadcasted_iota(jnp.int32, (32, 32), 0) == lax.broadcasted_iota(jnp.int32, (32, 32), 1)).astype(F32).astype(BF16)
    v_loc.wait()

    def turn(c, _):
        v = V0[pl.ds(pl.multiple_of(c * CHUNK, CHUNK), CHUNK), :]
        VT[OWN, :, cols_of(c)] = lax.dot_general(eye, v, (((1,), (1,)), ((), ())), preferred_element_type=F32).astype(BF16)
        return 0

    lax.fori_loop(0, N_CHUNK, turn, 0)
    x_loc.wait()

    def own_norm(c, _):
        r = pl.ds(pl.multiple_of(c * CHUNK, CHUNK), CHUNK)
        x = X[OWN, r, :].astype(F32)
        n = jnp.broadcast_to(jnp.sum(x * x, axis=1, keepdims=True), (CHUNK, 128)) * h1
        NA[OWN, r, :] = l1 - n
        NB[OWN, :, cols_of(c)] = -jnp.transpose(n)[0:1, :]
        return 0

    lax.fori_loop(0, N_CHUNK, own_norm, 0)
    for c in v_copies + n_copies:
        c.start()

    def send_strip(n, _):
        for j in range(2):
            x_copy(j, n).start()
        return 0

    lax.fori_loop(1, N_STRIP, send_strip, 0)

    def left_norm(s):
        def one(c, _):
            r = pl.ds(pl.multiple_of(c * CHUNK, CHUNK), CHUNK)
            NA[s, r, :] = l1 + jnp.transpose(jnp.broadcast_to(NB[s, :, cols_of(c)], (128, CHUNK)))
            return 0

        lax.fori_loop(0, N_CHUNK, one, 0)

    def gram(tile):
        s, a, t, b, _ = tile
        return lax.dot_general(X[s, rows_of(a), :], X[t, cols_of(b), :], (((1,), (1,)), ((), ())), preferred_element_type=F32)

    def kern(tile, g):
        s, a, t, b, _ = tile
        na = NA[s, rows_of(a), :]
        e = (g * CR[0:1, :] + NB[t, :, cols_of(b)]) + jnp.concatenate([na] * (CHUNK // 128), axis=1)
        return jnp.exp2(jnp.minimum(e, CR[1:2, :])).astype(BF16)

    def apply(tile, k, vec):
        s, a, t, b, to = tile
        YR[s, rows_of(a + 1), :] += lax.dot_general(k, vec[t, :, cols_of(b)], (((1,), (1,)), ((), ())), preferred_element_type=F32)
        YT[to, :, cols_of(b)] += jnp.dot(vec[s, :, rows_of(jnp.maximum(a, 0))], k, preferred_element_type=F32)

    def k_out(step, half):
        kr = (kr0, kr1)[half]
        return pltpu.make_async_copy(kr.at[step % 2], k_hbm.at[step, half], ko_sem.at[step % 2, half])

    def half_step(prev, cur, kr_new, d_new, kr_old, d_old):
        gs = [gram(t) for t in cur]
        for u in range(UNITS):
            apply(prev[u], kr_old[d_old, u], VT)
        for u in range(UNITS):
            kr_new[d_new, u] = kern(cur[u], gs[u])

    def flat(tiles):
        return tuple(x for t in tiles for x in t)

    def unflat(xs):
        return [tuple(xs[5 * u : 5 * u + 5]) for u in range(UNITS)]

    def step_of(step, prev):
        d = step % 2

        @pl.when(step >= 2)
        def _():
            for h in range(2):
                k_out(step - 2, h).wait()

        @pl.when(step >= 1)
        def _():
            for h in range(2):
                k_out(step - 1, h).start()

        first = [step_tile(step, u, core) for u in range(UNITS)]
        second = [step_tile(step, UNITS + u, core) for u in range(UNITS)]
        half_step(unflat(prev), first, kr0, d, kr1, 1 - d)
        half_step(first, second, kr1, d, kr0, d)
        return flat(second)

    none = flat([i32(OWN, -1, OWN, 0, TRASH)] * UNITS)

    def steps(lo, hi, prev):
        return lax.fori_loop(lo, hi, step_of, prev)

    def pre_step(step, prev):
        @pl.when(step == 4)
        def _():
            p_copy.wait_recv()
            v_copies[2].wait_recv()
            n_copies[2].wait_recv()

        return step_of(step, prev)

    prev = lax.fori_loop(0, PRE, pre_step, none)

    for j in range(2):
        v_copies[j].wait_recv()
        n_copies[j].wait_recv()
        left_norm(1 + j)

    def strip(n, prev):
        for j in range(2):
            x_copy(j, n).wait_recv()
        lo = table(STEP_BASE, n)
        return steps(lo, lo + table(STEPS, n), prev)

    prev = lax.fori_loop(0, N_STRIP - 1, strip, prev)

    for j in range(2):
        x_copy(j, N_STRIP - 1).wait_recv()

    def flush(step, prev):
        for u, t in enumerate(unflat(prev)):
            apply(t, kr1[step % 2, u], VT)

    homes = ((XNB, sx), (YNB, sy), (PAR, pt))

    def part_copy(j, c, send, recv, ss, rs):
        return remote(send.at[j, :, cols_of(c)], recv.at[j, :, cols_of(c)], ss.at[j, c], rs.at[j, c], homes[j][1])

    def finish(j, c, send):
        s = homes[j][0]
        part = YT[s, :, cols_of(c)]
        if j < 2:
            part = part + jnp.transpose(YR[s, sums_of(c), :])
            YR[s, sums_of(c), :] = jnp.zeros((CHUNK, 32), F32)
        send[j, :, cols_of(c)] = part
        YT[s, :, cols_of(c)] = jnp.zeros((32, CHUNK), F32)

    def finish_range(lo, hi, send, recv, ss, rs, js=(0, 1)):
        def one(c, _):
            for j in js:
                finish(j, c, send)
            return 0

        def go(c, _):
            for j in js:
                part_copy(j, c, send, recv, ss, rs).start()
            return 0

        lax.fori_loop(lo, hi, one, 0)
        lax.fori_loop(lo, hi, go, 0)

    def last_step(step, prev):
        prev = step_of(step, prev)
        flush(step, prev)
        i = step - TAIL0
        lo = table((0, 3, 5, 5), i)
        hi = table((3, 5, 5, 6), i)
        finish_range(lo, hi, SB, RB, s1_sem, r1_sem)
        return none

    prev = lax.fori_loop(TAIL0, LEFT0, last_step, prev)
    prev = steps(LEFT0, N_STEP, prev)
    flush(N_STEP - 1, prev)
    finish_range(0, N_CHUNK, SB, RB, s1_sem, r1_sem, (2,))
    for h in range(2):
        k_out(N_STEP - 2, h).wait()
        k_out(N_STEP - 1, h).start()
    for h in range(2):
        k_out(N_STEP - 1, h).wait()

    def order(i):
        return jnp.where(i < PRE, i, jnp.where(i < PRE + 2, LEFT0 + i - PRE, N_STEP - 1 + PRE - i))

    DEPTH = KB.shape[0]

    def k_in(i):
        return pltpu.make_async_copy(k_hbm.at[order(i)], KB.at[i % DEPTH], ki_sem.at[i % DEPTH])

    for i in range(DEPTH - 1):
        k_in(jnp.int32(i)).start()

    def y_copy(j, c):
        return remote(YV.at[OWN, :, cols_of(c)], YV.at[1 + j, :, cols_of(c)], sy_sem.at[j, c], ry_sem.at[j, c], (tx, ty, pt)[j])

    def middle(c, _):
        for j in range(3):
            part_copy(j, c, SB, RB, s1_sem, r1_sem).wait_recv()
        y = YT[OWN, :, cols_of(c)] + jnp.transpose(YR[OWN, sums_of(c), :])
        y = y + RB[0, :, cols_of(c)] + RB[1, :, cols_of(c)] + RB[2, :, cols_of(c)]
        YV[OWN, :, cols_of(c)] = y.astype(BF16)
        YT[OWN, :, cols_of(c)] = jnp.zeros((32, CHUNK), F32)
        YR[OWN, sums_of(c), :] = jnp.zeros((CHUNK, 32), F32)
        return 0

    def middle_go(c, _):
        for j in range(3):
            y_copy(j, c).start()
        return 0

    lax.fori_loop(0, N_CHUNK, middle, 0)
    lax.fori_loop(0, N_CHUNK, middle_go, 0)

    def second(i, _):
        step = order(i)
        k_in(i).wait()

        @pl.when(i + DEPTH - 1 < N_STEP)
        def _():
            k_in(i + DEPTH - 1).start()

        for j in range(6):
            apply(step_tile(step, j, core), KB[i % DEPTH, j // 3, j % 3], YV)
        return 0

    def wait_y(j):
        def one(c, _):
            y_copy(j, c).wait_recv()
            return 0

        lax.fori_loop(0, N_CHUNK, one, 0)

    lax.fori_loop(0, 4, second, 0)
    wait_y(2)
    lax.fori_loop(4, PRE + 2, second, 0)
    wait_y(0)
    wait_y(1)

    bounds = tuple(N_STEP + PRE - STEP_BASE[2 * c] for c in range(N_CHUNK))

    def second_chunk(k, lo):
        c = N_CHUNK - 1 - k
        hi = table(bounds, c)
        lax.fori_loop(lo, hi, second, 0)
        finish_range(c, c + 1, SB2, RB2, s2_sem, r2_sem, (0, 1))
        return hi

    lo = lax.fori_loop(0, N_CHUNK, second_chunk, jnp.int32(PRE + 2))
    finish_range(0, N_CHUNK, SB2, RB2, s2_sem, r2_sem, (2,))

    def final(k, _):
        c = N_CHUNK - 1 - k
        for j in range(3):
            part_copy(j, c, SB2, RB2, s2_sem, r2_sem).wait_recv()
        r = pl.ds(pl.multiple_of(c * CHUNK, CHUNK), CHUNK)
        w = YT[OWN, :, cols_of(c)] + RB2[0, :, cols_of(c)] + RB2[1, :, cols_of(c)] + RB2[2, :, cols_of(c)]
        out_ref[r, :] = YR[OWN, sums_of(c), :] + jnp.transpose(w)
        return 0

    lax.fori_loop(0, N_CHUNK, final, 0)

    p_copy.wait_send()
    for c in v_copies + n_copies:
        c.wait_send()

    def sent_x(n, _):
        for j in range(2):
            x_copy(j, n).wait_send()
        return 0

    lax.fori_loop(0, N_STRIP, sent_x, 0)

    def sent(c, _):
        for j in range(3):
            part_copy(j, c, SB, RB, s1_sem, r1_sem).wait_send()
            y_copy(j, c).wait_send()
            part_copy(j, c, SB2, RB2, s2_sem, r2_sem).wait_send()
        return 0

    lax.fori_loop(0, N_CHUNK, sent, 0)


def solution(mesh):
    def local_program(x_loc, v_loc, length_scale, out_scale):
        dma = pltpu.SemaphoreType.DMA
        hbm = pl.BlockSpec(memory_space=pltpu.HBM)
        smem = pl.BlockSpec(memory_space=pltpu.SMEM)
        w, _ = pl.pallas_call(
            body,
            out_shape=(
                jax.ShapeDtypeStruct((ROWS, 32), F32),
                jax.ShapeDtypeStruct((N_STEP, 2, UNITS, STRIP, CHUNK), BF16),
            ),
            in_specs=[hbm, hbm, smem, smem],
            out_specs=(pl.BlockSpec(memory_space=pltpu.VMEM), hbm),
            scratch_shapes=[
                pltpu.VMEM((4, ROWS, 768), BF16),
                pltpu.VMEM((ROWS, 32), BF16),
                pltpu.VMEM((4, 32, ROWS), BF16),
                pltpu.VMEM((4, 32, ROWS), BF16),
                pltpu.VMEM((3, ROWS, 128), F32),
                pltpu.VMEM((4, 1, ROWS), F32),
                pltpu.VMEM((8, CHUNK), F32),
                pltpu.VMEM((3, STRIP + ROWS, 32), F32),
                pltpu.VMEM((5, 32, ROWS), F32),
                pltpu.VMEM((3, 32, ROWS), F32),
                pltpu.VMEM((3, 32, ROWS), F32),
                pltpu.VMEM((3, 32, ROWS), F32),
                pltpu.VMEM((3, 32, ROWS), F32),
                pltpu.VMEM((2, UNITS, STRIP, CHUNK), BF16),
                pltpu.VMEM((2, UNITS, STRIP, CHUNK), BF16),
                pltpu.VMEM((4, 2, UNITS, STRIP, CHUNK), BF16),
                dma((2, N_STRIP)), dma((2, N_STRIP)),
                dma((3,)), dma((3,)), dma((3,)), dma((3,)), dma, dma, dma((2,)),
                dma((2, 2)), dma((4,)),
                dma((3, N_CHUNK)), dma((3, N_CHUNK)), dma((3, N_CHUNK)), dma((3, N_CHUNK)), dma((3, N_CHUNK)), dma((3, N_CHUNK)),
            ],
            compiler_params=pltpu.CompilerParams(collective_id=0, has_side_effects=True, vmem_limit_bytes=62 * 2**20),
            name="products",
        )(x_loc, v_loc, length_scale, out_scale)
        return w

    row_spec = P(("task", "row"), None)
    return jax.shard_map(local_program, mesh=mesh, in_specs=(row_spec, row_spec, P("task"), P("task")), out_specs=row_spec, check_vma=False)
```

```python
import functools

import jax
import jax.numpy as jnp
from jax import lax
from jax.experimental import pallas as pl
from jax.experimental.pallas import tpu as pltpu
from jax.sharding import PartitionSpec as P

MESH = pl.DeviceIdType.MESH
F32, BF16 = jnp.float32, jnp.bfloat16
LOG2E = 1.4426950408889634

ROWS = 3072
STRIP = 256
CHUNK = 512
N_STRIP = ROWS // STRIP
N_CHUNK = ROWS // CHUNK
UNITS = 3
OWN, XNB, YNB, PAR, TRASH = 0, 1, 2, 3, 4

PRE = 7
FILL = (0, 4, 4, 2, 2, 0, 0, 4, 4, 2, 2, 0)
TILES = tuple(12 + 2 * (n // 2) + 2 * (n % 2) for n in range(N_STRIP))
STEPS = tuple((TILES[n] + FILL[n]) // 6 for n in range(N_STRIP))
N_STEP = PRE + sum(STEPS) + 2
TAIL0 = PRE + sum(STEPS[:11])
LEFT0 = TAIL0 + STEPS[11]


def table(values, n):
    out = jnp.int32(values[0])
    for i in range(1, len(values)):
        if values[i] != values[i - 1]:
            out = out + (values[i] - values[i - 1]) * (n >= i).astype(jnp.int32)
    return out


def cumulative(values):
    out = [0]
    for v in values:
        out.append(out[-1] + v)
    return tuple(out[:-1])


FILL_BASE = tuple(PRE * 6 + c for c in cumulative(FILL))
STEP_BASE = tuple(PRE + c for c in cumulative(STEPS))


def pick(cond, a, b):
    return tuple(jnp.where(cond, x, y) for x, y in zip(a, b))


def i32(*xs):
    return tuple(jnp.int32(x) for x in xs)


def wrap(x):
    return jnp.where(x >= N_CHUNK, x - N_CHUNK, x)


def own_pair(i, d, half):
    return (jnp.int32(OWN), 2 * i + half, jnp.int32(OWN), wrap(i + d), jnp.where(d == 0, TRASH, OWN))


def par_pair(a, k, core):
    return (jnp.int32(OWN), a, jnp.int32(PAR), 2 * k + (((a >> 1) + core) & 1), jnp.int32(PAR))


def pre_tile(step, j, core):
    near = own_pair(3 * (step & 1) + j // 2, step >> 1, j % 2)
    return pick(step < 4, near, par_pair(2 * (step - 4) + j // 3, j % 3, core))


def fill_tile(w, j, core):
    e = w - 24
    a = (e * 171) >> 9
    return pick(w < 60, par_pair(a, e - 3 * a, core), own_pair((w - 60) >> 1, jnp.int32(2), j % 2))


def left_tile(step, j, core):
    u = step - LEFT0
    return own_pair(3 * (1 - u) + j // 2, 2 + u, j % 2)


def strip_tile(n, i, j, core):
    m, odd = n >> 1, n & 1
    r = 6 * (i - 2) + j
    t = (jnp.int32(1) + i, n, jnp.int32(OWN), jnp.int32(j), jnp.int32(OWN))
    t = pick(i < 2, t, (jnp.int32(XNB), n, jnp.int32(YNB), r, jnp.int32(YNB)))
    t = pick(r < m, t, (jnp.int32(YNB), n, jnp.int32(XNB), r - m, jnp.int32(XNB)))
    t = pick(r < 2 * m, t, (jnp.int32(XNB), n - 1 + (r - 2 * m), jnp.int32(YNB), m, jnp.int32(YNB)))
    end = 2 * (m + odd)
    return pick(r < end, t, fill_tile(table(FILL_BASE, n) + r - end, j, core))


def last_tile(i, j):
    n = jnp.int32(N_STRIP - 1)
    s, t = (XNB, YNB) if j % 2 else (YNB, XNB)
    cross = (jnp.int32(s), n, jnp.int32(t), 3 * i + j // 2, jnp.int32(t))
    if j >= 4:
        cross = pick(i < 1, cross, (jnp.int32(XNB), jnp.int32(N_STRIP - 2 + j % 2), jnp.int32(YNB), jnp.int32(5), jnp.int32(YNB)))
    return pick(i < 2, cross, (i - 1, n, jnp.int32(OWN), jnp.int32(j), jnp.int32(OWN)))


def strip_of(step):
    n = jnp.int32(0)
    for i in range(1, N_STRIP):
        n = n + (step >= STEP_BASE[i]).astype(jnp.int32)
    return n


def rows_of(a):
    return pl.ds(pl.multiple_of(a * STRIP, STRIP), STRIP)


def sums_of(c):
    return pl.ds(pl.multiple_of(STRIP + c * CHUNK, STRIP), CHUNK)


def cols_of(b):
    return pl.ds(pl.multiple_of(b * CHUNK, CHUNK), CHUNK)


def body(
    x_hbm, v_hbm, ell_ref, amp_ref, out_ref, k_hbm,
    X, VT, YV, NA, NB, CR, YR, YT, SB, RB, SB2, RB2, kr0, kr1, KB,
    sx_sem, rx_sem, sv_sem, rv_sem, sn_sem, rn_sem, sp_sem, rp_sem, loc_sem, ko_sem, ki_sem,
    s1_sem, r1_sem, sy_sem, ry_sem, s2_sem, r2_sem,
):
    me = lax.axis_index("row")
    core, cx, cy = me % 2, (me // 2) % 2, me // 4

    def dev(px, py, pc):
        return {"row": (py * 2 + px) * 2 + pc}

    tx = dev(1 - cx, cy, (core + 1 + cx) % 2)
    ty = dev(cx, 1 - cy, (core + 1 + cx + cy) % 2)
    sx = dev(1 - cx, cy, (core + cx) % 2)
    sy = dev(cx, 1 - cy, (core + cx + cy) % 2)
    pt = dev(cx, cy, 1 - core)

    def remote(src, dst, ss, rs, to):
        return pltpu.make_async_remote_copy(src_ref=src, dst_ref=dst, send_sem=ss, recv_sem=rs, device_id=to, device_id_type=MESH)

    def x_copy(j, n):
        return remote(x_hbm.at[rows_of(n)], X.at[1 + j, rows_of(n)], sx_sem.at[j, n], rx_sem.at[j, n], (tx, ty)[j])

    p_copy = remote(x_hbm, X.at[PAR], sp_sem, rp_sem, pt)
    v_copies = [remote(v_hbm, VT.at[1 + j], sv_sem.at[j], rv_sem.at[j], d) for j, d in enumerate((tx, ty, pt))]
    n_copies = [remote(NB.at[OWN], NB.at[1 + j], sn_sem.at[j], rn_sem.at[j], d) for j, d in enumerate((tx, ty, pt))]

    x_loc = pltpu.make_async_copy(x_hbm, X.at[OWN], loc_sem.at[0])
    v_loc = pltpu.make_async_copy(v_hbm, VT.at[OWN], loc_sem.at[1])
    v_loc.start()
    x_loc.start()

    barrier = pltpu.get_barrier_semaphore()
    for d in (tx, ty, sx, sy, pt):
        pl.semaphore_signal(barrier, inc=1, device_id=d, device_id_type=MESH)
    with jax.named_scope("barrier"):
        pl.semaphore_wait(barrier, 5)

    for c in v_copies:
        c.start()
    for j in range(2):
        x_copy(j, 0).start()
    p_copy.start()

    ell = jnp.full((1, CHUNK), ell_ref[0], F32)
    half = LOG2E / (2.0 * ell * ell)
    top = jnp.log2(jnp.full((1, CHUNK), amp_ref[0], F32))
    CR[0:1, :] = 2.0 * half
    CR[1:2, :] = top
    h1, l1 = half[:, 0:128], top[:, 0:128]

    for s in range(3):
        YR[s] = jnp.zeros((STRIP + ROWS, 32), F32)
    for t in range(5):
        YT[t] = jnp.zeros((32, ROWS), F32)
    kr0[...] = jnp.zeros_like(kr0)
    kr1[...] = jnp.zeros_like(kr1)

    v_loc.wait()
    with jax.named_scope("x_local"):
        x_loc.wait()

    def own_norm(c, _):
        r = pl.ds(pl.multiple_of(c * CHUNK, CHUNK), CHUNK)
        x = X[OWN, r, :].astype(F32)
        n = jnp.broadcast_to(jnp.sum(x * x, axis=1, keepdims=True), (CHUNK, 128)) * h1
        NA[OWN, r, :] = l1 - n
        NB[OWN, :, cols_of(c)] = -jnp.transpose(n)[0:1, :]
        return 0

    with jax.named_scope("own_norm"):
        lax.fori_loop(0, N_CHUNK, own_norm, 0)
    for c in n_copies:
        c.start()

    def send_strip(n, _):
        for j in range(2):
            x_copy(j, n).start()
        return 0

    lax.fori_loop(1, N_STRIP, send_strip, 0)

    def left_norm(s):
        def one(c, _):
            r = pl.ds(pl.multiple_of(c * CHUNK, CHUNK), CHUNK)
            NA[s, r, :] = l1 + jnp.transpose(jnp.broadcast_to(NB[s, :, cols_of(c)], (128, CHUNK)))
            return 0

        lax.fori_loop(0, N_CHUNK, one, 0)

    def gram(tile):
        s, a, t, b, _ = tile
        return lax.dot_general(X[s, rows_of(a), :], X[t, cols_of(b), :], (((1,), (1,)), ((), ())), preferred_element_type=F32)

    def kern(tile, g):
        s, a, t, b, _ = tile
        na = NA[s, rows_of(a), :]
        e = (g * CR[0:1, :] + NB[t, :, cols_of(b)]) + jnp.concatenate([na] * (CHUNK // 128), axis=1)
        return jnp.exp2(jnp.minimum(e, CR[1:2, :])).astype(BF16)

    def apply(tile, k, vec):
        s, a, t, b, to = tile
        YR[s, rows_of(a + 1), :] += lax.dot_general(k, vec[t, :, cols_of(b)], (((1,), (1,)), ((), ())), preferred_element_type=F32)
        YT[to, :, cols_of(b)] += jnp.dot(vec[s, :, rows_of(jnp.maximum(a, 0))], k, preferred_element_type=F32)

    def k_out(step, half):
        kr = (kr0, kr1)[half]
        return pltpu.make_async_copy(kr.at[step & 1], k_hbm.at[step, half], ko_sem.at[step & 1, half])

    def half_step(prev, cur, kr_new, d_new, kr_old, d_old):
        gs = [gram(t) for t in cur]
        for u in range(UNITS):
            apply(prev[u], kr_old[d_old, u], VT)
        for u in range(UNITS):
            kr_new[d_new, u] = kern(cur[u], gs[u])

    def flat(tiles):
        return tuple(x for t in tiles for x in t)

    def unflat(xs):
        return [tuple(xs[5 * u : 5 * u + 5]) for u in range(UNITS)]

    def step_of(step, prev, tile):
        d = step & 1

        @pl.when(step >= 2)
        def _():
            for h in range(2):
                k_out(step - 2, h).wait()

        @pl.when(step >= 1)
        def _():
            for h in range(2):
                k_out(step - 1, h).start()

        first = [tile(u) for u in range(UNITS)]
        second = [tile(UNITS + u) for u in range(UNITS)]
        half_step(unflat(prev), first, kr0, d, kr1, 1 - d)
        half_step(first, second, kr1, d, kr0, d)
        return flat(second)

    none = flat([i32(OWN, -1, OWN, 0, TRASH)] * UNITS)

    def pre_step(step, prev):
        @pl.when(step == 4)
        def _():
            p_copy.wait_recv()
            v_copies[2].wait_recv()
            n_copies[2].wait_recv()

        return step_of(step, prev, lambda j: pre_tile(step, j, core))

    with jax.named_scope("pre"):
        prev = lax.fori_loop(0, PRE, pre_step, none)

    with jax.named_scope("left_norm"):
        for j in range(2):
            v_copies[j].wait_recv()
            n_copies[j].wait_recv()
            left_norm(1 + j)

    def strip(n, prev):
        with jax.named_scope("wait_strip"):
            for j in range(2):
                x_copy(j, n).wait_recv()
            lo = table(STEP_BASE, n)
        with jax.named_scope("strip"):
            return lax.fori_loop(0, table(STEPS, n), lambda i, p: step_of(lo + i, p, lambda j: strip_tile(n, i, j, core)), prev)

    prev = lax.fori_loop(0, N_STRIP - 1, strip, prev)

    with jax.named_scope("wait_last"):
        for j in range(2):
            x_copy(j, N_STRIP - 1).wait_recv()

    def flush(step, prev):
        for u, t in enumerate(unflat(prev)):
            apply(t, kr1[step & 1, u], VT)

    homes = ((XNB, sx), (YNB, sy), (PAR, pt))

    def part_copy(j, c, send, recv, ss, rs):
        return remote(send.at[j, :, cols_of(c)], recv.at[j, :, cols_of(c)], ss.at[j, c], rs.at[j, c], homes[j][1])

    def finish(j, c, send):
        s = homes[j][0]
        part = YT[s, :, cols_of(c)]
        if j < 2:
            part = part + jnp.transpose(YR[s, sums_of(c), :])
            YR[s, sums_of(c), :] = jnp.zeros((CHUNK, 32), F32)
        send[j, :, cols_of(c)] = part
        YT[s, :, cols_of(c)] = jnp.zeros((32, CHUNK), F32)

    def finish_range(lo, hi, send, recv, ss, rs, js=(0, 1)):
        def one(c, _):
            for j in js:
                finish(j, c, send)
            return 0

        def go(c, _):
            for j in js:
                part_copy(j, c, send, recv, ss, rs).start()
            return 0

        lax.fori_loop(lo, hi, one, 0)
        lax.fori_loop(lo, hi, go, 0)

    def last_step(step, prev):
        i = step - TAIL0
        prev = step_of(step, prev, lambda j: last_tile(i, j))
        flush(step, prev)
        lo = table((0, 3, 5, 5), i)
        hi = table((3, 5, 5, 6), i)
        finish_range(lo, hi, SB, RB, s1_sem, r1_sem)
        return none

    with jax.named_scope("last"):
        prev = lax.fori_loop(TAIL0, LEFT0, last_step, prev)
    with jax.named_scope("left"):
        prev = lax.fori_loop(LEFT0, N_STEP, lambda step, p: step_of(step, p, lambda j: left_tile(step, j, core)), prev)
        flush(N_STEP - 1, prev)
    finish_range(0, N_CHUNK, SB, RB, s1_sem, r1_sem, (2,))
    for h in range(2):
        k_out(N_STEP - 2, h).wait()
        k_out(N_STEP - 1, h).start()
    for h in range(2):
        k_out(N_STEP - 1, h).wait()

    def order(i):
        return jnp.where(i < PRE, i, jnp.where(i < PRE + 2, LEFT0 + i - PRE, N_STEP - 1 + PRE - i))

    DEPTH = KB.shape[0]

    def k_in(i):
        return pltpu.make_async_copy(k_hbm.at[order(i)], KB.at[i & (DEPTH - 1)], ki_sem.at[i & (DEPTH - 1)])

    for i in range(DEPTH - 1):
        k_in(jnp.int32(i)).start()

    def y_copy(j, c):
        return remote(YV.at[OWN, :, cols_of(c)], YV.at[1 + j, :, cols_of(c)], sy_sem.at[j, c], ry_sem.at[j, c], (tx, ty, pt)[j])

    def middle(c, _):
        with jax.named_scope("wait_part"):
            for j in range(3):
                part_copy(j, c, SB, RB, s1_sem, r1_sem).wait_recv()
        y = YT[OWN, :, cols_of(c)] + jnp.transpose(YR[OWN, sums_of(c), :])
        y = y + RB[0, :, cols_of(c)] + RB[1, :, cols_of(c)] + RB[2, :, cols_of(c)]
        YV[OWN, :, cols_of(c)] = y.astype(BF16)
        YT[OWN, :, cols_of(c)] = jnp.zeros((32, CHUNK), F32)
        YR[OWN, sums_of(c), :] = jnp.zeros((CHUNK, 32), F32)
        return 0

    def middle_go(c, _):
        for j in range(3):
            y_copy(j, c).start()
        return 0

    with jax.named_scope("middle"):
        lax.fori_loop(0, N_CHUNK, middle, 0)
    lax.fori_loop(0, N_CHUNK, middle_go, 0)

    def second(i, tile):
        k_in(i).wait()

        @pl.when(i + DEPTH - 1 < N_STEP)
        def _():
            k_in(i + DEPTH - 1).start()

        for j in range(6):
            apply(tile(j), KB[i & (DEPTH - 1), j // 3, j % 3], YV)
        return 0

    def second_own(i, _):
        return second(i, lambda j: pick(i < PRE, pre_tile(i, j, core), left_tile(order(i), j, core)))

    def second_last(i, _):
        return second(i, lambda j: last_tile(order(i) - TAIL0, j))

    def second_strip(i, _):
        step = order(i)
        n = strip_of(step)
        k = step - table(STEP_BASE, n)
        return second(i, lambda j: strip_tile(n, k, j, core))

    def wait_y(j):
        def one(c, _):
            y_copy(j, c).wait_recv()
            return 0

        lax.fori_loop(0, N_CHUNK, one, 0)

    with jax.named_scope("second_own"):
        lax.fori_loop(0, 4, second_own, 0)
        wait_y(2)
        lax.fori_loop(4, PRE + 2, second_own, 0)
    with jax.named_scope("wait_y"):
        wait_y(0)
        wait_y(1)

    bounds = tuple(N_STEP + PRE - STEP_BASE[2 * c] for c in range(N_CHUNK))

    def second_chunk(k, lo):
        c = N_CHUNK - 1 - k
        hi = table(bounds, c)
        with jax.named_scope("second_chunk"):
            lax.fori_loop(lo, hi, second_strip, 0)
        finish_range(c, c + 1, SB2, RB2, s2_sem, r2_sem, (0, 1))
        return hi

    with jax.named_scope("second_last"):
        lax.fori_loop(PRE + 2, PRE + 2 + STEPS[11], second_last, 0)
    lo = lax.fori_loop(0, N_CHUNK, second_chunk, jnp.int32(PRE + 2 + STEPS[11]))
    finish_range(0, N_CHUNK, SB2, RB2, s2_sem, r2_sem, (2,))

    def final(k, _):
        c = N_CHUNK - 1 - k
        for j in range(3):
            part_copy(j, c, SB2, RB2, s2_sem, r2_sem).wait_recv()
        w = YT[OWN, :, cols_of(c)] + jnp.transpose(YR[OWN, sums_of(c), :]) + RB2[0, :, cols_of(c)] + RB2[1, :, cols_of(c)] + RB2[2, :, cols_of(c)]
        out_ref[:, cols_of(c)] = w
        return 0

    with jax.named_scope("final"):
        lax.fori_loop(0, N_CHUNK, final, 0)

    with jax.named_scope("drain"):
        p_copy.wait_send()
    for c in v_copies + n_copies:
        c.wait_send()

    def sent_x(n, _):
        for j in range(2):
            x_copy(j, n).wait_send()
        return 0

    lax.fori_loop(0, N_STRIP, sent_x, 0)

    def sent(c, _):
        for j in range(3):
            part_copy(j, c, SB, RB, s1_sem, r1_sem).wait_send()
            y_copy(j, c).wait_send()
            part_copy(j, c, SB2, RB2, s2_sem, r2_sem).wait_send()
        return 0

    lax.fori_loop(0, N_CHUNK, sent, 0)


def solution(mesh):
    def local_program(x_loc, v_loc, length_scale, out_scale):
        dma = pltpu.SemaphoreType.DMA
        hbm = pl.BlockSpec(memory_space=pltpu.HBM)
        smem = pl.BlockSpec(memory_space=pltpu.SMEM)
        w, _ = pl.pallas_call(
            body,
            out_shape=(
                jax.ShapeDtypeStruct((32, ROWS), F32),
                jax.ShapeDtypeStruct((N_STEP, 2, UNITS, STRIP, CHUNK), BF16),
            ),
            in_specs=[hbm, hbm, smem, smem],
            out_specs=(pl.BlockSpec(memory_space=pltpu.VMEM), hbm),
            scratch_shapes=[
                pltpu.VMEM((4, ROWS, 768), BF16),
                pltpu.VMEM((4, 32, ROWS), BF16),
                pltpu.VMEM((4, 32, ROWS), BF16),
                pltpu.VMEM((3, ROWS, 128), F32),
                pltpu.VMEM((4, 1, ROWS), F32),
                pltpu.VMEM((8, CHUNK), F32),
                pltpu.VMEM((3, STRIP + ROWS, 32), F32),
                pltpu.VMEM((5, 32, ROWS), F32),
                pltpu.VMEM((3, 32, ROWS), F32),
                pltpu.VMEM((3, 32, ROWS), F32),
                pltpu.VMEM((3, 32, ROWS), F32),
                pltpu.VMEM((3, 32, ROWS), F32),
                pltpu.VMEM((2, UNITS, STRIP, CHUNK), BF16),
                pltpu.VMEM((2, UNITS, STRIP, CHUNK), BF16),
                pltpu.VMEM((4, 2, UNITS, STRIP, CHUNK), BF16),
                dma((2, N_STRIP)), dma((2, N_STRIP)),
                dma((3,)), dma((3,)), dma((3,)), dma((3,)), dma, dma, dma((2,)),
                dma((2, 2)), dma((4,)),
                dma((3, N_CHUNK)), dma((3, N_CHUNK)), dma((3, N_CHUNK)), dma((3, N_CHUNK)), dma((3, N_CHUNK)), dma((3, N_CHUNK)),
            ],
            compiler_params=pltpu.CompilerParams(collective_id=0, has_side_effects=True, vmem_limit_bytes=62 * 2**20),
            name="products",
        )(x_loc, v_loc.T, length_scale, out_scale)
        return w.T

    row_spec = P(("task", "row"), None)
    return jax.shard_map(local_program, mesh=mesh, in_specs=(row_spec, row_spec, P("task"), P("task")), out_specs=row_spec, check_vma=False)
```

```python
import functools

import jax
import jax.numpy as jnp
from jax import lax
from jax.experimental import pallas as pl
from jax.experimental.pallas import tpu as pltpu
from jax.sharding import PartitionSpec as P

MESH = pl.DeviceIdType.MESH
F32, BF16 = jnp.float32, jnp.bfloat16
LOG2E = 1.4426950408889634

ROWS = 3072
STRIP = 256
CHUNK = 512
N_STRIP = ROWS // STRIP
N_CHUNK = ROWS // CHUNK
UNITS = 3
OWN, XNB, YNB, PAR, TRASH = 0, 1, 2, 3, 4

N_OWN, N_PAIR, N_CROSS = 7, 13, 12
PRE = 5
OWN_AT = (5, 7, 9, 11, 12, 13, 13, 13, 13, 13, 13, 13)
CROSS_AT = (0, 0, 0, 0, 1, 2, 3, 4, 5, 6, 8, 10)
CROSS_TILE = (0, 0, 2, 4, 8, 12, 18, 24, 32, 40, 50, 60)
OWN_PLACE = 1
CROSS_PLACE = OWN_PLACE + N_PAIR
STRIP_PLACE = CROSS_PLACE + N_CROSS
N_PLACE = STRIP_PLACE + 2 * N_STRIP
N_DOUBLE = N_PLACE // 2


def table(values, n):
    out = jnp.int32(values[0])
    for i in range(1, len(values)):
        if values[i] != values[i - 1]:
            out = out + (values[i] - values[i - 1]) * (n >= i).astype(jnp.int32)
    return out


def rank(bounds, x):
    out = jnp.int32(0)
    for b in bounds:
        out = out + (x >= b).astype(jnp.int32)
    return out


def pick(cond, a, b):
    return tuple(jnp.where(cond, x, y) for x, y in zip(a, b))


def i32(*xs):
    return tuple(jnp.int32(x) for x in xs)


def own_tile(o, j, core):
    p = 3 * o + j // 2
    c = rank((1, 3, 6, 10, 15), p)
    i = p - ((c * (c + 1)) >> 1)
    own = (jnp.int32(OWN), 2 * i + j % 2, jnp.int32(OWN), c, jnp.where(i == c, TRASH, OWN))
    a = 2 * (o - N_OWN) + j // 3
    par = (jnp.int32(OWN), a, jnp.int32(PAR), 2 * (j % 3) + (((a >> 1) + core) & 1), jnp.int32(PAR))
    return pick(o < N_OWN, own, par)


def strip_tile(n, side, j):
    return (1 + side, n, jnp.int32(OWN), jnp.int32(j), jnp.int32(OWN))


def cross_tile(q, j):
    g = 6 * q + j
    n = 1 + rank(CROSS_TILE[2:11], g)
    r = g - table(CROSS_TILE, n)
    m = n >> 1
    t = pick(r < m, (jnp.int32(XNB), n, jnp.int32(YNB), r, jnp.int32(YNB)), (jnp.int32(YNB), n, jnp.int32(XNB), r - m, jnp.int32(XNB)))
    return pick(r < 2 * m, t, (jnp.int32(XNB), n - 1 + (r - 2 * m), jnp.int32(YNB), m, jnp.int32(YNB)))


def last_tile(i, j):
    n = jnp.int32(N_STRIP - 1)
    s, t = (XNB, YNB) if j % 2 else (YNB, XNB)
    cross = (jnp.int32(s), n, jnp.int32(t), 3 * i + j // 2, jnp.int32(t))
    if j >= 4:
        cross = pick(i < 1, cross, (jnp.int32(XNB), jnp.int32(N_STRIP - 2 + j % 2), jnp.int32(YNB), jnp.int32(5), jnp.int32(YNB)))
    return cross


def rows_of(a):
    return pl.ds(pl.multiple_of(a * STRIP, STRIP), STRIP)


def sums_of(c):
    return pl.ds(pl.multiple_of(STRIP + c * CHUNK, STRIP), CHUNK)


def cols_of(b):
    return pl.ds(pl.multiple_of(b * CHUNK, CHUNK), CHUNK)


def body(
    x_hbm, v_hbm, ell_ref, amp_ref, out_ref, k_hbm,
    X, VT, YV, NA, NB, CR, YR, YT, SB, RB, SB2, RB2, kr0, kr1, KB,
    sx_sem, rx_sem, sv_sem, rv_sem, sn_sem, rn_sem, sp_sem, rp_sem, loc_sem, ko_sem, ki_sem,
    s1_sem, r1_sem, sy_sem, ry_sem, s2_sem, r2_sem,
):
    me = lax.axis_index("row")
    core, cx, cy = me % 2, (me // 2) % 2, me // 4

    def dev(px, py, pc):
        return {"row": (py * 2 + px) * 2 + pc}

    tx = dev(1 - cx, cy, (core + 1 + cx) % 2)
    ty = dev(cx, 1 - cy, (core + 1 + cx + cy) % 2)
    sx = dev(1 - cx, cy, (core + cx) % 2)
    sy = dev(cx, 1 - cy, (core + cx + cy) % 2)
    pt = dev(cx, cy, 1 - core)

    def remote(src, dst, ss, rs, to):
        return pltpu.make_async_remote_copy(src_ref=src, dst_ref=dst, send_sem=ss, recv_sem=rs, device_id=to, device_id_type=MESH)

    def x_copy(j, n):
        return remote(x_hbm.at[rows_of(n)], X.at[1 + j, rows_of(n)], sx_sem.at[j, n], rx_sem.at[j, n], (tx, ty)[j])

    p_copy = remote(x_hbm, X.at[PAR], sp_sem, rp_sem, pt)
    v_copies = [remote(v_hbm, VT.at[1 + j], sv_sem.at[j], rv_sem.at[j], d) for j, d in enumerate((tx, ty, pt))]
    n_copies = [remote(NB.at[OWN], NB.at[1 + j], sn_sem.at[j], rn_sem.at[j], d) for j, d in enumerate((tx, ty, pt))]

    x_loc = pltpu.make_async_copy(x_hbm, X.at[OWN], loc_sem.at[0])
    v_loc = pltpu.make_async_copy(v_hbm, VT.at[OWN], loc_sem.at[1])
    v_loc.start()
    x_loc.start()

    barrier = pltpu.get_barrier_semaphore()
    for d in (tx, ty, sx, sy, pt):
        pl.semaphore_signal(barrier, inc=1, device_id=d, device_id_type=MESH)
    with jax.named_scope("barrier"):
        pl.semaphore_wait(barrier, 5)

    for c in v_copies:
        c.start()
    for j in range(2):
        x_copy(j, 0).start()
    p_copy.start()

    ell = jnp.full((1, CHUNK), ell_ref[0], F32)
    half = LOG2E / (2.0 * ell * ell)
    top = jnp.log2(jnp.full((1, CHUNK), amp_ref[0], F32))
    CR[0:1, :] = 2.0 * half
    CR[1:2, :] = top
    h1, l1 = half[:, 0:128], top[:, 0:128]

    for s in range(3):
        YR[s] = jnp.zeros((STRIP + ROWS, 32), F32)
    for t in range(5):
        YT[t] = jnp.zeros((32, ROWS), F32)
    kr0[...] = jnp.zeros_like(kr0)
    kr1[...] = jnp.zeros_like(kr1)

    v_loc.wait()
    with jax.named_scope("x_local"):
        x_loc.wait()

    def own_norm(c, _):
        r = pl.ds(pl.multiple_of(c * CHUNK, CHUNK), CHUNK)
        x = X[OWN, r, :].astype(F32)
        n = jnp.broadcast_to(jnp.sum(x * x, axis=1, keepdims=True), (CHUNK, 128)) * h1
        NA[OWN, r, :] = l1 - n
        NB[OWN, :, cols_of(c)] = -jnp.transpose(n)[0:1, :]
        return 0

    with jax.named_scope("own_norm"):
        lax.fori_loop(0, N_CHUNK, own_norm, 0)
    for c in n_copies:
        c.start()

    def send_strip(n, _):
        for j in range(2):
            x_copy(j, n).start()
        return 0

    lax.fori_loop(1, N_STRIP, send_strip, 0)

    def left_norm(s):
        def one(c, _):
            r = pl.ds(pl.multiple_of(c * CHUNK, CHUNK), CHUNK)
            NA[s, r, :] = l1 + jnp.transpose(jnp.broadcast_to(NB[s, :, cols_of(c)], (128, CHUNK)))
            return 0

        lax.fori_loop(0, N_CHUNK, one, 0)

    def gram(tile):
        s, a, t, b, _ = tile
        return lax.dot_general(X[s, rows_of(a), :], X[t, cols_of(b), :], (((1,), (1,)), ((), ())), preferred_element_type=F32)

    def kern(tile, g):
        s, a, t, b, _ = tile
        na = NA[s, rows_of(a), :]
        e = (g * CR[0:1, :] + NB[t, :, cols_of(b)]) + jnp.concatenate([na] * (CHUNK // 128), axis=1)
        return jnp.exp2(jnp.minimum(e, CR[1:2, :])).astype(BF16)

    def apply(tile, k, vec):
        s, a, t, b, to = tile
        YR[s, rows_of(a + 1), :] += lax.dot_general(k, vec[t, :, cols_of(b)], (((1,), (1,)), ((), ())), preferred_element_type=F32)
        YT[to, :, cols_of(b)] += jnp.dot(vec[s, :, rows_of(jnp.maximum(a, 0))], k, preferred_element_type=F32)

    def k_out(seq, place, half):
        kr = (kr0, kr1)[half]
        return pltpu.make_async_copy(kr.at[seq & 1], k_hbm.at[place, half], ko_sem.at[seq & 1, half])

    def half_step(prev, cur, kr_new, d_new, kr_old, d_old):
        gs = [gram(t) for t in cur]
        for u in range(UNITS):
            apply(prev[u], kr_old[d_old, u], VT)
        for u in range(UNITS):
            kr_new[d_new, u] = kern(cur[u], gs[u])

    def flat(tiles):
        return tuple(x for t in tiles for x in t)

    def unflat(xs):
        return [tuple(xs[5 * u : 5 * u + 5]) for u in range(UNITS)]

    def step_of(state, place, tile):
        seq, before, prev = state[0], state[1], state[2:]
        d = seq & 1

        @pl.when(seq >= 2)
        def _():
            for h in range(2):
                k_out(seq, place, h).wait()

        @pl.when(seq >= 1)
        def _():
            for h in range(2):
                k_out(seq - 1, before, h).start()

        first = [tile(u) for u in range(UNITS)]
        second = [tile(UNITS + u) for u in range(UNITS)]
        half_step(unflat(prev), first, kr0, d, kr1, 1 - d)
        half_step(first, second, kr1, d, kr0, d)
        return (seq + 1, place) + flat(second)

    none = flat([i32(OWN, -1, OWN, 0, TRASH)] * UNITS)

    def flush(state):
        for u, t in enumerate(unflat(state[2:])):
            apply(t, kr1[(state[0] - 1) & 1, u], VT)
        return state[:2] + none

    def own_step(o, state):
        return step_of(state, OWN_PLACE + o, lambda j: own_tile(o, j, core))

    def cross_step(q, state):
        return step_of(state, CROSS_PLACE + q, lambda j: cross_tile(q, j))

    def strip_step(n, side, state):
        return step_of(state, STRIP_PLACE + 2 * (N_STRIP - 1 - n) + side, lambda j: strip_tile(n, side, j))

    with jax.named_scope("pre"):
        state = lax.fori_loop(0, PRE, own_step, i32(0, 0) + none)

    with jax.named_scope("left_norm"):
        for j in range(2):
            v_copies[j].wait_recv()
            n_copies[j].wait_recv()
            left_norm(1 + j)
        p_copy.wait_recv()
        v_copies[2].wait_recv()
        n_copies[2].wait_recv()

    def strip(n, state):
        with jax.named_scope("wait_strip"):
            for j in range(2):
                x_copy(j, n).wait_recv()
        with jax.named_scope("strip"):
            state = lax.fori_loop(0, 2, lambda side, st: strip_step(n, side, st), state)
            state = lax.fori_loop(table(CROSS_AT, n), table(CROSS_AT, n + 1), cross_step, state)
            return lax.fori_loop(table(OWN_AT, n), table(OWN_AT, n + 1), own_step, state)

    state = lax.fori_loop(0, N_STRIP - 1, strip, state)

    homes = ((XNB, sx), (YNB, sy), (PAR, pt))

    def part_copy(j, c, send, recv, ss, rs):
        return remote(send.at[j, :, cols_of(c)], recv.at[j, :, cols_of(c)], ss.at[j, c], rs.at[j, c], homes[j][1])

    def finish(j, c, send):
        s = homes[j][0]
        part = YT[s, :, cols_of(c)]
        if j < 2:
            part = part + jnp.transpose(YR[s, sums_of(c), :])
            YR[s, sums_of(c), :] = jnp.zeros((CHUNK, 32), F32)
        send[j, :, cols_of(c)] = part
        YT[s, :, cols_of(c)] = jnp.zeros((32, CHUNK), F32)

    def finish_range(lo, hi, send, recv, ss, rs, js=(0, 1)):
        def one(c, _):
            for j in js:
                finish(j, c, send)
            return 0

        def go(c, _):
            for j in js:
                part_copy(j, c, send, recv, ss, rs).start()
            return 0

        lax.fori_loop(lo, hi, one, 0)
        lax.fori_loop(lo, hi, go, 0)

    def k_in(i):
        return pltpu.make_async_copy(k_hbm.at[pl.ds(2 * i, 2)], KB.at[i & 3], ki_sem.at[i & 3])

    first_in = pltpu.make_async_copy(k_hbm.at[1], KB.at[0, 1], ki_sem.at[0])
    first_in.start()
    for i in range(1, 4):
        k_in(jnp.int32(i)).start()

    finish_range(0, N_CHUNK, SB, RB, s1_sem, r1_sem, (2,))
    with jax.named_scope("wait_last"):
        for j in range(2):
            x_copy(j, N_STRIP - 1).wait_recv()

    def last_step(i, state):
        state = step_of(state, CROSS_PLACE + 10 + i, lambda j: last_tile(i, j))
        state = flush(state)
        lo, hi = 3 * i, 3 + 2 * i
        finish_range(lo, hi, SB, RB, s1_sem, r1_sem)
        return state

    with jax.named_scope("last"):
        state = lax.fori_loop(0, 2, last_step, state)
        state = lax.fori_loop(0, 2, lambda side, st: strip_step(jnp.int32(N_STRIP - 1), side, st), state)
        state = flush(state)
        finish_range(5, 6, SB, RB, s1_sem, r1_sem)

    for h in range(2):
        k_out(state[0], 0, h).wait()
        k_out(state[0] - 1, state[1], h).start()

    def y_copy(j, c):
        return remote(YV.at[OWN, :, cols_of(c)], YV.at[1 + j, :, cols_of(c)], sy_sem.at[j, c], ry_sem.at[j, c], (tx, ty, pt)[j])

    def middle(lo, hi):
        def one(c, _):
            with jax.named_scope("wait_part"):
                for j in range(3):
                    part_copy(j, c, SB, RB, s1_sem, r1_sem).wait_recv()
            y = YT[OWN, :, cols_of(c)] + jnp.transpose(YR[OWN, sums_of(c), :])
            y = y + RB[0, :, cols_of(c)] + RB[1, :, cols_of(c)] + RB[2, :, cols_of(c)]
            YV[OWN, :, cols_of(c)] = y.astype(BF16)
            YT[OWN, :, cols_of(c)] = jnp.zeros((32, CHUNK), F32)
            YR[OWN, sums_of(c), :] = jnp.zeros((CHUNK, 32), F32)
            return 0

        def go(c, _):
            for j in range(3):
                y_copy(j, c).start()
            return 0

        lax.fori_loop(lo, hi, one, 0)
        lax.fori_loop(lo, hi, go, 0)

    def second(i, tile, count=2):
        @pl.when(i + 3 < N_DOUBLE)
        def _():
            k_in(i + 3).start()

        for h in range(2 - count, 2):
            for j in range(6):
                apply(tile(h, j), KB[i & 3, h, j // 3, j % 3], YV)

    def second_own(i, _):
        k_in(i).wait()
        second(i, lambda h, j: own_tile(2 * i + h - OWN_PLACE, j, core))
        return 0

    def second_cross(i, _):
        k_in(i).wait()

        def tile(h, j):
            q = 2 * i + h - CROSS_PLACE
            return pick(q < 10, cross_tile(q, j), last_tile(q - 10, j))

        second(i, tile)
        return 0

    def second_strip(i, _):
        k_in(i).wait()
        second(i, lambda h, j: strip_tile(N_STRIP - 1 + STRIP_PLACE // 2 - i, jnp.int32(h), j))
        return 0

    def wait_y(j):
        def one(c, _):
            y_copy(j, c).wait_recv()
            return 0

        lax.fori_loop(0, N_CHUNK, one, 0)

    with jax.named_scope("middle"):
        middle(0, 4)
    with jax.named_scope("second_own"):
        first_in.wait()
        for j in range(6):
            apply(own_tile(jnp.int32(0), j, core), KB[0, 1, j // 3, j % 3], YV)

        def own_and_middle(i, _):
            second_own(i, _)
            middle(i + 3, jnp.minimum(i + 4, N_CHUNK))
            return 0

        lax.fori_loop(1, 4, own_and_middle, 0)
        for h in range(2):
            k_out(state[0] - 1, 0, h).wait()
        wait_y(2)
        lax.fori_loop(4, 7, second_own, 0)
    finish_range(0, N_CHUNK, SB2, RB2, s2_sem, r2_sem, (2,))
    with jax.named_scope("wait_y"):
        wait_y(0)
        wait_y(1)
    with jax.named_scope("second_cross"):
        lax.fori_loop(CROSS_PLACE // 2, STRIP_PLACE // 2, second_cross, 0)

    def second_chunk(k, _):
        c = N_CHUNK - 1 - k
        lo = STRIP_PLACE // 2 + 2 * k
        with jax.named_scope("second_chunk"):
            lax.fori_loop(lo, lo + 2, second_strip, 0)
        finish_range(c, c + 1, SB2, RB2, s2_sem, r2_sem)
        return 0

    lax.fori_loop(0, N_CHUNK, second_chunk, 0)

    def final(k, _):
        c = N_CHUNK - 1 - k
        for j in range(3):
            part_copy(j, c, SB2, RB2, s2_sem, r2_sem).wait_recv()
        w = YT[OWN, :, cols_of(c)] + jnp.transpose(YR[OWN, sums_of(c), :]) + RB2[0, :, cols_of(c)] + RB2[1, :, cols_of(c)] + RB2[2, :, cols_of(c)]
        out_ref[:, cols_of(c)] = w
        return 0

    with jax.named_scope("final"):
        lax.fori_loop(0, N_CHUNK, final, 0)

    with jax.named_scope("drain"):
        p_copy.wait_send()
    for c in v_copies + n_copies:
        c.wait_send()

    def sent_x(n, _):
        for j in range(2):
            x_copy(j, n).wait_send()
        return 0

    lax.fori_loop(0, N_STRIP, sent_x, 0)

    def sent(c, _):
        for j in range(3):
            part_copy(j, c, SB, RB, s1_sem, r1_sem).wait_send()
            y_copy(j, c).wait_send()
            part_copy(j, c, SB2, RB2, s2_sem, r2_sem).wait_send()
        return 0

    lax.fori_loop(0, N_CHUNK, sent, 0)


def solution(mesh):
    def local_program(x_loc, v_loc, length_scale, out_scale):
        dma = pltpu.SemaphoreType.DMA
        hbm = pl.BlockSpec(memory_space=pltpu.HBM)
        smem = pl.BlockSpec(memory_space=pltpu.SMEM)
        w, _ = pl.pallas_call(
            body,
            out_shape=(
                jax.ShapeDtypeStruct((32, ROWS), F32),
                jax.ShapeDtypeStruct((N_PLACE, 2, UNITS, STRIP, CHUNK), BF16),
            ),
            in_specs=[hbm, hbm, smem, smem],
            out_specs=(pl.BlockSpec(memory_space=pltpu.VMEM), hbm),
            scratch_shapes=[
                pltpu.VMEM((4, ROWS, 768), BF16),
                pltpu.VMEM((4, 32, ROWS), BF16),
                pltpu.VMEM((4, 32, ROWS), BF16),
                pltpu.VMEM((3, ROWS, 128), F32),
                pltpu.VMEM((4, 1, ROWS), F32),
                pltpu.VMEM((8, CHUNK), F32),
                pltpu.VMEM((3, STRIP + ROWS, 32), F32),
                pltpu.VMEM((5, 32, ROWS), F32),
                pltpu.VMEM((3, 32, ROWS), F32),
                pltpu.VMEM((3, 32, ROWS), F32),
                pltpu.VMEM((3, 32, ROWS), F32),
                pltpu.VMEM((3, 32, ROWS), F32),
                pltpu.VMEM((2, UNITS, STRIP, CHUNK), BF16),
                pltpu.VMEM((2, UNITS, STRIP, CHUNK), BF16),
                pltpu.VMEM((4, 2, 2, UNITS, STRIP, CHUNK), BF16),
                dma((2, N_STRIP)), dma((2, N_STRIP)),
                dma((3,)), dma((3,)), dma((3,)), dma((3,)), dma, dma, dma((2,)),
                dma((2, 2)), dma((4,)),
                dma((3, N_CHUNK)), dma((3, N_CHUNK)), dma((3, N_CHUNK)), dma((3, N_CHUNK)), dma((3, N_CHUNK)), dma((3, N_CHUNK)),
            ],
            compiler_params=pltpu.CompilerParams(collective_id=0, has_side_effects=True, vmem_limit_bytes=62 * 2**20),
            name="products",
        )(x_loc, v_loc.T, length_scale, out_scale)
        return w.T

    row_spec = P(("task", "row"), None)
    return jax.shard_map(local_program, mesh=mesh, in_specs=(row_spec, row_spec, P("task"), P("task")), out_specs=row_spec, check_vma=False)
```

```python
import functools

import jax
import jax.numpy as jnp
from jax import lax
from jax.experimental import pallas as pl
from jax.experimental.pallas import tpu as pltpu
from jax.sharding import PartitionSpec as P

MESH = pl.DeviceIdType.MESH
F32, BF16 = jnp.float32, jnp.bfloat16
LOG2E = 1.4426950408889634

ROWS = 3072
STRIP = 256
CHUNK = 512
N_STRIP = ROWS // STRIP
N_CHUNK = ROWS // CHUNK
UNITS = 3
OWN, XNB, YNB, PAR, TRASH = 0, 1, 2, 3, 4

N_OWN, N_PAIR, N_CROSS = 7, 13, 12
PRE = 5
OWN_AT = (5, 7, 9, 11, 12, 13, 13, 13, 13, 13, 13, 13)
CROSS_AT = (0, 0, 0, 0, 1, 2, 3, 4, 5, 6, 8, 10)
CROSS_TILE = (0, 0, 2, 4, 8, 12, 18, 24, 32, 40, 50, 60)
OWN_PLACE = (1, 2, 3, 4, 5, 48, 49, 6, 7, 44, 45, 46, 47)
CROSS_PLACE = 8
STRIP_PLACE = CROSS_PLACE + N_CROSS
N_PLACE = STRIP_PLACE + 2 * N_STRIP + 6
STEP_ROWS = 6 * STRIP
HALF_ROWS = UNITS * STRIP
Y_NEED = (4, 5, 6)


def table(values, n):
    out = jnp.int32(values[0])
    for i in range(1, len(values)):
        if values[i] != values[i - 1]:
            out = out + (values[i] - values[i - 1]) * (n >= i).astype(jnp.int32)
    return out


def rank(bounds, x):
    out = jnp.int32(0)
    for b in bounds:
        out = out + (x >= b).astype(jnp.int32)
    return out


def pick(cond, a, b):
    return tuple(jnp.where(cond, x, y) for x, y in zip(a, b))


def i32(*xs):
    return tuple(jnp.int32(x) for x in xs)


def own_tile(o, j, core):
    p = 3 * o + j // 2
    c = rank((1, 3, 6, 10, 15), p)
    i = p - ((c * (c + 1)) >> 1)
    own = (jnp.int32(OWN), 2 * i + j % 2, jnp.int32(OWN), c, jnp.where(i == c, TRASH, OWN))
    p = 3 * (o - N_OWN) + j // 2
    c = 1 + rank((1, 3, 6, 10), p)
    i = p - ((c * (c - 1)) >> 1)
    same = core + 2 * (j // 2)
    i, c = pick(p < 15, (i, c), (same, same))
    par = (jnp.int32(OWN), 2 * i + j % 2, jnp.int32(PAR), c, jnp.int32(PAR))
    return pick(o < N_OWN, own, par)


def strip_tile(n, side, j):
    return (1 + side, n, jnp.int32(OWN), jnp.int32(j), jnp.int32(OWN))


def cross_tile(q, j):
    g = 6 * q + j
    n = 1 + rank(CROSS_TILE[2:11], g)
    r = g - table(CROSS_TILE, n)
    m = n >> 1
    t = pick(r < m, (jnp.int32(XNB), n, jnp.int32(YNB), r, jnp.int32(YNB)), (jnp.int32(YNB), n, jnp.int32(XNB), r - m, jnp.int32(XNB)))
    return pick(r < 2 * m, t, (jnp.int32(XNB), n - 1 + (r - 2 * m), jnp.int32(YNB), m, jnp.int32(YNB)))


def last_tile(i, j):
    n = jnp.int32(N_STRIP - 1)
    s, t = (XNB, YNB) if j % 2 else (YNB, XNB)
    cross = (jnp.int32(s), n, jnp.int32(t), 3 * i + j // 2, jnp.int32(t))
    if j >= 4:
        cross = pick(i < 1, cross, (jnp.int32(XNB), jnp.int32(N_STRIP - 2 + j % 2), jnp.int32(YNB), jnp.int32(5), jnp.int32(YNB)))
    return cross


def rows_of(a):
    return pl.ds(pl.multiple_of(a * STRIP, STRIP), STRIP)


def sums_of(c):
    return pl.ds(pl.multiple_of(STRIP + c * CHUNK, STRIP), CHUNK)


def cols_of(b):
    return pl.ds(pl.multiple_of(b * CHUNK, CHUNK), CHUNK)


def body(
    x_hbm, v_hbm, ell_hbm, amp_hbm, out_ref, RB2, k_hbm,
    X, VT, YV, NA, NB, CR, YR, YT, SB, RB, SB2, kr0, kr1, KB, ell_ref, amp_ref,
    sx_sem, rx_sem, sv_sem, rv_sem, sn_sem, rn_sem, sp_sem, rp_sem, loc_sem, ko_sem, kb_sem, kx_sem,
    s1_sem, r1_sem, sy_sem, ry_sem, ryp_sem, s2_sem, r2_sem,
):
    me = lax.axis_index("row")
    core, cx, cy = me % 2, (me // 2) % 2, me // 4

    def dev(px, py, pc):
        return {"row": (py * 2 + px) * 2 + pc}

    tx = dev(1 - cx, cy, (core + 1 + cx) % 2)
    ty = dev(cx, 1 - cy, (core + 1 + cx + cy) % 2)
    sx = dev(1 - cx, cy, (core + cx) % 2)
    sy = dev(cx, 1 - cy, (core + cx + cy) % 2)
    pt = dev(cx, cy, 1 - core)

    def remote(src, dst, ss, rs, to):
        return pltpu.make_async_remote_copy(src_ref=src, dst_ref=dst, send_sem=ss, recv_sem=rs, device_id=to, device_id_type=MESH)

    def x_copy(j, n):
        return remote(x_hbm.at[rows_of(n)], X.at[1 + j, rows_of(n)], sx_sem.at[j], rx_sem.at[n], (tx, ty)[j])

    def wait_strip(n):
        two = X.at[1:3, rows_of(n)]
        remote(two, two, sx_sem.at[0], rx_sem.at[n], tx).wait_recv()

    p_copy = remote(x_hbm, X.at[PAR], sp_sem, rp_sem, pt)
    v_copies = [remote(v_hbm, VT.at[1 + j], sv_sem, rv_sem.at[j // 2], d) for j, d in enumerate((tx, ty, pt))]
    n_copies = [remote(NB.at[OWN], NB.at[1 + j], sn_sem, rn_sem.at[j // 2], d) for j, d in enumerate((tx, ty, pt))]

    x_loc = pltpu.make_async_copy(x_hbm, X.at[OWN], loc_sem.at[0])
    v_loc = pltpu.make_async_copy(v_hbm, VT.at[OWN], loc_sem.at[1])
    scalars = [pltpu.make_async_copy(src, dst, loc_sem.at[2 + i]) for i, (src, dst) in enumerate(((ell_hbm, ell_ref), (amp_hbm, amp_ref)))]
    for c in scalars + [v_loc, x_loc]:
        c.start()

    barrier = pltpu.get_barrier_semaphore()
    for d in (tx, ty, sx, sy, pt):
        pl.semaphore_signal(barrier, inc=1, device_id=d, device_id_type=MESH)
    with jax.named_scope("barrier"):
        pl.semaphore_wait(barrier, 5)

    for c in v_copies:
        c.start()
    for j in range(2):
        x_copy(j, 0).start()
    p_copy.start()

    for c in scalars:
        c.wait()
    ell = jnp.full((1, CHUNK), ell_ref[0], F32)
    half = LOG2E / (2.0 * ell * ell)
    top = jnp.log2(jnp.full((1, CHUNK), amp_ref[0], F32))
    CR[0:1, :] = 2.0 * half
    CR[1:2, :] = top
    h1, l1 = half[:, 0:128], top[:, 0:128]

    for s in range(3):
        YR[s] = jnp.zeros((STRIP + ROWS, 32), F32)
    for t in range(5):
        YT[t] = jnp.zeros((32, ROWS), F32)
    kr0[...] = jnp.zeros_like(kr0)
    kr1[...] = jnp.zeros_like(kr1)

    v_loc.wait()
    with jax.named_scope("x_local"):
        x_loc.wait()

    def own_norm(c, _):
        r = pl.ds(pl.multiple_of(c * CHUNK, CHUNK), CHUNK)
        x = X[OWN, r, :].astype(F32)
        n = jnp.broadcast_to(jnp.sum(x * x, axis=1, keepdims=True), (CHUNK, 128)) * h1
        NA[OWN, r, :] = l1 - n
        NB[OWN, :, cols_of(c)] = -jnp.transpose(n)[0:1, :]
        return 0

    with jax.named_scope("own_norm"):
        lax.fori_loop(0, N_CHUNK, own_norm, 0)
    for c in n_copies:
        c.start()

    def send_strip(n, _):
        for j in range(2):
            x_copy(j, n).start()
        return 0

    lax.fori_loop(1, N_STRIP, send_strip, 0)

    def left_norm(s):
        def one(c, _):
            r = pl.ds(pl.multiple_of(c * CHUNK, CHUNK), CHUNK)
            NA[s, r, :] = l1 + jnp.transpose(jnp.broadcast_to(NB[s, :, cols_of(c)], (128, CHUNK)))
            return 0

        lax.fori_loop(0, N_CHUNK, one, 0)

    def gram(tile):
        s, a, t, b, _ = tile
        return lax.dot_general(X[s, rows_of(a), :], X[t, cols_of(b), :], (((1,), (1,)), ((), ())), preferred_element_type=F32)

    def kern(tile, g):
        s, a, t, b, _ = tile
        na = NA[s, rows_of(a), :]
        e = (g * CR[0:1, :] + NB[t, :, cols_of(b)]) + jnp.concatenate([na] * (CHUNK // 128), axis=1)
        return jnp.exp2(jnp.minimum(e, CR[1:2, :])).astype(BF16)

    def apply(tile, k, vec):
        s, a, t, b, to = tile
        YR[s, rows_of(a + 1), :] += lax.dot_general(k, vec[t, :, cols_of(b)], (((1,), (1,)), ((), ())), preferred_element_type=F32)
        YT[to, :, cols_of(b)] += jnp.dot(vec[s, :, rows_of(jnp.maximum(a, 0))], k, preferred_element_type=F32)

    def k_out(seq, place, half):
        kr = (kr0, kr1)[half]
        row = pl.multiple_of(place * STEP_ROWS + half * HALF_ROWS, STRIP)
        return pltpu.make_async_copy(kr.at[seq & 1], k_hbm.at[pl.ds(row, HALF_ROWS)], ko_sem.at[seq & 1, half])

    def half_step(prev, cur, kr_new, d_new, kr_old, d_old):
        gs = [gram(t) for t in cur]
        for u in range(UNITS):
            apply(prev[u], kr_old[d_old, u * STRIP : (u + 1) * STRIP, :], VT)
        for u in range(UNITS):
            kr_new[d_new, u * STRIP : (u + 1) * STRIP, :] = kern(cur[u], gs[u])

    def flat(tiles):
        return tuple(x for t in tiles for x in t)

    def unflat(xs):
        return [tuple(xs[5 * u : 5 * u + 5]) for u in range(UNITS)]

    def step_of(state, place, tile):
        seq, before, prev = state[0], state[1], state[2:]
        d = seq & 1

        @pl.when(seq >= 2)
        def _():
            for h in range(2):
                k_out(seq, place, h).wait()

        @pl.when(seq >= 1)
        def _():
            for h in range(2):
                k_out(seq - 1, before, h).start()

        first = [tile(u) for u in range(UNITS)]
        second = [tile(UNITS + u) for u in range(UNITS)]
        half_step(unflat(prev), first, kr0, d, kr1, 1 - d)
        half_step(first, second, kr1, d, kr0, d)
        return (seq + 1, place) + flat(second)

    none = flat([i32(OWN, -1, OWN, 0, TRASH)] * UNITS)

    def flush(state):
        for u, t in enumerate(unflat(state[2:])):
            apply(t, kr1[(state[0] - 1) & 1, u * STRIP : (u + 1) * STRIP, :], VT)
        return state[:2] + none

    def own_step(o, state):
        place = table(OWN_PLACE, o)
        return step_of(state, place, lambda j: own_tile(o, j, core))

    def cross_step(q, state):
        return step_of(state, CROSS_PLACE + q, lambda j: cross_tile(q, j))

    def strip_step(n, side, state):
        return step_of(state, STRIP_PLACE + 2 * (N_STRIP - 1 - n) + side, lambda j: strip_tile(n, side, j))

    with jax.named_scope("pre"):
        state = lax.fori_loop(0, PRE, own_step, i32(0, 0) + none)

    with jax.named_scope("left_norm"):
        remote(VT.at[1:3], VT.at[1:3], sv_sem, rv_sem.at[0], tx).wait_recv()
        remote(NB.at[1:3], NB.at[1:3], sn_sem, rn_sem.at[0], tx).wait_recv()
        for j in range(2):
            left_norm(1 + j)
        p_copy.wait_recv()
        v_copies[2].wait_recv()
        n_copies[2].wait_recv()

    def strip(n, state):
        with jax.named_scope("wait_strip"):
            wait_strip(n)
        with jax.named_scope("strip"):
            state = lax.fori_loop(0, 2, lambda side, st: strip_step(n, side, st), state)
            state = lax.fori_loop(table(CROSS_AT, n), table(CROSS_AT, n + 1), cross_step, state)
            return lax.fori_loop(table(OWN_AT, n), table(OWN_AT, n + 1), own_step, state)

    state = lax.fori_loop(0, N_STRIP - 1, strip, state)

    homes = ((XNB, sx), (YNB, sy), (PAR, pt))

    def part_copy(j, c, send, recv, ss, rs):
        return remote(send.at[j, :, cols_of(c)], recv.at[j, :, cols_of(c)], ss, rs.at[c] if send is SB else rs, homes[j][1])

    def finish(j, c, send):
        s = homes[j][0]
        part = YT[s, :, cols_of(c)]
        if j < 2:
            part = part + jnp.transpose(YR[s, sums_of(c), :])
        send[j, :, cols_of(c)] = part
        if send is SB:
            YT[s, :, cols_of(c)] = jnp.zeros((32, CHUNK), F32)
            if j < 2:
                YR[s, sums_of(c), :] = jnp.zeros((CHUNK, 32), F32)

    def finish_range(lo, hi, send, recv, ss, rs, js=(0, 1)):
        def one(c, _):
            for j in js:
                finish(j, c, send)
            return 0

        lax.fori_loop(lo, hi, one, 0)
        send_range(lo, hi, send, recv, ss, rs, js)

    def send_range(lo, hi, send, recv, ss, rs, js=(0, 1)):
        def go(c, _):
            for j in js:
                part_copy(j, c, send, recv, ss, rs).start()
            return 0

        lax.fori_loop(lo, hi, go, 0)

    def load_kb(d, slot):
        return pltpu.make_async_copy(k_hbm.at[pl.ds(pl.multiple_of(d * 2 * STEP_ROWS, STRIP), 2 * STEP_ROWS)], KB.at[slot], kb_sem.at[slot])

    def load_x(d, slot):
        src = k_hbm.at[pl.ds(pl.multiple_of(d * 2 * STEP_ROWS, STRIP), 2 * STEP_ROWS)]
        return pltpu.make_async_copy(src, X.at[slot, :, 0:CHUNK], kx_sem.at[slot])

    first_in = pltpu.make_async_copy(k_hbm.at[pl.ds(STEP_ROWS, STEP_ROWS)], KB.at[0, pl.ds(STEP_ROWS, STEP_ROWS)], kb_sem.at[0])
    first_in.start()
    for i in range(1, 4):
        load_kb(i, i).start()

    finish_range(0, N_CHUNK, SB, RB, s1_sem, r1_sem, (2,))
    with jax.named_scope("wait_last"):
        wait_strip(N_STRIP - 1)

    last = jnp.int32(N_STRIP - 1)
    with jax.named_scope("last"):
        state = step_of(state, CROSS_PLACE + 10, lambda j: last_tile(jnp.int32(0), j))
        state = flush(state)
        finish_range(0, 3, SB, RB, s1_sem, r1_sem)
        state = step_of(state, CROSS_PLACE + 11, lambda j: last_tile(jnp.int32(1), j))
        finish_range(3, 4, SB, RB, s1_sem, r1_sem)
        state = strip_step(last, jnp.int32(0), state)
        finish_range(4, 5, SB, RB, s1_sem, r1_sem)
        state = strip_step(last, jnp.int32(1), state)
        for i in range(3):
            load_x(4 + 2 * i, i).start()
        state = flush(state)
        finish_range(5, 6, SB, RB, s1_sem, r1_sem)

    for h in range(2):
        k_out(state[0], 0, h).wait()
        k_out(state[0] - 1, state[1], h).start()

    def y_copy(j, c):
        return remote(YV.at[OWN, :, cols_of(c)], YV.at[1 + j, :, cols_of(c)], sy_sem, ryp_sem.at[c >> 2] if j == 2 else ry_sem.at[c], (tx, ty, pt)[j])

    def middle(lo, hi):
        def one(c, _):
            with jax.named_scope("wait_part"):
                three = RB.at[:, :, cols_of(c)]
                remote(three, three, s1_sem, r1_sem.at[c], pt).wait_recv()
            y = YT[OWN, :, cols_of(c)] + jnp.transpose(YR[OWN, sums_of(c), :])
            y = y + RB[0, :, cols_of(c)] + RB[1, :, cols_of(c)] + RB[2, :, cols_of(c)]
            YV[OWN, :, cols_of(c)] = y.astype(BF16)
            YT[OWN, :, cols_of(c)] = jnp.zeros((32, CHUNK), F32)
            YR[OWN, sums_of(c), :] = jnp.zeros((CHUNK, 32), F32)
            for j in range(3):
                y_copy(j, c).start()
            return 0

        lax.fori_loop(lo, hi, one, 0)

    def use(k, slot, tile):
        for h in range(2):
            for j in range(6):
                r = (6 * h + j) * STRIP
                apply(tile(h, j), k[slot, r : r + STRIP, 0:CHUNK], YV)

    def quad(t, tile, beside=None):
        slot = t & 3
        load_x(0, slot).wait()
        load_kb(0, slot).wait()

        @pl.when(jnp.logical_and(t >= 1, t <= 7))
        def _():
            load_x(10 + 2 * t, (t - 1) & 3).start()

        @pl.when(jnp.logical_and(t >= 1, t <= 6))
        def _():
            load_kb(11 + 2 * t, (t - 1) & 3).start()

        if beside is not None:
            beside()
        use(X, slot, lambda h, j: tile(0, h, j))
        use(KB, slot, lambda h, j: tile(1, h, j))

    def wait_y(lo, hi):
        def one(c, _):
            two = YV.at[1:3, :, cols_of(c)]
            remote(two, two, sy_sem, ry_sem.at[c], tx).wait_recv()
            return 0

        lax.fori_loop(lo, hi, one, 0)

    def wait_y_par(late):
        part = YV.at[PAR, :, pl.ds((0, 4)[late] * CHUNK, (4, 2)[late] * CHUNK)]
        remote(part, part, sy_sem, ryp_sem.at[late], pt).wait_recv()

    with jax.named_scope("middle"):
        middle(0, 4)
    with jax.named_scope("second_own"):
        first_in.wait()
        for j in range(6):
            apply(own_tile(jnp.int32(0), j, core), KB[0, STEP_ROWS + j * STRIP : STEP_ROWS + (j + 1) * STRIP, :], YV)
        load_kb(5, 0).start()

        def own_and_middle(i, _):
            load_kb(0, i).wait()
            use(KB, i, lambda h, j: own_tile(2 * i - 1 + h, j, core))
            load_kb(5 + 2 * i, i).start()
            middle(i + 3, i + 4)
            return 0

        lax.fori_loop(1, 3, own_and_middle, 0)
        for h in range(2):
            k_out(state[0] - 1, 0, h).wait()
        load_x(10, 3).start()
        wait_y_par(0)
        load_kb(0, 3).wait()
        use(KB, 3, lambda h, j: own_tile(jnp.int32(N_OWN + h), j, core))
        load_kb(11, 3).start()
    with jax.named_scope("second_cross"):

        def second_cross(t, _):
            with jax.named_scope("wait_y"):
                wait_y(table((0,) + Y_NEED[:-1], t), table(Y_NEED, t))

            def tile(d, h, j):
                q = 4 * t + 2 * d + h
                return pick(q < 10, cross_tile(q, j), last_tile(q - 10, j))

            quad(t, tile)
            return 0

        lax.fori_loop(0, 3, second_cross, 0)

    def second_chunk(k, _):
        done = N_CHUNK - jnp.maximum(k, 1)

        def beside():
            for j in range(2):
                finish(j, done, SB2)

        with jax.named_scope("second_chunk"):
            quad(3 + k, lambda d, h, j: strip_tile(2 * (N_CHUNK - 1 - k) + 1 - d, jnp.int32(h), j), beside)
        send_range(done, done + jnp.minimum(k, 1), SB2, RB2, s2_sem, r2_sem)
        return 0

    lax.fori_loop(0, N_CHUNK, second_chunk, 0)
    finish_range(0, 1, SB2, RB2, s2_sem, r2_sem)

    with jax.named_scope("second_par"):
        wait_y_par(1)
        quad(jnp.int32(9), lambda d, h, j: own_tile(jnp.int32(N_OWN + 2 + 2 * d + h), j, core))
        finish_range(0, N_CHUNK, SB2, RB2, s2_sem, r2_sem, (2,))

    with jax.named_scope("second_end"):
        load_x(0, 2).wait()
        use(X, 2, lambda h, j: own_tile(jnp.int32(5 + h), j, core))

    with jax.named_scope("sent"):
        p_copy.wait_send()
        for j in range(2):
            remote(x_hbm, X.at[1 + j], sx_sem.at[j], rx_sem.at[0], tx).wait_send()
        for buf, sem in ((VT, sv_sem), (NB, sn_sem), (YV, sy_sem)):
            remote(buf.at[1:4], buf.at[1:4], sem, rx_sem.at[0], tx).wait_send()
        remote(SB, RB, s1_sem, rx_sem.at[0], tx).wait_send()

    def final(c, _):
        out_ref[:, cols_of(c)] = YT[OWN, :, cols_of(c)] + jnp.transpose(YR[OWN, sums_of(c), :])
        return 0

    with jax.named_scope("final"):
        lax.fori_loop(0, N_CHUNK, final, 0)
        all_sums = remote(SB2, RB2, s2_sem, r2_sem, pt)
        all_sums.wait_send()
        all_sums.wait_recv()


def solution(mesh):
    def local_program(x_loc, v_loc, length_scale, out_scale):
        dma = pltpu.SemaphoreType.DMA
        hbm = pl.BlockSpec(memory_space=pltpu.HBM)
        vmem = pl.BlockSpec(memory_space=pltpu.VMEM)
        own, parts, _ = pl.pallas_call(
            body,
            out_shape=(
                pltpu.VMEM((32, ROWS), F32),
                pltpu.VMEM((3, 32, ROWS), F32),
                jax.ShapeDtypeStruct((N_PLACE * STEP_ROWS, CHUNK), BF16),
            ),
            in_specs=[hbm, hbm, hbm, hbm],
            out_specs=(vmem, vmem, hbm),
            scratch_shapes=[
                pltpu.VMEM((4, ROWS, 768), BF16),
                pltpu.VMEM((4, 32, ROWS), BF16),
                pltpu.VMEM((4, 32, ROWS), BF16),
                pltpu.VMEM((3, ROWS, 128), F32),
                pltpu.VMEM((4, 1, ROWS), F32),
                pltpu.VMEM((8, CHUNK), F32),
                pltpu.VMEM((3, STRIP + ROWS, 32), F32),
                pltpu.VMEM((5, 32, ROWS), F32),
                pltpu.VMEM((3, 32, ROWS), F32),
                pltpu.VMEM((3, 32, ROWS), F32),
                pltpu.VMEM((3, 32, ROWS), F32),
                pltpu.VMEM((2, HALF_ROWS, CHUNK), BF16),
                pltpu.VMEM((2, HALF_ROWS, CHUNK), BF16),
                pltpu.VMEM((4, 2 * STEP_ROWS, CHUNK), BF16),
                pltpu.SMEM((1,), F32), pltpu.SMEM((1,), F32),
                dma((2,)), dma((N_STRIP,)), dma, dma((2,)), dma, dma((2,)), dma, dma,
                dma((4,)), dma((2, 2)), dma((4,)), dma((4,)),
                dma, dma((N_CHUNK,)), dma, dma((N_CHUNK,)), dma((2,)), dma, dma,
            ],
            compiler_params=pltpu.CompilerParams(collective_id=0, has_side_effects=True, vmem_limit_bytes=56 * 2**20),
            name="products",
        )(x_loc, v_loc.T, length_scale, out_scale)
        return (own + parts[0] + parts[1] + parts[2]).T

    row_spec = P(("task", "row"), None)
    return jax.shard_map(local_program, mesh=mesh, in_specs=(row_spec, row_spec, P("task"), P("task")), out_specs=row_spec, check_vma=False)
```

```python
import functools

import jax
import jax.numpy as jnp
from jax import lax
from jax.experimental import pallas as pl
from jax.experimental.pallas import tpu as pltpu
from jax.sharding import PartitionSpec as P

MESH = pl.DeviceIdType.MESH
F32, BF16 = jnp.float32, jnp.bfloat16
LOG2E = 1.4426950408889634

ROWS = 3072
STRIP = 256
CHUNK = 512
N_STRIP = ROWS // STRIP
N_CHUNK = ROWS // CHUNK
UNITS = 3
OWN, XNB, YNB, PAR, TRASH = 0, 1, 2, 3, 4

N_OWN, N_PAIR, N_CROSS = 7, 13, 12
PRE = 5
OWN_AT = (5, 7, 9, 11, 12, 13, 13, 13, 13, 13, 13, 13)
CROSS_AT = (0, 0, 0, 0, 1, 2, 3, 4, 5, 6, 8, 10)
CROSS_TILE = (0, 0, 2, 4, 8, 12, 18, 24, 32, 40, 50, 60)
OWN_PLACE = (1, 2, 3, 4, 5, 48, 49, 6, 7, 44, 45, 46, 47)
STRIP_PLACE = tuple(10 - 2 * n if n < 2 else 46 - 2 * n for n in range(N_STRIP))
CROSS_PLACE = 12
N_PLACE = 50
STEP_ROWS = 6 * STRIP
HALF_ROWS = UNITS * STRIP
Y_NEED = (4, 5, 6)


def table(values, n):
    out = jnp.int32(values[0])
    for i in range(1, len(values)):
        if values[i] != values[i - 1]:
            out = out + (values[i] - values[i - 1]) * (n >= i).astype(jnp.int32)
    return out


def rank(bounds, x):
    out = jnp.int32(0)
    for b in bounds:
        out = out + (x >= b).astype(jnp.int32)
    return out


def pick(cond, a, b):
    return tuple(jnp.where(cond, x, y) for x, y in zip(a, b))


def i32(*xs):
    return tuple(jnp.int32(x) for x in xs)


def own_tile(o, j, core):
    p = 3 * o + j // 2
    c = rank((1, 3, 6, 10, 15), p)
    i = p - ((c * (c + 1)) >> 1)
    own = (jnp.int32(OWN), 2 * i + j % 2, jnp.int32(OWN), c, jnp.where(i == c, TRASH, OWN))
    p = 3 * (o - N_OWN) + j // 2
    c = 1 + rank((1, 3, 6, 10), p)
    i = p - ((c * (c - 1)) >> 1)
    same = core + 2 * (j // 2)
    i, c = pick(p < 15, (i, c), (same, same))
    par = (jnp.int32(OWN), 2 * i + j % 2, jnp.int32(PAR), c, jnp.int32(PAR))
    return pick(o < N_OWN, own, par)


def strip_tile(n, side, j):
    return (1 + side, n, jnp.int32(OWN), jnp.int32(j), jnp.int32(OWN))


def cross_tile(q, j):
    g = 6 * q + j
    n = 1 + rank(CROSS_TILE[2:11], g)
    r = g - table(CROSS_TILE, n)
    m = n >> 1
    t = pick(r < m, (jnp.int32(XNB), n, jnp.int32(YNB), r, jnp.int32(YNB)), (jnp.int32(YNB), n, jnp.int32(XNB), r - m, jnp.int32(XNB)))
    return pick(r < 2 * m, t, (jnp.int32(XNB), n - 1 + (r - 2 * m), jnp.int32(YNB), m, jnp.int32(YNB)))


def last_tile(i, j):
    n = jnp.int32(N_STRIP - 1)
    s, t = (XNB, YNB) if j % 2 else (YNB, XNB)
    cross = (jnp.int32(s), n, jnp.int32(t), 3 * i + j // 2, jnp.int32(t))
    if j >= 4:
        cross = pick(i < 1, cross, (jnp.int32(XNB), jnp.int32(N_STRIP - 2 + j % 2), jnp.int32(YNB), jnp.int32(5), jnp.int32(YNB)))
    return cross


def rows_of(a):
    return pl.ds(pl.multiple_of(a * STRIP, STRIP), STRIP)


def sums_of(c):
    return pl.ds(pl.multiple_of(STRIP + c * CHUNK, STRIP), CHUNK)


def cols_of(b):
    return pl.ds(pl.multiple_of(b * CHUNK, CHUNK), CHUNK)


def body(
    x_hbm, v_hbm, ell_hbm, amp_hbm, out_ref, RB2, k_hbm,
    X, VT, YV, NA, NB, CR, YR, YT, SB, RB, SB2, kr0, kr1, KB, ell_ref, amp_ref,
    sx_sem, rx_sem, sv_sem, rv_sem, sn_sem, rn_sem, sp_sem, rp_sem, loc_sem, ko_sem, kb_sem, kx_sem,
    s1_sem, r1_sem, sy_sem, ry_sem, ryp_sem, s2_sem, r2_sem,
):
    me = lax.axis_index("row")
    core, cx, cy = me % 2, (me // 2) % 2, me // 4

    def dev(px, py, pc):
        return {"row": (py * 2 + px) * 2 + pc}

    tx = dev(1 - cx, cy, (core + 1 + cx) % 2)
    ty = dev(cx, 1 - cy, (core + 1 + cx + cy) % 2)
    sx = dev(1 - cx, cy, (core + cx) % 2)
    sy = dev(cx, 1 - cy, (core + cx + cy) % 2)
    pt = dev(cx, cy, 1 - core)

    def remote(src, dst, ss, rs, to):
        return pltpu.make_async_remote_copy(src_ref=src, dst_ref=dst, send_sem=ss, recv_sem=rs, device_id=to, device_id_type=MESH)

    def x_copy(j, n):
        return remote(x_hbm.at[rows_of(n)], X.at[1 + j, rows_of(n)], sx_sem.at[j], rx_sem.at[n], (tx, ty)[j])

    def wait_strip(n):
        two = X.at[1:3, rows_of(n)]
        remote(two, two, sx_sem.at[0], rx_sem.at[n], tx).wait_recv()

    p_copy = remote(x_hbm, X.at[PAR], sp_sem, rp_sem, pt)
    v_copies = [remote(v_hbm, VT.at[1 + j], sv_sem, rv_sem.at[j // 2], d) for j, d in enumerate((tx, ty, pt))]
    n_copies = [remote(NB.at[OWN], NB.at[1 + j], sn_sem, rn_sem.at[j // 2], d) for j, d in enumerate((tx, ty, pt))]

    x_loc = pltpu.make_async_copy(x_hbm, X.at[OWN], loc_sem.at[0])
    v_loc = pltpu.make_async_copy(v_hbm, VT.at[OWN], loc_sem.at[1])
    scalars = [pltpu.make_async_copy(src, dst, loc_sem.at[2 + i]) for i, (src, dst) in enumerate(((ell_hbm, ell_ref), (amp_hbm, amp_ref)))]
    for c in scalars + [v_loc, x_loc]:
        c.start()

    barrier = pltpu.get_barrier_semaphore()
    for d in (tx, ty, sx, sy, pt):
        pl.semaphore_signal(barrier, inc=1, device_id=d, device_id_type=MESH)
    with jax.named_scope("barrier"):
        pl.semaphore_wait(barrier, 5)

    for c in v_copies:
        c.start()
    for j in range(2):
        x_copy(j, 0).start()
    p_copy.start()

    for c in scalars:
        c.wait()
    ell = jnp.full((1, CHUNK), ell_ref[0], F32)
    half = LOG2E / (2.0 * ell * ell)
    top = jnp.log2(jnp.full((1, CHUNK), amp_ref[0], F32))
    CR[0:1, :] = 2.0 * half
    CR[1:2, :] = top
    h1, l1 = half[:, 0:128], top[:, 0:128]

    for s in range(3):
        YR[s] = jnp.zeros((STRIP + ROWS, 32), F32)
    for t in range(5):
        YT[t] = jnp.zeros((32, ROWS), F32)
    kr0[...] = jnp.zeros_like(kr0)
    kr1[...] = jnp.zeros_like(kr1)

    v_loc.wait()
    with jax.named_scope("x_local"):
        x_loc.wait()

    def own_norm(c, _):
        r = pl.ds(pl.multiple_of(c * CHUNK, CHUNK), CHUNK)
        x = X[OWN, r, :].astype(F32)
        n = jnp.broadcast_to(jnp.sum(x * x, axis=1, keepdims=True), (CHUNK, 128)) * h1
        NA[OWN, r, :] = l1 - n
        NB[OWN, :, cols_of(c)] = -jnp.transpose(n)[0:1, :]
        return 0

    with jax.named_scope("own_norm"):
        lax.fori_loop(0, N_CHUNK, own_norm, 0)
    for c in n_copies:
        c.start()

    def send_strip(n, _):
        for j in range(2):
            x_copy(j, n).start()
        return 0

    lax.fori_loop(1, N_STRIP, send_strip, 0)

    def left_norm(s):
        def one(c, _):
            r = pl.ds(pl.multiple_of(c * CHUNK, CHUNK), CHUNK)
            NA[s, r, :] = l1 + jnp.transpose(jnp.broadcast_to(NB[s, :, cols_of(c)], (128, CHUNK)))
            return 0

        lax.fori_loop(0, N_CHUNK, one, 0)

    def gram(tile):
        s, a, t, b, _ = tile
        return lax.dot_general(X[s, rows_of(a), :], X[t, cols_of(b), :], (((1,), (1,)), ((), ())), preferred_element_type=F32)

    def kern(tile, g):
        s, a, t, b, _ = tile
        na = NA[s, rows_of(a), :]
        e = (g * CR[0:1, :] + NB[t, :, cols_of(b)]) + jnp.concatenate([na] * (CHUNK // 128), axis=1)
        return jnp.exp2(jnp.minimum(e, CR[1:2, :])).astype(BF16)

    def apply(tile, k, vec):
        s, a, t, b, to = tile
        YR[s, rows_of(a + 1), :] += lax.dot_general(k, vec[t, :, cols_of(b)], (((1,), (1,)), ((), ())), preferred_element_type=F32)
        YT[to, :, cols_of(b)] += jnp.dot(vec[s, :, rows_of(jnp.maximum(a, 0))], k, preferred_element_type=F32)

    def k_out(seq, place, half):
        kr = (kr0, kr1)[half]
        row = pl.multiple_of(place * STEP_ROWS + half * HALF_ROWS, STRIP)
        return pltpu.make_async_copy(kr.at[seq & 1], k_hbm.at[pl.ds(row, HALF_ROWS)], ko_sem.at[seq & 1, half])

    def half_step(prev, cur, kr_new, d_new, kr_old, d_old):
        gs = [gram(t) for t in cur]
        for u in range(UNITS):
            apply(prev[u], kr_old[d_old, u * STRIP : (u + 1) * STRIP, :], VT)
        for u in range(UNITS):
            kr_new[d_new, u * STRIP : (u + 1) * STRIP, :] = kern(cur[u], gs[u])

    def flat(tiles):
        return tuple(x for t in tiles for x in t)

    def unflat(xs):
        return [tuple(xs[5 * u : 5 * u + 5]) for u in range(UNITS)]

    def step_of(state, place, tile):
        seq, before, prev = state[0], state[1], state[2:]
        d = seq & 1

        @pl.when(seq >= 2)
        def _():
            for h in range(2):
                k_out(seq, place, h).wait()

        @pl.when(seq >= 1)
        def _():
            for h in range(2):
                k_out(seq - 1, before, h).start()

        first = [tile(u) for u in range(UNITS)]
        second = [tile(UNITS + u) for u in range(UNITS)]
        half_step(unflat(prev), first, kr0, d, kr1, 1 - d)
        half_step(first, second, kr1, d, kr0, d)
        return (seq + 1, place) + flat(second)

    none = flat([i32(OWN, -1, OWN, 0, TRASH)] * UNITS)

    def flush(state):
        for u, t in enumerate(unflat(state[2:])):
            apply(t, kr1[(state[0] - 1) & 1, u * STRIP : (u + 1) * STRIP, :], VT)
        return state[:2] + none

    def own_step(o, state):
        place = table(OWN_PLACE, o)
        return step_of(state, place, lambda j: own_tile(o, j, core))

    def cross_step(q, state):
        return step_of(state, CROSS_PLACE + q, lambda j: cross_tile(q, j))

    def strip_step(n, side, state):
        return step_of(state, table(STRIP_PLACE, n) + side, lambda j: strip_tile(n, side, j))

    with jax.named_scope("pre"):
        state = lax.fori_loop(0, PRE, own_step, i32(0, 0) + none)

    with jax.named_scope("left_norm"):
        remote(VT.at[1:3], VT.at[1:3], sv_sem, rv_sem.at[0], tx).wait_recv()
        remote(NB.at[1:3], NB.at[1:3], sn_sem, rn_sem.at[0], tx).wait_recv()
        for j in range(2):
            left_norm(1 + j)
        p_copy.wait_recv()
        v_copies[2].wait_recv()
        n_copies[2].wait_recv()

    def strip(n, state):
        with jax.named_scope("wait_strip"):
            wait_strip(n)
        with jax.named_scope("strip"):
            state = lax.fori_loop(0, 2, lambda side, st: strip_step(n, side, st), state)
            state = lax.fori_loop(table(CROSS_AT, n), table(CROSS_AT, n + 1), cross_step, state)
            return lax.fori_loop(table(OWN_AT, n), table(OWN_AT, n + 1), own_step, state)

    state = lax.fori_loop(0, N_STRIP - 1, strip, state)

    homes = ((XNB, sx), (YNB, sy), (PAR, pt))

    def part_copy(j, c, send, recv, ss, rs):
        return remote(send.at[j, :, cols_of(c)], recv.at[j, :, cols_of(c)], ss, rs.at[c] if send is SB else rs, homes[j][1])

    def finish(j, c, send):
        s = homes[j][0]
        part = YT[s, :, cols_of(c)]
        if j < 2:
            part = part + jnp.transpose(YR[s, sums_of(c), :])
        send[j, :, cols_of(c)] = part
        if send is SB:
            YT[s, :, cols_of(c)] = jnp.zeros((32, CHUNK), F32)
            if j < 2:
                YR[s, sums_of(c), :] = jnp.zeros((CHUNK, 32), F32)

    def finish_range(lo, hi, send, recv, ss, rs, js=(0, 1)):
        def one(c, _):
            for j in js:
                finish(j, c, send)
            return 0

        lax.fori_loop(lo, hi, one, 0)
        send_range(lo, hi, send, recv, ss, rs, js)

    def send_range(lo, hi, send, recv, ss, rs, js=(0, 1)):
        def go(c, _):
            for j in js:
                part_copy(j, c, send, recv, ss, rs).start()
            return 0

        lax.fori_loop(lo, hi, go, 0)

    def load_kb(d, slot):
        return pltpu.make_async_copy(k_hbm.at[pl.ds(pl.multiple_of(d * 2 * STEP_ROWS, STRIP), 2 * STEP_ROWS)], KB.at[slot], kb_sem.at[slot])

    def load_x(d, slot):
        src = k_hbm.at[pl.ds(pl.multiple_of(d * 2 * STEP_ROWS, STRIP), 2 * STEP_ROWS)]
        return pltpu.make_async_copy(src, X.at[slot, :, 0:CHUNK], kx_sem.at[slot])

    first_in = pltpu.make_async_copy(k_hbm.at[pl.ds(STEP_ROWS, STEP_ROWS)], KB.at[0, pl.ds(STEP_ROWS, STEP_ROWS)], kb_sem.at[0])
    first_in.start()
    for i in range(1, 4):
        load_kb(i, i).start()

    finish_range(0, N_CHUNK, SB, RB, s1_sem, r1_sem, (2,))
    with jax.named_scope("wait_last"):
        wait_strip(N_STRIP - 1)

    last = jnp.int32(N_STRIP - 1)
    with jax.named_scope("last"):
        state = step_of(state, CROSS_PLACE + 10, lambda j: last_tile(jnp.int32(0), j))
        state = flush(state)
        finish_range(0, 3, SB, RB, s1_sem, r1_sem)
        state = step_of(state, CROSS_PLACE + 11, lambda j: last_tile(jnp.int32(1), j))
        finish_range(3, 4, SB, RB, s1_sem, r1_sem)
        state = strip_step(last, jnp.int32(0), state)
        finish_range(4, 5, SB, RB, s1_sem, r1_sem)
        state = strip_step(last, jnp.int32(1), state)
        for i in range(4):
            load_x(4 + 2 * i, i).start()
        state = flush(state)
        finish_range(5, 6, SB, RB, s1_sem, r1_sem)

    for h in range(2):
        k_out(state[0], 0, h).wait()
        k_out(state[0] - 1, state[1], h).start()

    def y_copy(j, c):
        return remote(YV.at[OWN, :, cols_of(c)], YV.at[1 + j, :, cols_of(c)], sy_sem, ryp_sem.at[c >> 2] if j == 2 else ry_sem.at[c], (tx, ty, pt)[j])

    def middle(lo, hi):
        def one(c, _):
            with jax.named_scope("wait_part"):
                three = RB.at[:, :, cols_of(c)]
                remote(three, three, s1_sem, r1_sem.at[c], pt).wait_recv()
            y = YT[OWN, :, cols_of(c)] + jnp.transpose(YR[OWN, sums_of(c), :])
            y = y + RB[0, :, cols_of(c)] + RB[1, :, cols_of(c)] + RB[2, :, cols_of(c)]
            YV[OWN, :, cols_of(c)] = y.astype(BF16)
            YT[OWN, :, cols_of(c)] = jnp.zeros((32, CHUNK), F32)
            YR[OWN, sums_of(c), :] = jnp.zeros((CHUNK, 32), F32)
            for j in range(3):
                y_copy(j, c).start()
            return 0

        lax.fori_loop(lo, hi, one, 0)

    def use(k, slot, tile):
        for h in range(2):
            for j in range(6):
                r = (6 * h + j) * STRIP
                apply(tile(h, j), k[slot, r : r + STRIP, 0:CHUNK], YV)

    def quad(t, tile, beside=None):
        slot = t & 3
        load_x(0, slot).wait()
        load_kb(0, slot).wait()

        @pl.when(jnp.logical_and(t >= 1, t <= 7))
        def _():
            load_x(10 + 2 * t, (t - 1) & 3).start()

        @pl.when(jnp.logical_and(t >= 1, t <= 6))
        def _():
            load_kb(11 + 2 * t, (t - 1) & 3).start()

        if beside is not None:
            beside()
        use(X, slot, lambda h, j: tile(0, h, j))
        use(KB, slot, lambda h, j: tile(1, h, j))

    def wait_y(lo, hi):
        def one(c, _):
            two = YV.at[1:3, :, cols_of(c)]
            remote(two, two, sy_sem, ry_sem.at[c], tx).wait_recv()
            return 0

        lax.fori_loop(lo, hi, one, 0)

    def wait_y_par(late):
        part = YV.at[PAR, :, pl.ds((0, 4)[late] * CHUNK, (4, 2)[late] * CHUNK)]
        remote(part, part, sy_sem, ryp_sem.at[late], pt).wait_recv()

    with jax.named_scope("middle"):
        middle(0, 3)
    with jax.named_scope("second_own"):
        first_in.wait()
        for j in range(6):
            apply(own_tile(jnp.int32(0), j, core), KB[0, STEP_ROWS + j * STRIP : STEP_ROWS + (j + 1) * STRIP, :], YV)
        load_kb(5, 0).start()
        middle(3, 4)

        def own_and_middle(i, _):
            load_kb(0, i).wait()
            use(KB, i, lambda h, j: own_tile(2 * i - 1 + h, j, core))
            load_kb(5 + 2 * i, i).start()
            middle(i + 3, i + 4)
            return 0

        lax.fori_loop(1, 3, own_and_middle, 0)
        for h in range(2):
            k_out(state[0] - 1, 0, h).wait()
        wait_y_par(0)
        load_kb(0, 3).wait()
        use(KB, 3, lambda h, j: own_tile(jnp.int32(N_OWN + h), j, core))
        load_kb(11, 3).start()
    def strip_quad(c):
        return lambda d, h, j: strip_tile(2 * c + 1 - d, jnp.int32(h), j)

    with jax.named_scope("second_first"):
        wait_y(0, 1)
        quad(jnp.int32(0), strip_quad(jnp.int32(0)))
    with jax.named_scope("second_cross"):

        def second_cross(t, _):
            with jax.named_scope("wait_y"):
                wait_y(table((1, 1) + Y_NEED[:-1], t), table((1,) + Y_NEED, t))

            def tile(d, h, j):
                q = 4 * (t - 1) + 2 * d + h
                return pick(q < 10, cross_tile(q, j), last_tile(q - 10, j))

            quad(t, tile)
            return 0

        lax.fori_loop(1, 4, second_cross, 0)

    def second_chunk(k, _):
        done = jnp.where(k == 0, 0, N_CHUNK - k)

        def beside():
            for j in range(2):
                finish(j, done, SB2)

        with jax.named_scope("second_chunk"):
            quad(4 + k, strip_quad(N_CHUNK - 1 - k), beside)
        send_range(done, done + 1, SB2, RB2, s2_sem, r2_sem)
        return 0

    lax.fori_loop(0, N_CHUNK - 2, second_chunk, 0)

    def finish_strip(n):
        cols = pl.ds(n * STRIP, STRIP)
        for j in range(2):
            s = homes[j][0]
            SB2[j, :, cols] = YT[s, :, cols] + jnp.transpose(YR[s, pl.ds((n + 1) * STRIP, STRIP), :])
        for j in range(2):
            remote(SB2.at[j, :, cols], RB2.at[j, :, cols], s2_sem, r2_sem, homes[j][1]).start()

    with jax.named_scope("second_chunk"):
        load_x(0, 0).wait()
        load_kb(0, 0).wait()
        for j in range(2):
            finish(j, 2, SB2)
        use(X, 0, lambda h, j: strip_tile(jnp.int32(3), jnp.int32(h), j))
        send_range(2, 3, SB2, RB2, s2_sem, r2_sem)
        finish_strip(3)
        use(KB, 0, lambda h, j: strip_tile(jnp.int32(2), jnp.int32(h), j))
        finish_strip(2)

    with jax.named_scope("second_par"):
        wait_y_par(1)
        quad(jnp.int32(9), lambda d, h, j: own_tile(jnp.int32(N_OWN + 2 + 2 * d + h), j, core))
        remote(YT.at[PAR], RB2.at[2], s2_sem, r2_sem, pt).start()

    with jax.named_scope("second_end"):
        load_x(0, 2).wait()
        use(X, 2, lambda h, j: own_tile(jnp.int32(5 + h), j, core))

    with jax.named_scope("sent"):
        p_copy.wait_send()
        for j in range(2):
            remote(x_hbm, X.at[1 + j], sx_sem.at[j], rx_sem.at[0], tx).wait_send()
        for buf, sem in ((VT, sv_sem), (NB, sn_sem), (YV, sy_sem)):
            remote(buf.at[1:4], buf.at[1:4], sem, rx_sem.at[0], tx).wait_send()
        remote(SB, RB, s1_sem, rx_sem.at[0], tx).wait_send()

    def final(c, _):
        out_ref[:, cols_of(c)] = YT[OWN, :, cols_of(c)] + jnp.transpose(YR[OWN, sums_of(c), :])
        return 0

    with jax.named_scope("final"):
        lax.fori_loop(0, N_CHUNK, final, 0)
        all_sums = remote(SB2, RB2, s2_sem, r2_sem, pt)
        all_sums.wait_send()
        all_sums.wait_recv()


def solution(mesh):
    def local_program(x_loc, v_loc, length_scale, out_scale):
        dma = pltpu.SemaphoreType.DMA
        hbm = pl.BlockSpec(memory_space=pltpu.HBM)
        vmem = pl.BlockSpec(memory_space=pltpu.VMEM)
        own, parts, _ = pl.pallas_call(
            body,
            out_shape=(
                pltpu.VMEM((32, ROWS), F32),
                pltpu.VMEM((3, 32, ROWS), F32),
                jax.ShapeDtypeStruct((N_PLACE * STEP_ROWS, CHUNK), BF16),
            ),
            in_specs=[hbm, hbm, hbm, hbm],
            out_specs=(vmem, vmem, hbm),
            scratch_shapes=[
                pltpu.VMEM((4, ROWS, 768), BF16),
                pltpu.VMEM((4, 32, ROWS), BF16),
                pltpu.VMEM((4, 32, ROWS), BF16),
                pltpu.VMEM((3, ROWS, 128), F32),
                pltpu.VMEM((4, 1, ROWS), F32),
                pltpu.VMEM((8, CHUNK), F32),
                pltpu.VMEM((3, STRIP + ROWS, 32), F32),
                pltpu.VMEM((5, 32, ROWS), F32),
                pltpu.VMEM((3, 32, ROWS), F32),
                pltpu.VMEM((3, 32, ROWS), F32),
                pltpu.VMEM((3, 32, ROWS), F32),
                pltpu.VMEM((2, HALF_ROWS, CHUNK), BF16),
                pltpu.VMEM((2, HALF_ROWS, CHUNK), BF16),
                pltpu.VMEM((4, 2 * STEP_ROWS, CHUNK), BF16),
                pltpu.SMEM((1,), F32), pltpu.SMEM((1,), F32),
                dma((2,)), dma((N_STRIP,)), dma, dma((2,)), dma, dma((2,)), dma, dma,
                dma((4,)), dma((2, 2)), dma((4,)), dma((4,)),
                dma, dma((N_CHUNK,)), dma, dma((N_CHUNK,)), dma((2,)), dma, dma,
            ],
            compiler_params=pltpu.CompilerParams(collective_id=0, has_side_effects=True, vmem_limit_bytes=56 * 2**20),
            name="products",
        )(x_loc, v_loc.T, length_scale, out_scale)
        return (own + parts[0] + parts[1] + parts[2]).T

    row_spec = P(("task", "row"), None)
    return jax.shard_map(local_program, mesh=mesh, in_specs=(row_spec, row_spec, P("task"), P("task")), out_specs=row_spec, check_vma=False)
```

```python
import functools

import jax
import jax.numpy as jnp
from jax import lax
from jax.experimental import pallas as pl
from jax.experimental.pallas import tpu as pltpu
from jax.sharding import PartitionSpec as P

MESH = pl.DeviceIdType.MESH
F32, BF16 = jnp.float32, jnp.bfloat16
LOG2E = 1.4426950408889634

ROWS = 3072
STRIP = 256
CHUNK = 512
N_STRIP = ROWS // STRIP
N_CHUNK = ROWS // CHUNK
UNITS = 3
OWN, XNB, YNB, PAR, TRASH = 0, 1, 2, 3, 4

N_OWN, N_PAIR, N_CROSS = 7, 13, 12
PRE = 5
OWN_AT = (5, 7, 9, 11, 12, 13, 13, 13, 13, 13, 13, 13)
CROSS_AT = (0, 0, 0, 0, 1, 2, 3, 4, 5, 6, 8, 10)
CROSS_TILE = (0, 0, 2, 4, 8, 12, 18, 24, 32, 40, 50, 60)
OWN_PLACE = (1, 2, 3, 4, 5, 48, 49, 6, 7, 44, 45, 46, 47)
STRIP_PLACE = tuple(10 - 2 * n if n < 2 else 46 - 2 * n for n in range(N_STRIP))
CROSS_PLACE = 12
N_PLACE = 50
STEP_ROWS = 6 * STRIP
HALF_ROWS = UNITS * STRIP
Y_NEED = (4, 5, 6)


def table(values, n):
    out = jnp.int32(values[0])
    for i in range(1, len(values)):
        if values[i] != values[i - 1]:
            out = out + (values[i] - values[i - 1]) * (n >= i).astype(jnp.int32)
    return out


def rank(bounds, x):
    out = jnp.int32(0)
    for b in bounds:
        out = out + (x >= b).astype(jnp.int32)
    return out


def pick(cond, a, b):
    return tuple(jnp.where(cond, x, y) for x, y in zip(a, b))


def i32(*xs):
    return tuple(jnp.int32(x) for x in xs)


def own_tile(o, j, core):
    p = 3 * o + j // 2
    c = rank((1, 3, 6, 10, 15), p)
    i = p - ((c * (c + 1)) >> 1)
    own = (jnp.int32(OWN), 2 * i + j % 2, jnp.int32(OWN), c, jnp.where(i == c, TRASH, OWN))
    p = 3 * (o - N_OWN) + j // 2
    c = 1 + rank((1, 3, 6, 10), p)
    i = p - ((c * (c - 1)) >> 1)
    same = core + 2 * (j // 2)
    i, c = pick(p < 15, (i, c), (same, same))
    par = (jnp.int32(OWN), 2 * i + j % 2, jnp.int32(PAR), c, jnp.int32(PAR))
    return pick(o < N_OWN, own, par)


def strip_tile(n, side, j):
    return (1 + side, n, jnp.int32(OWN), jnp.int32(j), jnp.int32(OWN))


def cross_tile(q, j):
    g = 6 * q + j
    n = 1 + rank(CROSS_TILE[2:11], g)
    r = g - table(CROSS_TILE, n)
    m = n >> 1
    t = pick(r < m, (jnp.int32(XNB), n, jnp.int32(YNB), r, jnp.int32(YNB)), (jnp.int32(YNB), n, jnp.int32(XNB), r - m, jnp.int32(XNB)))
    return pick(r < 2 * m, t, (jnp.int32(XNB), n - 1 + (r - 2 * m), jnp.int32(YNB), m, jnp.int32(YNB)))


def last_tile(i, j):
    n = jnp.int32(N_STRIP - 1)
    s, t = (XNB, YNB) if j % 2 else (YNB, XNB)
    cross = (jnp.int32(s), n, jnp.int32(t), 3 * i + j // 2, jnp.int32(t))
    if j >= 4:
        cross = pick(i < 1, cross, (jnp.int32(XNB), jnp.int32(N_STRIP - 2 + j % 2), jnp.int32(YNB), jnp.int32(5), jnp.int32(YNB)))
    return cross


def rows_of(a):
    return pl.ds(pl.multiple_of(a * STRIP, STRIP), STRIP)


def sums_of(c):
    return pl.ds(pl.multiple_of(STRIP + c * CHUNK, STRIP), CHUNK)


def cols_of(b):
    return pl.ds(pl.multiple_of(b * CHUNK, CHUNK), CHUNK)


def body(
    x_hbm, v_hbm, ell_hbm, amp_hbm, out_ref, RB2, k_hbm,
    X, VT, YV, NA, NB, CR, YR, YT, SB, RB, SB2, kr0, kr1, KB, ell_ref, amp_ref,
    sx_sem, rx_sem, sv_sem, rv_sem, sn_sem, rn_sem, sp_sem, rp_sem, loc_sem, ko_sem, kb_sem, kx_sem,
    s1_sem, r1_sem, sy_sem, ry_sem, ryp_sem, s2_sem, r2_sem,
):
    me = lax.axis_index("row")
    core, cx, cy = me % 2, (me // 2) % 2, me // 4

    def dev(px, py, pc):
        return {"row": (py * 2 + px) * 2 + pc}

    tx = dev(1 - cx, cy, (core + 1 + cx) % 2)
    ty = dev(cx, 1 - cy, (core + 1 + cx + cy) % 2)
    sx = dev(1 - cx, cy, (core + cx) % 2)
    sy = dev(cx, 1 - cy, (core + cx + cy) % 2)
    pt = dev(cx, cy, 1 - core)

    def remote(src, dst, ss, rs, to):
        return pltpu.make_async_remote_copy(src_ref=src, dst_ref=dst, send_sem=ss, recv_sem=rs, device_id=to, device_id_type=MESH)

    def x_copy(j, n):
        return remote(x_hbm.at[rows_of(n)], X.at[1 + j, rows_of(n)], sx_sem.at[j], rx_sem.at[n], (tx, ty)[j])

    def wait_strip(n):
        two = X.at[1:3, rows_of(n)]
        remote(two, two, sx_sem.at[0], rx_sem.at[n], tx).wait_recv()

    p_copy = remote(x_hbm, X.at[PAR], sp_sem, rp_sem, pt)
    v_copies = [remote(v_hbm, VT.at[1 + j], sv_sem, rv_sem.at[j // 2], d) for j, d in enumerate((tx, ty, pt))]
    n_copies = [remote(NB.at[OWN], NB.at[1 + j], sn_sem, rn_sem.at[j // 2], d) for j, d in enumerate((tx, ty, pt))]

    x_loc = pltpu.make_async_copy(x_hbm, X.at[OWN], loc_sem.at[0])
    v_loc = pltpu.make_async_copy(v_hbm, VT.at[OWN], loc_sem.at[1])
    scalars = [pltpu.make_async_copy(src, dst, loc_sem.at[2 + i]) for i, (src, dst) in enumerate(((ell_hbm, ell_ref), (amp_hbm, amp_ref)))]
    for c in scalars + [v_loc, x_loc]:
        c.start()

    barrier = pltpu.get_barrier_semaphore()
    for d in (tx, ty, sx, sy, pt):
        pl.semaphore_signal(barrier, inc=1, device_id=d, device_id_type=MESH)
    with jax.named_scope("barrier"):
        pl.semaphore_wait(barrier, 5)

    for c in v_copies:
        c.start()
    for j in range(2):
        x_copy(j, 0).start()
    p_copy.start()

    for c in scalars:
        c.wait()
    ell = jnp.full((1, CHUNK), ell_ref[0], F32)
    half = LOG2E / (2.0 * ell * ell)
    top = jnp.log2(jnp.full((1, CHUNK), amp_ref[0], F32))
    CR[0:1, :] = 2.0 * half
    CR[1:2, :] = top
    h1, l1 = half[:, 0:128], top[:, 0:128]

    for s in range(3):
        YR[s] = jnp.zeros((STRIP + ROWS, 32), F32)
    for t in range(5):
        YT[t] = jnp.zeros((32, ROWS), F32)
    kr0[...] = jnp.zeros_like(kr0)
    kr1[...] = jnp.zeros_like(kr1)

    v_loc.wait()
    with jax.named_scope("x_local"):
        x_loc.wait()

    def own_norm(c, _):
        r = pl.ds(pl.multiple_of(c * CHUNK, CHUNK), CHUNK)
        x = X[OWN, r, :].astype(F32)
        n = jnp.broadcast_to(jnp.sum(x * x, axis=1, keepdims=True), (CHUNK, 128)) * h1
        NA[OWN, r, :] = l1 - n
        NB[OWN, :, cols_of(c)] = -jnp.transpose(n)[0:1, :]
        return 0

    with jax.named_scope("own_norm"):
        lax.fori_loop(0, N_CHUNK, own_norm, 0)
    for c in n_copies:
        c.start()

    def send_strip(n, _):
        for j in range(2):
            x_copy(j, n).start()
        return 0

    lax.fori_loop(1, N_STRIP, send_strip, 0)

    def left_norm(s):
        def one(c, _):
            r = pl.ds(pl.multiple_of(c * CHUNK, CHUNK), CHUNK)
            NA[s, r, :] = l1 + jnp.transpose(jnp.broadcast_to(NB[s, :, cols_of(c)], (128, CHUNK)))
            return 0

        lax.fori_loop(0, N_CHUNK, one, 0)

    def gram(tile):
        s, a, t, b, _ = tile
        return lax.dot_general(X[s, rows_of(a), :], X[t, cols_of(b), :], (((1,), (1,)), ((), ())), preferred_element_type=F32)

    def kern(tile, g):
        s, a, t, b, _ = tile
        na = NA[s, rows_of(a), :]
        e = (g * CR[0:1, :] + NB[t, :, cols_of(b)]) + jnp.concatenate([na] * (CHUNK // 128), axis=1)
        return jnp.exp2(jnp.minimum(e, CR[1:2, :])).astype(BF16)

    def apply(tile, k, vec):
        s, a, t, b, to = tile
        YR[s, rows_of(a + 1), :] += lax.dot_general(k, vec[t, :, cols_of(b)], (((1,), (1,)), ((), ())), preferred_element_type=F32)
        YT[to, :, cols_of(b)] += jnp.dot(vec[s, :, rows_of(jnp.maximum(a, 0))], k, preferred_element_type=F32)

    def k_out(seq, place, half):
        kr = (kr0, kr1)[half]
        row = pl.multiple_of(place * STEP_ROWS + half * HALF_ROWS, STRIP)
        return pltpu.make_async_copy(kr.at[seq & 1], k_hbm.at[pl.ds(row, HALF_ROWS)], ko_sem.at[seq & 1, half])

    def half_step(prev, cur, kr_new, d_new, kr_old, d_old):
        gs = [gram(t) for t in cur]
        for u in range(UNITS):
            apply(prev[u], kr_old[d_old, u * STRIP : (u + 1) * STRIP, :], VT)
        for u in range(UNITS):
            kr_new[d_new, u * STRIP : (u + 1) * STRIP, :] = kern(cur[u], gs[u])

    def flat(tiles):
        return tuple(x for t in tiles for x in t)

    def unflat(xs):
        return [tuple(xs[5 * u : 5 * u + 5]) for u in range(UNITS)]

    def step_of(state, place, tile):
        seq, before, prev = state[0], state[1], state[2:]
        d = seq & 1

        @pl.when(seq >= 2)
        def _():
            for h in range(2):
                k_out(seq, place, h).wait()

        @pl.when(seq >= 1)
        def _():
            for h in range(2):
                k_out(seq - 1, before, h).start()

        first = [tile(u) for u in range(UNITS)]
        second = [tile(UNITS + u) for u in range(UNITS)]
        half_step(unflat(prev), first, kr0, d, kr1, 1 - d)
        half_step(first, second, kr1, d, kr0, d)
        return (seq + 1, place) + flat(second)

    none = flat([i32(OWN, -1, OWN, 0, TRASH)] * UNITS)

    def flush(state):
        for u, t in enumerate(unflat(state[2:])):
            apply(t, kr1[(state[0] - 1) & 1, u * STRIP : (u + 1) * STRIP, :], VT)
        return state[:2] + none

    def own_step(o, state):
        place = table(OWN_PLACE, o)
        return step_of(state, place, lambda j: own_tile(o, j, core))

    def cross_step(q, state):
        return step_of(state, CROSS_PLACE + q, lambda j: cross_tile(q, j))

    def strip_step(n, side, state):
        return step_of(state, table(STRIP_PLACE, n) + side, lambda j: strip_tile(n, side, j))

    with jax.named_scope("pre"):
        state = lax.fori_loop(0, PRE, own_step, i32(0, 0) + none)

    with jax.named_scope("left_norm"):
        remote(VT.at[1:3], VT.at[1:3], sv_sem, rv_sem.at[0], tx).wait_recv()
        remote(NB.at[1:3], NB.at[1:3], sn_sem, rn_sem.at[0], tx).wait_recv()
        for j in range(2):
            left_norm(1 + j)
        p_copy.wait_recv()
        v_copies[2].wait_recv()
        n_copies[2].wait_recv()

    def strip(n, state):
        with jax.named_scope("wait_strip"):
            wait_strip(n)
        with jax.named_scope("strip"):
            state = lax.fori_loop(0, 2, lambda side, st: strip_step(n, side, st), state)
            state = lax.fori_loop(table(CROSS_AT, n), table(CROSS_AT, n + 1), cross_step, state)
            return lax.fori_loop(table(OWN_AT, n), table(OWN_AT, n + 1), own_step, state)

    state = lax.fori_loop(0, N_STRIP - 1, strip, state)

    homes = ((XNB, sx), (YNB, sy), (PAR, pt))

    def part_copy(j, c, send, recv, ss, rs):
        return remote(send.at[j, :, cols_of(c)], recv.at[j, :, cols_of(c)], ss, rs.at[c] if send is SB else rs, homes[j][1])

    def finish(j, c, send):
        s = homes[j][0]
        part = YT[s, :, cols_of(c)]
        if j < 2:
            part = part + jnp.transpose(YR[s, sums_of(c), :])
        send[j, :, cols_of(c)] = part
        if send is SB:
            YT[s, :, cols_of(c)] = jnp.zeros((32, CHUNK), F32)
            if j < 2:
                YR[s, sums_of(c), :] = jnp.zeros((CHUNK, 32), F32)

    def finish_range(lo, hi, send, recv, ss, rs, js=(0, 1)):
        def one(c, _):
            for j in js:
                finish(j, c, send)
            return 0

        lax.fori_loop(lo, hi, one, 0)
        send_range(lo, hi, send, recv, ss, rs, js)

    def send_range(lo, hi, send, recv, ss, rs, js=(0, 1)):
        def go(c, _):
            for j in js:
                part_copy(j, c, send, recv, ss, rs).start()
            return 0

        lax.fori_loop(lo, hi, go, 0)

    def load_kb(d, slot):
        return pltpu.make_async_copy(k_hbm.at[pl.ds(pl.multiple_of(d * 2 * STEP_ROWS, STRIP), 2 * STEP_ROWS)], KB.at[slot], kb_sem.at[slot])

    def load_x(d, slot):
        src = k_hbm.at[pl.ds(pl.multiple_of(d * 2 * STEP_ROWS, STRIP), 2 * STEP_ROWS)]
        return pltpu.make_async_copy(src, X.at[slot, :, 0:CHUNK], kx_sem.at[slot])

    first_in = pltpu.make_async_copy(k_hbm.at[pl.ds(STEP_ROWS, STEP_ROWS)], KB.at[0, pl.ds(STEP_ROWS, STEP_ROWS)], kb_sem.at[0])
    first_in.start()
    for i in range(1, 4):
        load_kb(i, i).start()

    finish_range(0, N_CHUNK, SB, RB, s1_sem, r1_sem, (2,))
    with jax.named_scope("wait_last"):
        wait_strip(N_STRIP - 1)

    last = jnp.int32(N_STRIP - 1)
    with jax.named_scope("last"):
        state = step_of(state, CROSS_PLACE + 10, lambda j: last_tile(jnp.int32(0), j))
        state = flush(state)
        finish_range(0, 3, SB, RB, s1_sem, r1_sem)
        state = step_of(state, CROSS_PLACE + 11, lambda j: last_tile(jnp.int32(1), j))
        finish_range(3, 4, SB, RB, s1_sem, r1_sem)
        state = strip_step(last, jnp.int32(0), state)
        finish_range(4, 5, SB, RB, s1_sem, r1_sem)
        state = strip_step(last, jnp.int32(1), state)
        load_x(4, 0).start()
        state = flush(state)
        finish_range(5, 6, SB, RB, s1_sem, r1_sem)

    for h in range(2):
        k_out(state[0], 0, h).wait()
        k_out(state[0] - 1, state[1], h).start()

    def y_copy(j, c):
        return remote(YV.at[OWN, :, cols_of(c)], YV.at[1 + j, :, cols_of(c)], sy_sem, ryp_sem.at[c >> 2] if j == 2 else ry_sem.at[c], (tx, ty, pt)[j])

    def middle(lo, hi):
        def one(c, _):
            with jax.named_scope("wait_part"):
                three = RB.at[:, :, cols_of(c)]
                remote(three, three, s1_sem, r1_sem.at[c], pt).wait_recv()
            y = YT[OWN, :, cols_of(c)] + jnp.transpose(YR[OWN, sums_of(c), :])
            y = y + RB[0, :, cols_of(c)] + RB[1, :, cols_of(c)] + RB[2, :, cols_of(c)]
            YV[OWN, :, cols_of(c)] = y.astype(BF16)
            YT[OWN, :, cols_of(c)] = jnp.zeros((32, CHUNK), F32)
            YR[OWN, sums_of(c), :] = jnp.zeros((CHUNK, 32), F32)
            for j in range(3):
                y_copy(j, c).start()
            return 0

        lax.fori_loop(lo, hi, one, 0)

    def use(k, slot, tile):
        for h in range(2):
            for j in range(6):
                r = (6 * h + j) * STRIP
                apply(tile(h, j), k[slot, r : r + STRIP, 0:CHUNK], YV)

    def quad(t, tile, beside=None):
        slot = t & 3
        load_x(0, slot).wait()
        load_kb(0, slot).wait()

        @pl.when(jnp.logical_and(t >= 1, t <= 7))
        def _():
            load_x(10 + 2 * t, (t - 1) & 3).start()

        @pl.when(jnp.logical_and(t >= 1, t <= 6))
        def _():
            load_kb(11 + 2 * t, (t - 1) & 3).start()

        if beside is not None:
            beside()
        use(X, slot, lambda h, j: tile(0, h, j))
        use(KB, slot, lambda h, j: tile(1, h, j))

    def wait_y(lo, hi):
        def one(c, _):
            two = YV.at[1:3, :, cols_of(c)]
            remote(two, two, sy_sem, ry_sem.at[c], tx).wait_recv()
            return 0

        lax.fori_loop(lo, hi, one, 0)

    def wait_y_par(late):
        part = YV.at[PAR, :, pl.ds((0, 4)[late] * CHUNK, (4, 2)[late] * CHUNK)]
        remote(part, part, sy_sem, ryp_sem.at[late], pt).wait_recv()

    with jax.named_scope("middle"):
        middle(0, 2)
    with jax.named_scope("second_own"):
        first_in.wait()
        for j in range(6):
            apply(own_tile(jnp.int32(0), j, core), KB[0, STEP_ROWS + j * STRIP : STEP_ROWS + (j + 1) * STRIP, :], YV)
        load_kb(5, 0).start()
        middle(2, 4)

        def own_and_middle(i, _):
            load_kb(0, i).wait()
            use(KB, i, lambda h, j: own_tile(2 * i - 1 + h, j, core))
            load_x(4 + 2 * i, i).start()
            load_kb(5 + 2 * i, i).start()
            middle(i + 3, 5)
            return 0

        lax.fori_loop(1, 3, own_and_middle, 0)
        for h in range(2):
            k_out(state[0] - 1, 0, h).wait()
        wait_y_par(0)
        load_kb(0, 3).wait()
        use(KB, 3, lambda h, j: own_tile(jnp.int32(N_OWN + h), j, core))
        load_x(10, 3).start()
        load_kb(11, 3).start()
        middle(5, 6)
    def strip_quad(c):
        return lambda d, h, j: strip_tile(2 * c + 1 - d, jnp.int32(h), j)

    with jax.named_scope("second_first"):
        wait_y(0, 1)
        quad(jnp.int32(0), strip_quad(jnp.int32(0)))
    with jax.named_scope("second_cross"):

        def second_cross(t, _):
            with jax.named_scope("wait_y"):
                wait_y(table((1, 1) + Y_NEED[:-1], t), table((1,) + Y_NEED, t))

            def tile(d, h, j):
                q = 4 * (t - 1) + 2 * d + h
                return pick(q < 10, cross_tile(q, j), last_tile(q - 10, j))

            quad(t, tile)
            return 0

        lax.fori_loop(1, 4, second_cross, 0)

    def second_chunk(k, _):
        done = jnp.where(k == 0, 0, N_CHUNK - k)

        def beside():
            for j in range(2):
                finish(j, done, SB2)

        with jax.named_scope("second_chunk"):
            quad(4 + k, strip_quad(N_CHUNK - 1 - k), beside)
        send_range(done, done + 1, SB2, RB2, s2_sem, r2_sem)
        return 0

    lax.fori_loop(0, N_CHUNK - 2, second_chunk, 0)

    def finish_strip(n):
        cols = pl.ds(n * STRIP, STRIP)
        for j in range(2):
            s = homes[j][0]
            SB2[j, :, cols] = YT[s, :, cols] + jnp.transpose(YR[s, pl.ds((n + 1) * STRIP, STRIP), :])
        for j in range(2):
            remote(SB2.at[j, :, cols], RB2.at[j, :, cols], s2_sem, r2_sem, homes[j][1]).start()

    with jax.named_scope("second_chunk"):
        load_x(0, 0).wait()
        load_kb(0, 0).wait()
        for j in range(2):
            finish(j, 2, SB2)
        use(X, 0, lambda h, j: strip_tile(jnp.int32(3), jnp.int32(h), j))
        send_range(2, 3, SB2, RB2, s2_sem, r2_sem)
        finish_strip(3)
        use(KB, 0, lambda h, j: strip_tile(jnp.int32(2), jnp.int32(h), j))
        finish_strip(2)

    with jax.named_scope("second_par"):
        wait_y_par(1)
        quad(jnp.int32(9), lambda d, h, j: own_tile(jnp.int32(N_OWN + 2 + 2 * d + h), j, core))
        remote(YT.at[PAR], RB2.at[2], s2_sem, r2_sem, pt).start()

    with jax.named_scope("second_end"):
        load_x(0, 2).wait()
        use(X, 2, lambda h, j: own_tile(jnp.int32(5 + h), j, core))

    with jax.named_scope("sent"):
        p_copy.wait_send()
        for j in range(2):
            remote(x_hbm, X.at[1 + j], sx_sem.at[j], rx_sem.at[0], tx).wait_send()
        for buf, sem in ((VT, sv_sem), (NB, sn_sem), (YV, sy_sem)):
            remote(buf.at[1:4], buf.at[1:4], sem, rx_sem.at[0], tx).wait_send()
        remote(SB, RB, s1_sem, rx_sem.at[0], tx).wait_send()

    def final(c, _):
        out_ref[:, cols_of(c)] = YT[OWN, :, cols_of(c)] + jnp.transpose(YR[OWN, sums_of(c), :])
        return 0

    with jax.named_scope("final"):
        lax.fori_loop(0, N_CHUNK, final, 0)
        all_sums = remote(SB2, RB2, s2_sem, r2_sem, pt)
        all_sums.wait_send()
        all_sums.wait_recv()


def solution(mesh):
    def local_program(x_loc, v_loc, length_scale, out_scale):
        dma = pltpu.SemaphoreType.DMA
        hbm = pl.BlockSpec(memory_space=pltpu.HBM)
        vmem = pl.BlockSpec(memory_space=pltpu.VMEM)
        own, parts, _ = pl.pallas_call(
            body,
            out_shape=(
                pltpu.VMEM((32, ROWS), F32),
                pltpu.VMEM((3, 32, ROWS), F32),
                jax.ShapeDtypeStruct((N_PLACE * STEP_ROWS, CHUNK), BF16),
            ),
            in_specs=[hbm, hbm, hbm, hbm],
            out_specs=(vmem, vmem, hbm),
            scratch_shapes=[
                pltpu.VMEM((4, ROWS, 768), BF16),
                pltpu.VMEM((4, 32, ROWS), BF16),
                pltpu.VMEM((4, 32, ROWS), BF16),
                pltpu.VMEM((3, ROWS, 128), F32),
                pltpu.VMEM((4, 1, ROWS), F32),
                pltpu.VMEM((8, CHUNK), F32),
                pltpu.VMEM((3, STRIP + ROWS, 32), F32),
                pltpu.VMEM((5, 32, ROWS), F32),
                pltpu.VMEM((3, 32, ROWS), F32),
                pltpu.VMEM((3, 32, ROWS), F32),
                pltpu.VMEM((3, 32, ROWS), F32),
                pltpu.VMEM((2, HALF_ROWS, CHUNK), BF16),
                pltpu.VMEM((2, HALF_ROWS, CHUNK), BF16),
                pltpu.VMEM((4, 2 * STEP_ROWS, CHUNK), BF16),
                pltpu.SMEM((1,), F32), pltpu.SMEM((1,), F32),
                dma((2,)), dma((N_STRIP,)), dma, dma((2,)), dma, dma((2,)), dma, dma,
                dma((4,)), dma((2, 2)), dma((4,)), dma((4,)),
                dma, dma((N_CHUNK,)), dma, dma((N_CHUNK,)), dma((2,)), dma, dma,
            ],
            compiler_params=pltpu.CompilerParams(collective_id=0, has_side_effects=True, vmem_limit_bytes=56 * 2**20),
            name="products",
        )(x_loc, v_loc.T, length_scale, out_scale)
        return (own + parts[0] + parts[1] + parts[2]).T

    row_spec = P(("task", "row"), None)
    return jax.shard_map(local_program, mesh=mesh, in_specs=(row_spec, row_spec, P("task"), P("task")), out_specs=row_spec, check_vma=False)
```

```python
import functools

import jax
import jax.numpy as jnp
from jax import lax
from jax.experimental import pallas as pl
from jax.experimental.pallas import tpu as pltpu
from jax.sharding import PartitionSpec as P

MESH = pl.DeviceIdType.MESH
F32, BF16 = jnp.float32, jnp.bfloat16
LOG2E = 1.4426950408889634

ROWS = 3072
STRIP = 256
CHUNK = 512
N_STRIP = ROWS // STRIP
N_CHUNK = ROWS // CHUNK
UNITS = 3
OWN, XNB, YNB, PAR, TRASH = 0, 1, 2, 3, 4

N_OWN, N_PAIR, N_CROSS = 7, 13, 12
PRE = 5
OWN_AT = (5, 7, 9, 11, 12, 13, 13, 13, 13, 13, 13, 13)
CROSS_AT = (0, 0, 0, 0, 1, 2, 3, 4, 5, 6, 8, 10)
CROSS_TILE = (0, 0, 2, 4, 8, 12, 18, 24, 32, 40, 50, 60)
OWN_PLACE = (1, 2, 3, 4, 5, 48, 49, 6, 7, 44, 45, 46, 47)
STRIP_PLACE = tuple(10 - 2 * n if n < 2 else 46 - 2 * n for n in range(N_STRIP))
CROSS_PLACE = 12
N_PLACE = 50
STEP_ROWS = 6 * STRIP
HALF_ROWS = UNITS * STRIP
Y_NEED = (4, 5, 6)


def table(values, n):
    out = jnp.int32(values[0])
    for i in range(1, len(values)):
        if values[i] != values[i - 1]:
            out = out + (values[i] - values[i - 1]) * (n >= i).astype(jnp.int32)
    return out


def rank(bounds, x):
    out = jnp.int32(0)
    for b in bounds:
        out = out + (x >= b).astype(jnp.int32)
    return out


def pick(cond, a, b):
    return tuple(jnp.where(cond, x, y) for x, y in zip(a, b))


def i32(*xs):
    return tuple(jnp.int32(x) for x in xs)


def own_tile(o, j, core):
    p = 3 * o + j // 2
    c = rank((1, 3, 6, 10, 15), p)
    i = p - ((c * (c + 1)) >> 1)
    own = (jnp.int32(OWN), 2 * i + j % 2, jnp.int32(OWN), c, jnp.where(i == c, TRASH, OWN))
    p = 3 * (o - N_OWN) + j // 2
    c = 1 + rank((1, 3, 6, 10), p)
    i = p - ((c * (c - 1)) >> 1)
    same = core + 2 * (j // 2)
    i, c = pick(p < 15, (i, c), (same, same))
    par = (jnp.int32(OWN), 2 * i + j % 2, jnp.int32(PAR), c, jnp.int32(PAR))
    return pick(o < N_OWN, own, par)


def strip_tile(n, side, j):
    return (1 + side, n, jnp.int32(OWN), jnp.int32(j), jnp.int32(OWN))


def cross_tile(q, j):
    g = 6 * q + j
    n = 1 + rank(CROSS_TILE[2:11], g)
    r = g - table(CROSS_TILE, n)
    m = n >> 1
    t = pick(r < m, (jnp.int32(XNB), n, jnp.int32(YNB), r, jnp.int32(YNB)), (jnp.int32(YNB), n, jnp.int32(XNB), r - m, jnp.int32(XNB)))
    return pick(r < 2 * m, t, (jnp.int32(XNB), n - 1 + (r - 2 * m), jnp.int32(YNB), m, jnp.int32(YNB)))


def last_tile(i, j):
    n = jnp.int32(N_STRIP - 1)
    s, t = (XNB, YNB) if j % 2 else (YNB, XNB)
    cross = (jnp.int32(s), n, jnp.int32(t), 3 * i + j // 2, jnp.int32(t))
    if j >= 4:
        cross = pick(i < 1, cross, (jnp.int32(XNB), jnp.int32(N_STRIP - 2 + j % 2), jnp.int32(YNB), jnp.int32(5), jnp.int32(YNB)))
    return cross


def span(start, size, unit):
    return pl.ds(start if isinstance(start, int) else pl.multiple_of(start, unit), size)


def rows_of(a):
    return span(a * STRIP, STRIP, STRIP)


def sums_of(c):
    return span(STRIP + c * CHUNK, CHUNK, STRIP)


def cols_of(b):
    return span(b * CHUNK, CHUNK, CHUNK)


def body(
    x_hbm, v_hbm, ell_hbm, amp_hbm, out_ref, RB2, k_hbm,
    X, VT, YV, NA, NB, CR, YR, YT, SB, RB, SB2, kr0, kr1, KB, ell_ref, amp_ref,
    sx_sem, rx_sem, sv_sem, rv_sem, sn_sem, rn_sem, sp_sem, rp_sem, loc_sem, ko_sem, kb_sem, kx_sem,
    s1_sem, r1_sem, sy_sem, ry_sem, ryp_sem, s2_sem, r2_sem,
):
    me = lax.axis_index("row")
    core, cx, cy = me % 2, (me // 2) % 2, me // 4

    def dev(px, py, pc):
        return {"row": (py * 2 + px) * 2 + pc}

    tx = dev(1 - cx, cy, (core + 1 + cx) % 2)
    ty = dev(cx, 1 - cy, (core + 1 + cx + cy) % 2)
    sx = dev(1 - cx, cy, (core + cx) % 2)
    sy = dev(cx, 1 - cy, (core + cx + cy) % 2)
    pt = dev(cx, cy, 1 - core)

    def remote(src, dst, ss, rs, to):
        return pltpu.make_async_remote_copy(src_ref=src, dst_ref=dst, send_sem=ss, recv_sem=rs, device_id=to, device_id_type=MESH)

    def x_copy(j, n):
        return remote(x_hbm.at[rows_of(n)], X.at[1 + j, rows_of(n)], sx_sem.at[j], rx_sem.at[n], (tx, ty)[j])

    def wait_strip(n):
        two = X.at[1:3, rows_of(n)]
        remote(two, two, sx_sem.at[0], rx_sem.at[n], tx).wait_recv()

    p_copy = remote(x_hbm, X.at[PAR], sp_sem, rp_sem, pt)
    v_copies = [remote(v_hbm, VT.at[1 + j], sv_sem, rv_sem.at[j // 2], d) for j, d in enumerate((tx, ty, pt))]
    n_copies = [remote(NB.at[OWN], NB.at[1 + j], sn_sem, rn_sem.at[j // 2], d) for j, d in enumerate((tx, ty, pt))]

    x_loc = pltpu.make_async_copy(x_hbm, X.at[OWN], loc_sem.at[0])
    v_loc = pltpu.make_async_copy(v_hbm, VT.at[OWN], loc_sem.at[1])
    scalars = [pltpu.make_async_copy(src, dst, loc_sem.at[2 + i]) for i, (src, dst) in enumerate(((ell_hbm, ell_ref), (amp_hbm, amp_ref)))]
    for c in scalars + [v_loc, x_loc]:
        c.start()

    barrier = pltpu.get_barrier_semaphore()
    for d in (tx, ty, sx, sy, pt):
        pl.semaphore_signal(barrier, inc=1, device_id=d, device_id_type=MESH)
    with jax.named_scope("barrier"):
        pl.semaphore_wait(barrier, 5)

    for c in v_copies:
        c.start()
    for j in range(2):
        x_copy(j, 0).start()
    p_copy.start()

    for c in scalars:
        c.wait()
    ell = jnp.full((1, CHUNK), ell_ref[0], F32)
    half = LOG2E / (2.0 * ell * ell)
    top = jnp.log2(jnp.full((1, CHUNK), amp_ref[0], F32))
    CR[0:1, :] = 2.0 * half
    CR[1:2, :] = top
    h1, l1 = half[:, 0:128], top[:, 0:128]

    for s in range(3):
        YR[s] = jnp.zeros((STRIP + ROWS, 32), F32)
    for t in range(5):
        YT[t] = jnp.zeros((32, ROWS), F32)
    kr0[...] = jnp.zeros_like(kr0)
    kr1[...] = jnp.zeros_like(kr1)

    v_loc.wait()
    with jax.named_scope("x_local"):
        x_loc.wait()

    def own_norm(c, _):
        r = pl.ds(pl.multiple_of(c * CHUNK, CHUNK), CHUNK)
        x = X[OWN, r, :].astype(F32)
        n = jnp.broadcast_to(jnp.sum(x * x, axis=1, keepdims=True), (CHUNK, 128)) * h1
        NA[OWN, r, :] = l1 - n
        NB[OWN, :, cols_of(c)] = -jnp.transpose(n)[0:1, :]
        return 0

    with jax.named_scope("own_norm"):
        lax.fori_loop(0, N_CHUNK, own_norm, 0)
    for c in n_copies:
        c.start()

    def send_strip(n, _):
        for j in range(2):
            x_copy(j, n).start()
        return 0

    lax.fori_loop(1, N_STRIP, send_strip, 0)

    def left_norm(s):
        def one(c, _):
            r = pl.ds(pl.multiple_of(c * CHUNK, CHUNK), CHUNK)
            NA[s, r, :] = l1 + jnp.transpose(jnp.broadcast_to(NB[s, :, cols_of(c)], (128, CHUNK)))
            return 0

        lax.fori_loop(0, N_CHUNK, one, 0)

    def gram(tile):
        s, a, t, b, _ = tile
        return lax.dot_general(X[s, rows_of(a), :], X[t, cols_of(b), :], (((1,), (1,)), ((), ())), preferred_element_type=F32)

    def kern(tile, g):
        s, a, t, b, _ = tile
        na = NA[s, rows_of(a), :]
        e = (g * CR[0:1, :] + NB[t, :, cols_of(b)]) + jnp.concatenate([na] * (CHUNK // 128), axis=1)
        return jnp.exp2(jnp.minimum(e, CR[1:2, :])).astype(BF16)

    def apply(tile, k, vec):
        s, a, t, b, to = tile
        YR[s, rows_of(a + 1), :] += lax.dot_general(k, vec[t, :, cols_of(b)], (((1,), (1,)), ((), ())), preferred_element_type=F32)
        YT[to, :, cols_of(b)] += jnp.dot(vec[s, :, rows_of(jnp.maximum(a, 0))], k, preferred_element_type=F32)

    def k_out(seq, place, half):
        kr = (kr0, kr1)[half]
        row = pl.multiple_of(place * STEP_ROWS + half * HALF_ROWS, STRIP)
        return pltpu.make_async_copy(kr.at[seq & 1], k_hbm.at[pl.ds(row, HALF_ROWS)], ko_sem.at[seq & 1, half])

    def half_step(prev, cur, kr_new, d_new, kr_old, d_old):
        gs = [gram(t) for t in cur]
        for u in range(UNITS):
            apply(prev[u], kr_old[d_old, u * STRIP : (u + 1) * STRIP, :], VT)
        for u in range(UNITS):
            kr_new[d_new, u * STRIP : (u + 1) * STRIP, :] = kern(cur[u], gs[u])

    def flat(tiles):
        return tuple(x for t in tiles for x in t)

    def unflat(xs):
        return [tuple(xs[5 * u : 5 * u + 5]) for u in range(UNITS)]

    def step_of(state, place, tile):
        seq, before, prev = state[0], state[1], state[2:]
        d = seq & 1

        @pl.when(seq >= 2)
        def _():
            for h in range(2):
                k_out(seq, place, h).wait()

        @pl.when(seq >= 1)
        def _():
            for h in range(2):
                k_out(seq - 1, before, h).start()

        first = [tile(u) for u in range(UNITS)]
        second = [tile(UNITS + u) for u in range(UNITS)]
        half_step(unflat(prev), first, kr0, d, kr1, 1 - d)
        half_step(first, second, kr1, d, kr0, d)
        return (seq + 1, place) + flat(second)

    none = flat([i32(OWN, -1, OWN, 0, TRASH)] * UNITS)

    def flush(state):
        for u, t in enumerate(unflat(state[2:])):
            apply(t, kr1[(state[0] - 1) & 1, u * STRIP : (u + 1) * STRIP, :], VT)
        return state[:2] + none

    def own_step(o, state):
        place = table(OWN_PLACE, o)
        return step_of(state, place, lambda j: own_tile(o, j, core))

    def cross_step(q, state):
        return step_of(state, CROSS_PLACE + q, lambda j: cross_tile(q, j))

    def strip_step(n, side, state):
        return step_of(state, table(STRIP_PLACE, n) + side, lambda j: strip_tile(n, side, j))

    with jax.named_scope("pre"):
        state = lax.fori_loop(0, PRE, own_step, i32(0, 0) + none)

    with jax.named_scope("left_norm"):
        remote(VT.at[1:3], VT.at[1:3], sv_sem, rv_sem.at[0], tx).wait_recv()
        remote(NB.at[1:3], NB.at[1:3], sn_sem, rn_sem.at[0], tx).wait_recv()
        for j in range(2):
            left_norm(1 + j)
        p_copy.wait_recv()
        v_copies[2].wait_recv()
        n_copies[2].wait_recv()

    def strip(n, state):
        with jax.named_scope("wait_strip"):
            wait_strip(n)
        with jax.named_scope("strip"):
            state = lax.fori_loop(0, 2, lambda side, st: strip_step(n, side, st), state)
            state = lax.fori_loop(table(CROSS_AT, n), table(CROSS_AT, n + 1), cross_step, state)
            return lax.fori_loop(table(OWN_AT, n), table(OWN_AT, n + 1), own_step, state)

    state = lax.fori_loop(0, N_STRIP - 1, strip, state)

    homes = ((XNB, sx), (YNB, sy), (PAR, pt))

    def part_copy(j, c, send, recv, ss, rs):
        return remote(send.at[j, :, cols_of(c)], recv.at[j, :, cols_of(c)], ss, rs.at[c] if send is SB else rs, homes[j][1])

    def finish(j, c, send):
        s = homes[j][0]
        part = YT[s, :, cols_of(c)]
        if j < 2:
            part = part + jnp.transpose(YR[s, sums_of(c), :])
        send[j, :, cols_of(c)] = part
        if send is SB:
            YT[s, :, cols_of(c)] = jnp.zeros((32, CHUNK), F32)
            if j < 2:
                YR[s, sums_of(c), :] = jnp.zeros((CHUNK, 32), F32)

    def finish_range(lo, hi, send, recv, ss, rs, js=(0, 1)):
        def one(c, _):
            for j in js:
                finish(j, c, send)
            return 0

        for c in range(lo, hi):
            one(c, 0)
            for j in js:
                part_copy(j, c, send, recv, ss, rs).start()

    def send_range(lo, hi, send, recv, ss, rs, js=(0, 1)):
        def go(c, _):
            for j in js:
                part_copy(j, c, send, recv, ss, rs).start()
            return 0

        lax.fori_loop(lo, hi, go, 0)

    def load_kb(d, slot):
        return pltpu.make_async_copy(k_hbm.at[pl.ds(pl.multiple_of(d * 2 * STEP_ROWS, STRIP), 2 * STEP_ROWS)], KB.at[slot], kb_sem.at[slot])

    def load_x(d, slot):
        src = k_hbm.at[pl.ds(pl.multiple_of(d * 2 * STEP_ROWS, STRIP), 2 * STEP_ROWS)]
        return pltpu.make_async_copy(src, X.at[slot, :, 0:CHUNK], kx_sem.at[slot])

    first_in = pltpu.make_async_copy(k_hbm.at[pl.ds(STEP_ROWS, STEP_ROWS)], KB.at[0, pl.ds(STEP_ROWS, STEP_ROWS)], kb_sem.at[0])
    first_in.start()
    for i in range(1, 4):
        load_kb(i, i).start()

    finish_range(0, N_CHUNK, SB, RB, s1_sem, r1_sem, (2,))
    with jax.named_scope("wait_last"):
        wait_strip(N_STRIP - 1)

    last = jnp.int32(N_STRIP - 1)
    with jax.named_scope("last"):
        state = step_of(state, CROSS_PLACE + 10, lambda j: last_tile(jnp.int32(0), j))
        finish_range(0, 1, SB, RB, s1_sem, r1_sem)
        state = flush(state)
        finish_range(1, 3, SB, RB, s1_sem, r1_sem)
        state = step_of(state, CROSS_PLACE + 11, lambda j: last_tile(jnp.int32(1), j))
        finish_range(3, 4, SB, RB, s1_sem, r1_sem)
        state = strip_step(last, jnp.int32(0), state)
        finish_range(4, 5, SB, RB, s1_sem, r1_sem)
        state = strip_step(last, jnp.int32(1), state)
        load_x(4, 0).start()
        state = flush(state)
        finish_range(5, 6, SB, RB, s1_sem, r1_sem)

    for h in range(2):
        k_out(state[0], 0, h).wait()
        k_out(state[0] - 1, state[1], h).start()

    def y_copy(j, c):
        return remote(YV.at[OWN, :, cols_of(c)], YV.at[1 + j, :, cols_of(c)], sy_sem, ryp_sem.at[c >> 2] if j == 2 else ry_sem.at[c], (tx, ty, pt)[j])

    def middle(lo, hi):
        def one(c, _):
            with jax.named_scope("wait_part"):
                three = RB.at[:, :, cols_of(c)]
                remote(three, three, s1_sem, r1_sem.at[c], pt).wait_recv()
            y = YT[OWN, :, cols_of(c)] + jnp.transpose(YR[OWN, sums_of(c), :])
            y = y + RB[0, :, cols_of(c)] + RB[1, :, cols_of(c)] + RB[2, :, cols_of(c)]
            YV[OWN, :, cols_of(c)] = y.astype(BF16)
            YT[OWN, :, cols_of(c)] = jnp.zeros((32, CHUNK), F32)
            YR[OWN, sums_of(c), :] = jnp.zeros((CHUNK, 32), F32)
            for j in range(3):
                y_copy(j, c).start()
            return 0

        lax.fori_loop(lo, hi, one, 0)

    def use(k, slot, tile):
        for h in range(2):
            use_step(k, slot, h, functools.partial(tile, h))

    def use_step(k, slot, h, tile):
        for j in range(6):
            r = (6 * h + j) * STRIP
            apply(tile(j), k[slot, r : r + STRIP, 0:CHUNK], YV)

    def quad(t, tile, beside=None):
        slot = t & 3
        load_x(0, slot).wait()
        load_kb(0, slot).wait()

        @pl.when(jnp.logical_and(t >= 1, t <= 7))
        def _():
            load_x(10 + 2 * t, (t - 1) & 3).start()

        @pl.when(jnp.logical_and(t >= 1, t <= 6))
        def _():
            load_kb(11 + 2 * t, (t - 1) & 3).start()

        if beside is not None:
            beside()
        use(X, slot, lambda h, j: tile(0, h, j))
        use(KB, slot, lambda h, j: tile(1, h, j))

    def wait_y(lo, hi):
        def one(c, _):
            two = YV.at[1:3, :, cols_of(c)]
            remote(two, two, sy_sem, ry_sem.at[c], tx).wait_recv()
            return 0

        lax.fori_loop(lo, hi, one, 0)

    def wait_y_par(late):
        part = YV.at[PAR, :, pl.ds((0, 4)[late] * CHUNK, (4, 2)[late] * CHUNK)]
        remote(part, part, sy_sem, ryp_sem.at[late], pt).wait_recv()

    with jax.named_scope("middle"):
        middle(0, 2)
    with jax.named_scope("second_own"):
        first_in.wait()
        for j in range(6):
            apply(own_tile(jnp.int32(0), j, core), KB[0, STEP_ROWS + j * STRIP : STEP_ROWS + (j + 1) * STRIP, :], YV)
        load_kb(5, 0).start()
        middle(2, 3)
        load_kb(0, 1).wait()
        use_step(KB, 1, 0, lambda j: own_tile(jnp.int32(1), j, core))
        middle(3, 4)
        use_step(KB, 1, 1, lambda j: own_tile(jnp.int32(2), j, core))
        load_x(6, 1).start()
        load_kb(7, 1).start()
        middle(4, 5)
        load_kb(0, 2).wait()
        use(KB, 2, lambda h, j: own_tile(jnp.int32(3 + h), j, core))
        load_x(8, 2).start()
        load_kb(9, 2).start()
        for h in range(2):
            k_out(state[0] - 1, 0, h).wait()
        wait_y_par(0)
        load_kb(0, 3).wait()
        use(KB, 3, lambda h, j: own_tile(jnp.int32(N_OWN + h), j, core))
        load_x(10, 3).start()
        load_kb(11, 3).start()
        middle(5, 6)
    def strip_quad(c):
        return lambda d, h, j: strip_tile(2 * c + 1 - d, jnp.int32(h), j)

    with jax.named_scope("second_first"):
        wait_y(0, 1)
        quad(jnp.int32(0), strip_quad(jnp.int32(0)))
    with jax.named_scope("second_cross"):

        def second_cross(t, _):
            with jax.named_scope("wait_y"):
                wait_y(table((1, 1) + Y_NEED[:-1], t), table((1,) + Y_NEED, t))

            def tile(d, h, j):
                q = 4 * (t - 1) + 2 * d + h
                return pick(q < 10, cross_tile(q, j), last_tile(q - 10, j))

            quad(t, tile)
            return 0

        lax.fori_loop(1, 4, second_cross, 0)

    def second_chunk(k, _):
        done = jnp.where(k == 0, 0, N_CHUNK - k)

        def beside():
            for j in range(2):
                finish(j, done, SB2)

        with jax.named_scope("second_chunk"):
            quad(4 + k, strip_quad(N_CHUNK - 1 - k), beside)
        send_range(done, done + 1, SB2, RB2, s2_sem, r2_sem)
        return 0

    lax.fori_loop(0, N_CHUNK - 2, second_chunk, 0)

    def finish_strip(n):
        cols = pl.ds(n * STRIP, STRIP)
        for j in range(2):
            s = homes[j][0]
            SB2[j, :, cols] = YT[s, :, cols] + jnp.transpose(YR[s, pl.ds((n + 1) * STRIP, STRIP), :])
        for j in range(2):
            remote(SB2.at[j, :, cols], RB2.at[j, :, cols], s2_sem, r2_sem, homes[j][1]).start()

    with jax.named_scope("second_chunk"):
        load_x(0, 0).wait()
        load_kb(0, 0).wait()
        for j in range(2):
            finish(j, 2, SB2)
        use(X, 0, lambda h, j: strip_tile(jnp.int32(3), jnp.int32(h), j))
        send_range(2, 3, SB2, RB2, s2_sem, r2_sem)
        finish_strip(3)
        use(KB, 0, lambda h, j: strip_tile(jnp.int32(2), jnp.int32(h), j))
        finish_strip(2)

    with jax.named_scope("second_par"):
        wait_y_par(1)
        quad(jnp.int32(9), lambda d, h, j: own_tile(jnp.int32(N_OWN + 2 + 2 * d + h), j, core))
        remote(YT.at[PAR], RB2.at[2], s2_sem, r2_sem, pt).start()

    with jax.named_scope("second_end"):
        load_x(0, 2).wait()
        use(X, 2, lambda h, j: own_tile(jnp.int32(5 + h), j, core))

    with jax.named_scope("sent"):
        p_copy.wait_send()
        for j in range(2):
            remote(x_hbm, X.at[1 + j], sx_sem.at[j], rx_sem.at[0], tx).wait_send()
        for buf, sem in ((VT, sv_sem), (NB, sn_sem), (YV, sy_sem)):
            remote(buf.at[1:4], buf.at[1:4], sem, rx_sem.at[0], tx).wait_send()
        remote(SB, RB, s1_sem, rx_sem.at[0], tx).wait_send()

    def final(c, _):
        out_ref[:, cols_of(c)] = YT[OWN, :, cols_of(c)] + jnp.transpose(YR[OWN, sums_of(c), :])
        return 0

    with jax.named_scope("final"):
        for c in range(N_CHUNK):
            final(c, 0)
        all_sums = remote(SB2, RB2, s2_sem, r2_sem, pt)
        all_sums.wait_send()
        all_sums.wait_recv()


def solution(mesh):
    def local_program(x_loc, v_loc, length_scale, out_scale):
        dma = pltpu.SemaphoreType.DMA
        hbm = pl.BlockSpec(memory_space=pltpu.HBM)
        vmem = pl.BlockSpec(memory_space=pltpu.VMEM)
        own, parts, _ = pl.pallas_call(
            body,
            out_shape=(
                pltpu.VMEM((32, ROWS), F32),
                pltpu.VMEM((3, 32, ROWS), F32),
                jax.ShapeDtypeStruct((N_PLACE * STEP_ROWS, CHUNK), BF16),
            ),
            in_specs=[hbm, hbm, hbm, hbm],
            out_specs=(vmem, vmem, hbm),
            scratch_shapes=[
                pltpu.VMEM((4, ROWS, 768), BF16),
                pltpu.VMEM((4, 32, ROWS), BF16),
                pltpu.VMEM((4, 32, ROWS), BF16),
                pltpu.VMEM((3, ROWS, 128), F32),
                pltpu.VMEM((4, 1, ROWS), F32),
                pltpu.VMEM((8, CHUNK), F32),
                pltpu.VMEM((3, STRIP + ROWS, 32), F32),
                pltpu.VMEM((5, 32, ROWS), F32),
                pltpu.VMEM((3, 32, ROWS), F32),
                pltpu.VMEM((3, 32, ROWS), F32),
                pltpu.VMEM((3, 32, ROWS), F32),
                pltpu.VMEM((2, HALF_ROWS, CHUNK), BF16),
                pltpu.VMEM((2, HALF_ROWS, CHUNK), BF16),
                pltpu.VMEM((4, 2 * STEP_ROWS, CHUNK), BF16),
                pltpu.SMEM((1,), F32), pltpu.SMEM((1,), F32),
                dma((2,)), dma((N_STRIP,)), dma, dma((2,)), dma, dma((2,)), dma, dma,
                dma((4,)), dma((2, 2)), dma((4,)), dma((4,)),
                dma, dma((N_CHUNK,)), dma, dma((N_CHUNK,)), dma((2,)), dma, dma,
            ],
            compiler_params=pltpu.CompilerParams(collective_id=0, has_side_effects=True, vmem_limit_bytes=56 * 2**20),
            name="products",
        )(x_loc, v_loc.T, length_scale, out_scale)
        return (own + parts[0] + parts[1] + parts[2]).T

    row_spec = P(("task", "row"), None)
    return jax.shard_map(local_program, mesh=mesh, in_specs=(row_spec, row_spec, P("task"), P("task")), out_specs=row_spec, check_vma=False)
```

```python
import functools

import jax
import jax.numpy as jnp
from jax import lax
from jax.experimental import pallas as pl
from jax.experimental.pallas import tpu as pltpu
from jax.sharding import PartitionSpec as P

MESH = pl.DeviceIdType.MESH
F32, BF16 = jnp.float32, jnp.bfloat16
LOG2E = 1.4426950408889634

ROWS = 3072
STRIP = 256
CHUNK = 512
N_STRIP = ROWS // STRIP
N_CHUNK = ROWS // CHUNK
UNITS = 3
OWN, XNB, YNB, PAR, TRASH = 0, 1, 2, 3, 4

N_OWN, N_PAIR = 7, 13
REMOTE_AT = (0, 0, 7, 7, 13, 13, 18, 18, 21, 21, 23, 23)
REMOTE_TILE = (0, 44, 80, 108, 128, 140)
CROSS_AT = (0, 0, 0, 0, 1, 2, 3, 4, 5, 6, 8, 10)
CROSS_TILE = (0, 0, 2, 4, 8, 12, 18, 24, 32, 40, 50, 60)
OWN_PLACE = (1, 2, 3, 6, 7, 48, 49, 4, 5, 44, 45, 46, 47)
REMOTE_ORDER = (20, 21, 22, 23, 16, 17, 18, 19, 10, 13, 14, 15, 4, 5, 6, 7, 8, 9, 11, 12)
REMOTE_PLACE = tuple(8 + p if p < 4 else 24 + REMOTE_ORDER.index(p) for p in range(24))
CROSS_PLACE = 12
N_PLACE = 50
STEP_ROWS = 6 * STRIP
HALF_ROWS = UNITS * STRIP
Y_NEED = (4, 5, 6)


def table(values, n):
    out = jnp.int32(values[0])
    for i in range(1, len(values)):
        if values[i] != values[i - 1]:
            out = out + (values[i] - values[i - 1]) * (n >= i).astype(jnp.int32)
    return out


def rank(bounds, x):
    out = jnp.int32(0)
    for b in bounds:
        out = out + (x >= b).astype(jnp.int32)
    return out


def pick(cond, a, b):
    return tuple(jnp.where(cond, x, y) for x, y in zip(a, b))


def i32(*xs):
    return tuple(jnp.int32(x) for x in xs)


def own_tile(o, j, core):
    p = 3 * o + j // 2
    c = rank((1, 3, 6, 10, 15), p)
    i = p - ((c * (c + 1)) >> 1)
    own = (jnp.int32(OWN), 2 * i + j % 2, jnp.int32(OWN), c, jnp.where(i == c, TRASH, OWN))
    p = 3 * (o - N_OWN) + j // 2
    c = 1 + rank((1, 3, 6, 10), p)
    i = p - ((c * (c - 1)) >> 1)
    same = core + 2 * (j // 2)
    i, c = pick(p < 15, (i, c), (same, same))
    par = (jnp.int32(OWN), 2 * i + j % 2, jnp.int32(PAR), c, jnp.int32(PAR))
    return pick(o < N_OWN, own, par)


def remote_tile(p, j):
    g = 6 * p + j
    d, first = jnp.int32(0), jnp.int32(0)
    for i in range(1, N_CHUNK):
        d, first = pick(g >= REMOTE_TILE[i], (i, REMOTE_TILE[i]), (d, first))
    r = g - first
    rest = r - (22 - 4 * d)
    k, side, odd = pick(rest >= 0, (rest >> 1, r & 1, 1), (r >> 1, r & 1, 0))
    k, side, odd = pick(d == 0, (r >> 2, (r >> 1) & 1, r & 1), (k, side, odd))
    t = jnp.where((k & 1) == (k > 0).astype(jnp.int32), OWN, PAR)
    return (1 + side, 2 * d + odd, t, d + ((k + 1) >> 1), t)


def cross_tile(q, j):
    g = 6 * q + j
    n = 1 + rank(CROSS_TILE[2:11], g)
    r = g - table(CROSS_TILE, n)
    m = n >> 1
    t = pick(r < m, (jnp.int32(XNB), n, jnp.int32(YNB), r, jnp.int32(YNB)), (jnp.int32(YNB), n, jnp.int32(XNB), r - m, jnp.int32(XNB)))
    return pick(r < 2 * m, t, (jnp.int32(XNB), n - 1 + (r - 2 * m), jnp.int32(YNB), m, jnp.int32(YNB)))


def last_tiles():
    n = N_STRIP - 1
    tiles = [t for c in range(N_CHUNK - 1) for t in ((YNB, n, XNB, c, XNB), (XNB, n, YNB, c, YNB))]
    tiles += [(XNB, n - 1, YNB, N_CHUNK - 1, YNB), (XNB, n, YNB, N_CHUNK - 1, YNB)]
    return [i32(*t) for t in tiles]


def span(start, size, unit):
    return pl.ds(start if isinstance(start, int) else pl.multiple_of(start, unit), size)


def rows_of(a):
    return span(a * STRIP, STRIP, STRIP)


def sums_of(c):
    return span(STRIP + c * CHUNK, CHUNK, STRIP)


def cols_of(b):
    return span(b * CHUNK, CHUNK, CHUNK)


def body(
    x_hbm, v_hbm, ell_hbm, amp_hbm, out_ref, RB2, k_hbm,
    X, VT, YV, NA, NB, CR, YR, YT, SB, RB, SB2, kr0, kr1, KL, KB, ell_ref, amp_ref,
    sx_sem, rx_sem, sv_sem, rv_sem, sn_sem, rn_sem, sp_sem, rp_sem, loc_sem, ko_sem, kb_sem, kx_sem,
    s1_sem, r1_sem, sy_sem, ry_sem, ryp_sem, s2_sem, r2_sem,
):
    me = lax.axis_index("row")
    core, cx, cy = me % 2, (me // 2) % 2, me // 4

    def dev(px, py, pc):
        return {"row": (py * 2 + px) * 2 + pc}

    tx = dev(1 - cx, cy, (core + 1 + cx) % 2)
    ty = dev(cx, 1 - cy, (core + 1 + cx + cy) % 2)
    sx = dev(1 - cx, cy, (core + cx) % 2)
    sy = dev(cx, 1 - cy, (core + cx + cy) % 2)
    pt = dev(cx, cy, 1 - core)

    def remote(src, dst, ss, rs, to):
        return pltpu.make_async_remote_copy(src_ref=src, dst_ref=dst, send_sem=ss, recv_sem=rs, device_id=to, device_id_type=MESH)

    def x_copy(j, n):
        return remote(x_hbm.at[rows_of(n)], X.at[1 + j, rows_of(n)], sx_sem.at[j], rx_sem.at[n], (tx, ty)[j])

    def wait_strip(n):
        two = X.at[1:3, rows_of(n)]
        remote(two, two, sx_sem.at[0], rx_sem.at[n], tx).wait_recv()

    p_copy = remote(x_hbm, X.at[PAR], sp_sem, rp_sem, pt)
    v_copies = [remote(v_hbm, VT.at[1 + j], sv_sem, rv_sem.at[j // 2], d) for j, d in enumerate((tx, ty, pt))]
    n_copies = [remote(NB.at[OWN], NB.at[1 + j], sn_sem, rn_sem.at[j // 2], d) for j, d in enumerate((tx, ty, pt))]

    x_loc = pltpu.make_async_copy(x_hbm, X.at[OWN], loc_sem.at[0])
    v_loc = pltpu.make_async_copy(v_hbm, VT.at[OWN], loc_sem.at[1])
    scalars = [pltpu.make_async_copy(src, dst, loc_sem.at[2 + i]) for i, (src, dst) in enumerate(((ell_hbm, ell_ref), (amp_hbm, amp_ref)))]
    for c in scalars + [v_loc, x_loc]:
        c.start()

    barrier = pltpu.get_barrier_semaphore()
    for d in (tx, ty, sx, sy, pt):
        pl.semaphore_signal(barrier, inc=1, device_id=d, device_id_type=MESH)
    with jax.named_scope("barrier"):
        pl.semaphore_wait(barrier, 5)

    for c in v_copies:
        c.start()
    for j in range(2):
        x_copy(j, 0).start()
    p_copy.start()

    for c in scalars:
        c.wait()
    ell = jnp.full((1, CHUNK), ell_ref[0], F32)
    half = LOG2E / (2.0 * ell * ell)
    top = jnp.log2(jnp.full((1, CHUNK), amp_ref[0], F32))
    CR[0:1, :] = 2.0 * half
    CR[1:2, :] = top
    h1, l1 = half[:, 0:128], top[:, 0:128]

    for s in range(3):
        YR[s] = jnp.zeros((STRIP + ROWS, 32), F32)
    for t in range(5):
        YT[t] = jnp.zeros((32, ROWS), F32)
    kr0[...] = jnp.zeros_like(kr0)
    kr1[...] = jnp.zeros_like(kr1)

    v_loc.wait()
    with jax.named_scope("x_local"):
        x_loc.wait()

    def own_norm(c, _):
        r = pl.ds(pl.multiple_of(c * CHUNK, CHUNK), CHUNK)
        x = X[OWN, r, :].astype(F32)
        n = jnp.broadcast_to(jnp.sum(x * x, axis=1, keepdims=True), (CHUNK, 128)) * h1
        NA[OWN, r, :] = l1 - n
        NB[OWN, :, cols_of(c)] = -jnp.transpose(n)[0:1, :]
        return 0

    with jax.named_scope("own_norm"):
        lax.fori_loop(0, N_CHUNK, own_norm, 0)
    for c in n_copies:
        c.start()

    def send_strip(n, _):
        for j in range(2):
            x_copy(j, n).start()
        return 0

    lax.fori_loop(1, N_STRIP, send_strip, 0)

    def left_norm(s):
        def one(c, _):
            r = pl.ds(pl.multiple_of(c * CHUNK, CHUNK), CHUNK)
            NA[s, r, :] = l1 + jnp.transpose(jnp.broadcast_to(NB[s, :, cols_of(c)], (128, CHUNK)))
            return 0

        lax.fori_loop(0, N_CHUNK, one, 0)

    def gram(tile):
        s, a, t, b, _ = tile
        return lax.dot_general(X[s, rows_of(a), :], X[t, cols_of(b), :], (((1,), (1,)), ((), ())), preferred_element_type=F32)

    def kern(tile, g):
        s, a, t, b, _ = tile
        na = NA[s, rows_of(a), :]
        e = (g * CR[0:1, :] + NB[t, :, cols_of(b)]) + jnp.concatenate([na] * (CHUNK // 128), axis=1)
        return jnp.exp2(jnp.minimum(e, CR[1:2, :])).astype(BF16)

    def apply(tile, k, vec):
        s, a, t, b, to = tile
        YR[s, rows_of(a + 1), :] += lax.dot_general(k, vec[t, :, cols_of(b)], (((1,), (1,)), ((), ())), preferred_element_type=F32)
        YT[to, :, cols_of(b)] += jnp.dot(vec[s, :, rows_of(jnp.maximum(a, 0))], k, preferred_element_type=F32)

    def k_out(seq, place, half):
        kr = (kr0, kr1)[half]
        row = pl.multiple_of(place * STEP_ROWS + half * HALF_ROWS, STRIP)
        return pltpu.make_async_copy(kr.at[seq & 1], k_hbm.at[pl.ds(row, HALF_ROWS)], ko_sem.at[seq & 1, half])

    def half_step(prev, cur, kr_new, d_new, kr_old, d_old):
        gs = [gram(t) for t in cur]
        for u in range(UNITS):
            apply(prev[u], kr_old[d_old, u * STRIP : (u + 1) * STRIP, :], VT)
        for u in range(UNITS):
            kr_new[d_new, u * STRIP : (u + 1) * STRIP, :] = kern(cur[u], gs[u])

    def flat(tiles):
        return tuple(x for t in tiles for x in t)

    def unflat(xs):
        return [tuple(xs[5 * u : 5 * u + 5]) for u in range(UNITS)]

    def begin(seq, before, place):
        @pl.when(seq >= 2)
        def _():
            for h in range(2):
                k_out(seq, place, h).wait()

        @pl.when(seq >= 1)
        def _():
            for h in range(2):
                k_out(seq - 1, before, h).start()

        return seq & 1

    def step_of(state, place, tile):
        seq, before, prev = state[0], state[1], state[2:]
        d = begin(seq, before, place)
        first = [tile(u) for u in range(UNITS)]
        second = [tile(UNITS + u) for u in range(UNITS)]
        half_step(unflat(prev), first, kr0, d, kr1, 1 - d)
        half_step(first, second, kr1, d, kr0, d)
        return (seq + 1, place) + flat(second)

    none = flat([i32(OWN, -1, OWN, 0, TRASH)] * UNITS)

    def own_step(o, state):
        @pl.when(o == N_OWN)
        def _():
            p_copy.wait_recv()
            v_copies[2].wait_recv()
            n_copies[2].wait_recv()

        return step_of(state, table(OWN_PLACE, o), lambda j: own_tile(o, j, core))

    def remote_step(p, state):
        return step_of(state, table(REMOTE_PLACE, p), lambda j: remote_tile(p, j))

    def cross_step(q, state):
        return step_of(state, CROSS_PLACE + q, lambda j: cross_tile(q, j))

    with jax.named_scope("pre"):
        state = lax.fori_loop(0, N_PAIR, own_step, i32(0, 0) + none)

    with jax.named_scope("left_norm"):
        remote(VT.at[1:3], VT.at[1:3], sv_sem, rv_sem.at[0], tx).wait_recv()
        remote(NB.at[1:3], NB.at[1:3], sn_sem, rn_sem.at[0], tx).wait_recv()
        for j in range(2):
            left_norm(1 + j)

    def strip(n, state):
        with jax.named_scope("wait_strip"):
            wait_strip(n)
        with jax.named_scope("strip"):
            state = lax.fori_loop(table(REMOTE_AT, n), table(REMOTE_AT, n + 1), remote_step, state)
            return lax.fori_loop(table(CROSS_AT, n), table(CROSS_AT, n + 1), cross_step, state)

    state = lax.fori_loop(0, N_STRIP - 1, strip, state)

    homes = ((XNB, sx), (YNB, sy), (PAR, pt))

    def part_copy(j, c, send, recv, ss, rs):
        return remote(send.at[j, :, cols_of(c)], recv.at[j, :, cols_of(c)], ss, rs.at[c] if send is SB else rs, homes[j][1])

    def finish(j, c, send):
        s = homes[j][0]
        part = YT[s, :, cols_of(c)]
        if j < 2:
            part = part + jnp.transpose(YR[s, sums_of(c), :])
        send[j, :, cols_of(c)] = part
        if send is SB:
            YT[s, :, cols_of(c)] = jnp.zeros((32, CHUNK), F32)
            if j < 2:
                YR[s, sums_of(c), :] = jnp.zeros((CHUNK, 32), F32)

    def finish_range(lo, hi, send, recv, ss, rs, js=(0, 1)):
        def one(c, _):
            for j in js:
                finish(j, c, send)
            return 0

        for c in range(lo, hi):
            one(c, 0)
            for j in js:
                part_copy(j, c, send, recv, ss, rs).start()

    def send_range(lo, hi, send, recv, ss, rs, js=(0, 1)):
        def go(c, _):
            for j in js:
                part_copy(j, c, send, recv, ss, rs).start()
            return 0

        lax.fori_loop(lo, hi, go, 0)

    def load_kb(d, slot):
        return pltpu.make_async_copy(k_hbm.at[pl.ds(pl.multiple_of(d * 2 * STEP_ROWS, STRIP), 2 * STEP_ROWS)], KB.at[slot], kb_sem.at[slot])

    def load_x(d, slot):
        src = k_hbm.at[pl.ds(pl.multiple_of(d * 2 * STEP_ROWS, STRIP), 2 * STEP_ROWS)]
        return pltpu.make_async_copy(src, X.at[slot, :, 0:CHUNK], kx_sem.at[slot])

    first_in = pltpu.make_async_copy(k_hbm.at[pl.ds(STEP_ROWS, STEP_ROWS)], KB.at[0, pl.ds(STEP_ROWS, STEP_ROWS)], kb_sem.at[0])
    first_in.start()
    for i in range(1, 4):
        load_kb(i, i).start()

    def y_copy(j, c):
        return remote(YV.at[OWN, :, cols_of(c)], YV.at[1 + j, :, cols_of(c)], sy_sem, ryp_sem.at[(c >= 3).astype(jnp.int32) + (c >= 4).astype(jnp.int32)] if j == 2 else ry_sem.at[c], (tx, ty, pt)[j])

    def middle(lo, hi):
        def one(c, _):
            with jax.named_scope("wait_part"):
                three = RB.at[:, :, cols_of(c)]
                remote(three, three, s1_sem, r1_sem.at[c], pt).wait_recv()
            y = YT[OWN, :, cols_of(c)] + jnp.transpose(YR[OWN, sums_of(c), :])
            y = y + RB[0, :, cols_of(c)] + RB[1, :, cols_of(c)] + RB[2, :, cols_of(c)]
            YV[OWN, :, cols_of(c)] = y.astype(BF16)
            YT[OWN, :, cols_of(c)] = jnp.zeros((32, CHUNK), F32)
            YR[OWN, sums_of(c), :] = jnp.zeros((CHUNK, 32), F32)
            for j in range(3):
                y_copy(j, c).start()
            return 0

        lax.fori_loop(lo, hi, one, 0)

    last = last_tiles()
    late = [remote_tile(jnp.int32(23), j) for j in range(6)]

    def rows_in(u, d):
        if d is None:
            return KL, (slice(u * STRIP, (u + 1) * STRIP), slice(None))
        return (kr0, kr1)[u % 6 // UNITS], (d, slice(u % UNITS * STRIP, (u % UNITS + 1) * STRIP), slice(None))

    def grams(tiles, first, d):
        gs = [gram(t) for t in tiles]

        def put():
            for u, (t, g) in enumerate(zip(tiles, gs), first):
                ref, at = rows_in(u, d)
                ref[at] = kern(t, g)

        return put

    def applies(tiles, first, d):
        for u, t in enumerate(tiles, first):
            ref, at = rows_in(u, d)
            apply(t, ref[at], VT)

    kl_out = pltpu.make_async_copy(KL, k_hbm.at[pl.ds(REMOTE_PLACE[23] * STEP_ROWS, STEP_ROWS)], loc_sem.at[0])
    seq, before, due = state[0], state[1], unflat(state[2:])
    d = begin(seq, before, before)
    put = grams(late[0:2], 0, None)
    applies(due, UNITS, 1 - d)
    put()
    applies(late[0:2], 0, None)
    finish_range(0, N_CHUNK, SB, RB, s1_sem, r1_sem, (2,))
    with jax.named_scope("wait_last"):
        wait_strip(N_STRIP - 1)
    with jax.named_scope("last"):
        for c in range(N_CHUNK):
            if c == 3:
                d = begin(seq + 1, jnp.int32(CROSS_PLACE + 10), before)
            put = grams(last[2 * c : 2 * c + 2], 2 * c, d)
            if c > 0:
                applies(last[2 * c - 2 : 2 * c], 2 * c - 2, 1 - d if c == 3 else d)
            put()
            if c > 0:
                finish_range(c - 1, c, SB, RB, s1_sem, r1_sem)
        put = grams(late[2:6], 2, None)
        applies(last[10:12], 10, d)
        put()
        kl_out.start()
        load_x(4, 0).start()
        middle(0, 1)
        applies(late[2:6], 2, None)
        finish_range(5, 6, SB, RB, s1_sem, r1_sem)

    for h in range(2):
        k_out(seq, 0, h).wait()
        k_out(seq + 1, CROSS_PLACE + 11, h).start()

    def use(k, slot, tile):
        for h in range(2):
            use_step(k, slot, h, functools.partial(tile, h))

    def use_step(k, slot, h, tile):
        for j in range(6):
            r = (6 * h + j) * STRIP
            apply(tile(j), k[slot, r : r + STRIP, 0:CHUNK], YV)

    def quad(t, tile, beside=None):
        slot = t & 3
        load_x(0, slot).wait()
        load_kb(0, slot).wait()

        @pl.when(jnp.logical_and(t >= 1, t <= 7))
        def _():
            load_x(10 + 2 * t, (t - 1) & 3).start()

        @pl.when(jnp.logical_and(t >= 1, t <= 6))
        def _():
            load_kb(11 + 2 * t, (t - 1) & 3).start()

        if beside is not None:
            beside()
        use(X, slot, lambda h, j: tile(0, h, j))
        use(KB, slot, lambda h, j: tile(1, h, j))

    def wait_y(lo, hi):
        def one(c, _):
            two = YV.at[1:3, :, cols_of(c)]
            remote(two, two, sy_sem, ry_sem.at[c], tx).wait_recv()
            return 0

        lax.fori_loop(lo, hi, one, 0)

    def wait_y_par(late):
        part = YV.at[PAR, :, pl.ds((0, 3, 4)[late] * CHUNK, (3, 1, 2)[late] * CHUNK)]
        remote(part, part, sy_sem, ryp_sem.at[late], pt).wait_recv()

    with jax.named_scope("middle"):
        middle(1, 2)
    with jax.named_scope("second_own"):
        first_in.wait()
        for j in range(6):
            apply(own_tile(jnp.int32(0), j, core), KB[0, STEP_ROWS + j * STRIP : STEP_ROWS + (j + 1) * STRIP, :], YV)
        load_kb(5, 0).start()
        middle(2, 3)
        load_kb(0, 1).wait()
        use_step(KB, 1, 0, lambda j: own_tile(jnp.int32(1), j, core))
        wait_y_par(0)
        load_kb(0, 2).wait()
        use_step(KB, 2, 0, lambda j: own_tile(jnp.int32(N_OWN), j, core))
        middle(3, 4)
        use_step(KB, 1, 1, lambda j: own_tile(jnp.int32(2), j, core))
        load_x(6, 1).start()
        load_kb(7, 1).start()
        wait_y_par(1)
        use_step(KB, 2, 1, lambda j: own_tile(jnp.int32(N_OWN + 1), j, core))
        load_x(8, 2).start()
        load_kb(9, 2).start()
        middle(4, 5)
        load_kb(0, 3).wait()
        use(KB, 3, lambda h, j: own_tile(jnp.int32(3 + h), j, core))
        load_x(10, 3).start()
        kl_out.wait()
        for h in range(2):
            k_out(seq + 1, 0, h).wait()
        load_kb(11, 3).start()

    def remote_quad(step):
        ps = [step(i) for i in range(4)]
        return lambda d, h, j: remote_tile(ps[2 * d + h], j)

    with jax.named_scope("second_first"):
        wait_y(0, 1)
        quad(jnp.int32(0), remote_quad(jnp.int32))
        middle(5, 6)
    with jax.named_scope("second_cross"):

        def second_cross(t, _):
            with jax.named_scope("wait_y"):
                wait_y(table((1, 1) + Y_NEED[:-1], t), table((1,) + Y_NEED, t))

            def tile(d, h, j):
                cross = cross_tile(4 * (t - 1) + 2 * d + h, j)
                return pick(t < 3, cross, last[6 * h + j]) if d else cross

            quad(t, tile)
            return 0

        lax.fori_loop(1, 4, second_cross, 0)
        wait_y_par(2)

    def second_remote(k, _):
        def beside():
            for j in range(2):
                finish(j, table((4, 4, 3, 2), k), SB2)
                finish(j, table((5, 5, 3, 2), k), SB2)

        with jax.named_scope("second_chunk"):
            quad(4 + k, remote_quad(lambda i: table(REMOTE_ORDER, 4 * k + i)), beside)
        send_range(table((0, 4, 3, 2), k), table((0, 6, 4, 3), k), SB2, RB2, s2_sem, r2_sem)
        return 0

    lax.fori_loop(0, 4, second_remote, 0)

    def finish_strip(n):
        cols = pl.ds(n * STRIP, STRIP)
        for j in range(2):
            s = homes[j][0]
            SB2[j, :, cols] = YT[s, :, cols] + jnp.transpose(YR[s, pl.ds((n + 1) * STRIP, STRIP), :])
        for j in range(2):
            remote(SB2.at[j, :, cols], RB2.at[j, :, cols], s2_sem, r2_sem, homes[j][1]).start()

    with jax.named_scope("second_chunk"):
        finish_range(0, 1, SB2, RB2, s2_sem, r2_sem)
        load_x(0, 0).wait()
        load_kb(0, 0).wait()
        use(X, 0, lambda h, j: remote_tile(jnp.int32(REMOTE_ORDER[16 + h]), j))
        finish_strip(2)
        use(KB, 0, lambda h, j: remote_tile(jnp.int32(REMOTE_ORDER[18 + h]), j))
        finish_strip(3)

    with jax.named_scope("second_par"):
        quad(jnp.int32(9), lambda d, h, j: own_tile(jnp.int32(N_OWN + 2 + 2 * d + h), j, core))
        remote(YT.at[PAR], RB2.at[2], s2_sem, r2_sem, pt).start()

    with jax.named_scope("second_end"):
        load_x(0, 2).wait()
        use(X, 2, lambda h, j: own_tile(jnp.int32(5 + h), j, core))

    with jax.named_scope("sent"):
        p_copy.wait_send()
        for j in range(2):
            remote(x_hbm, X.at[1 + j], sx_sem.at[j], rx_sem.at[0], tx).wait_send()
        for buf, sem in ((VT, sv_sem), (NB, sn_sem), (YV, sy_sem)):
            remote(buf.at[1:4], buf.at[1:4], sem, rx_sem.at[0], tx).wait_send()
        remote(SB, RB, s1_sem, rx_sem.at[0], tx).wait_send()

    def final(c, _):
        out_ref[:, cols_of(c)] = YT[OWN, :, cols_of(c)] + jnp.transpose(YR[OWN, sums_of(c), :])
        return 0

    with jax.named_scope("final"):
        for c in range(N_CHUNK):
            final(c, 0)
        all_sums = remote(SB2, RB2, s2_sem, r2_sem, pt)
        all_sums.wait_send()
        all_sums.wait_recv()


def solution(mesh):
    def local_program(x_loc, v_loc, length_scale, out_scale):
        dma = pltpu.SemaphoreType.DMA
        hbm = pl.BlockSpec(memory_space=pltpu.HBM)
        vmem = pl.BlockSpec(memory_space=pltpu.VMEM)
        own, parts, _ = pl.pallas_call(
            body,
            out_shape=(
                pltpu.VMEM((32, ROWS), F32),
                pltpu.VMEM((3, 32, ROWS), F32),
                jax.ShapeDtypeStruct((N_PLACE * STEP_ROWS, CHUNK), BF16),
            ),
            in_specs=[hbm, hbm, hbm, hbm],
            out_specs=(vmem, vmem, hbm),
            scratch_shapes=[
                pltpu.VMEM((4, ROWS, 768), BF16),
                pltpu.VMEM((4, 32, ROWS), BF16),
                pltpu.VMEM((4, 32, ROWS), BF16),
                pltpu.VMEM((3, ROWS, 128), F32),
                pltpu.VMEM((4, 1, ROWS), F32),
                pltpu.VMEM((8, CHUNK), F32),
                pltpu.VMEM((3, STRIP + ROWS, 32), F32),
                pltpu.VMEM((5, 32, ROWS), F32),
                pltpu.VMEM((3, 32, ROWS), F32),
                pltpu.VMEM((3, 32, ROWS), F32),
                pltpu.VMEM((3, 32, ROWS), F32),
                pltpu.VMEM((2, HALF_ROWS, CHUNK), BF16),
                pltpu.VMEM((2, HALF_ROWS, CHUNK), BF16),
                pltpu.VMEM((STEP_ROWS, CHUNK), BF16),
                pltpu.VMEM((4, 2 * STEP_ROWS, CHUNK), BF16),
                pltpu.SMEM((1,), F32), pltpu.SMEM((1,), F32),
                dma((2,)), dma((N_STRIP,)), dma, dma((2,)), dma, dma((2,)), dma, dma,
                dma((4,)), dma((2, 2)), dma((4,)), dma((4,)),
                dma, dma((N_CHUNK,)), dma, dma((N_CHUNK,)), dma((3,)), dma, dma,
            ],
            compiler_params=pltpu.CompilerParams(collective_id=0, has_side_effects=True, vmem_limit_bytes=58 * 2**20),
            name="products",
        )(x_loc, v_loc.T, length_scale, out_scale)
        return (own + parts[0] + parts[1] + parts[2]).T

    row_spec = P(("task", "row"), None)
    return jax.shard_map(local_program, mesh=mesh, in_specs=(row_spec, row_spec, P("task"), P("task")), out_specs=row_spec, check_vma=False)
```

```python
import functools

import jax
import jax.numpy as jnp
from jax import lax
from jax.experimental import pallas as pl
from jax.experimental.pallas import tpu as pltpu
from jax.sharding import PartitionSpec as P

MESH = pl.DeviceIdType.MESH
F32, BF16 = jnp.float32, jnp.bfloat16
LOG2E = 1.4426950408889634

ROWS = 3072
STRIP = 256
CHUNK = 512
N_STRIP = ROWS // STRIP
N_CHUNK = ROWS // CHUNK
UNITS = 3
OWN, XNB, YNB, PAR, TRASH = 0, 1, 2, 3, 4

N_OWN, N_PAIR = 7, 13
REMOTE_AT = (0, 0, 7, 7, 13, 13, 18, 18, 21, 21, 23, 23)
REMOTE_TILE = (0, 44, 80, 108, 128, 140)
CROSS_AT = (0, 0, 0, 0, 1, 2, 3, 4, 5, 6, 8, 10)
CROSS_TILE = (0, 0, 2, 4, 8, 12, 18, 24, 32, 40, 50, 60)
OWN_PLACE = (1, 2, 3, 6, 7, 48, 49, 4, 5, 44, 45, 46, 47)
REMOTE_ORDER = (20, 21, 22, 23, 16, 17, 18, 19, 10, 13, 14, 15, 4, 5, 6, 7, 8, 9, 11, 12)
REMOTE_PLACE = tuple(8 + p if p < 4 else 24 + REMOTE_ORDER.index(p) for p in range(24))
CROSS_PLACE = 12
N_PLACE = 50
STEP_ROWS = 6 * STRIP
HALF_ROWS = UNITS * STRIP
Y_NEED = (4, 5, 6)


def table(values, n):
    out = jnp.int32(values[0])
    for i in range(1, len(values)):
        if values[i] != values[i - 1]:
            out = out + (values[i] - values[i - 1]) * (n >= i).astype(jnp.int32)
    return out


def rank(bounds, x):
    out = jnp.int32(0)
    for b in bounds:
        out = out + (x >= b).astype(jnp.int32)
    return out


def pick(cond, a, b):
    return tuple(jnp.where(cond, x, y) for x, y in zip(a, b))


def i32(*xs):
    return tuple(jnp.int32(x) for x in xs)


def own_tile(o, j, core):
    p = 3 * o + j // 2
    c = rank((1, 3, 6, 10, 15), p)
    i = p - ((c * (c + 1)) >> 1)
    own = (jnp.int32(OWN), 2 * i + j % 2, jnp.int32(OWN), c, jnp.where(i == c, TRASH, OWN))
    p = 3 * (o - N_OWN) + j // 2
    c = 1 + rank((1, 3, 6, 10), p)
    i = p - ((c * (c - 1)) >> 1)
    same = core + 2 * (j // 2)
    i, c = pick(p < 15, (i, c), (same, same))
    par = (jnp.int32(OWN), 2 * i + j % 2, jnp.int32(PAR), c, jnp.int32(PAR))
    return pick(o < N_OWN, own, par)


def remote_tile(p, j):
    g = 6 * p + j
    d, first = jnp.int32(0), jnp.int32(0)
    for i in range(1, N_CHUNK):
        d, first = pick(g >= REMOTE_TILE[i], (i, REMOTE_TILE[i]), (d, first))
    r = g - first
    rest = r - (22 - 4 * d)
    k, side, odd = pick(rest >= 0, (rest >> 1, r & 1, 1), (r >> 1, r & 1, 0))
    k, side, odd = pick(d == 0, (r >> 2, (r >> 1) & 1, r & 1), (k, side, odd))
    t = jnp.where((k & 1) == (k > 0).astype(jnp.int32), OWN, PAR)
    return (1 + side, 2 * d + odd, t, d + ((k + 1) >> 1), t)


def cross_tile(q, j):
    g = 6 * q + j
    n = 1 + rank(CROSS_TILE[2:11], g)
    r = g - table(CROSS_TILE, n)
    m = n >> 1
    t = pick(r < m, (jnp.int32(XNB), n, jnp.int32(YNB), r, jnp.int32(YNB)), (jnp.int32(YNB), n, jnp.int32(XNB), r - m, jnp.int32(XNB)))
    return pick(r < 2 * m, t, (jnp.int32(XNB), n - 1 + (r - 2 * m), jnp.int32(YNB), m, jnp.int32(YNB)))


def last_tiles():
    n = N_STRIP - 1
    tiles = [t for c in range(N_CHUNK - 1) for t in ((YNB, n, XNB, c, XNB), (XNB, n, YNB, c, YNB))]
    tiles += [(XNB, n - 1, YNB, N_CHUNK - 1, YNB), (XNB, n, YNB, N_CHUNK - 1, YNB)]
    return [i32(*t) for t in tiles]


def span(start, size, unit):
    return pl.ds(start if isinstance(start, int) else pl.multiple_of(start, unit), size)


def rows_of(a):
    return span(a * STRIP, STRIP, STRIP)


def sums_of(c):
    return span(STRIP + c * CHUNK, CHUNK, STRIP)


def cols_of(b):
    return span(b * CHUNK, CHUNK, CHUNK)


def body(
    x_hbm, v_hbm, ell_hbm, amp_hbm, out_ref, RB2, k_hbm,
    X, VT, YV, NA, NB, CR, YR, YT, SB, RB, SB2, kr0, kr1, KL, KB, ell_ref, amp_ref,
    sx_sem, rx_sem, sv_sem, rv_sem, sn_sem, rn_sem, sp_sem, rp_sem, loc_sem, ko_sem, kb_sem, kx_sem,
    s1_sem, r1_sem, sy_sem, ry_sem, ryp_sem, s2_sem, r2_sem,
):
    me = lax.axis_index("row")
    core, cx, cy = me % 2, (me // 2) % 2, me // 4

    def dev(px, py, pc):
        return {"row": (py * 2 + px) * 2 + pc}

    tx = dev(1 - cx, cy, (core + 1 + cx) % 2)
    ty = dev(cx, 1 - cy, (core + 1 + cx + cy) % 2)
    sx = dev(1 - cx, cy, (core + cx) % 2)
    sy = dev(cx, 1 - cy, (core + cx + cy) % 2)
    pt = dev(cx, cy, 1 - core)

    def remote(src, dst, ss, rs, to):
        return pltpu.make_async_remote_copy(src_ref=src, dst_ref=dst, send_sem=ss, recv_sem=rs, device_id=to, device_id_type=MESH)

    def x_copy(j, n):
        return remote(x_hbm.at[rows_of(n)], X.at[1 + j, rows_of(n)], sx_sem.at[j], rx_sem.at[n], (tx, ty)[j])

    def wait_strip(n):
        two = X.at[1:3, rows_of(n)]
        remote(two, two, sx_sem.at[0], rx_sem.at[n], tx).wait_recv()

    p_copy = remote(x_hbm, X.at[PAR], sp_sem, rp_sem, pt)
    v_copies = [remote(v_hbm, VT.at[1 + j], sv_sem, rv_sem.at[j // 2], d) for j, d in enumerate((tx, ty, pt))]
    n_copies = [remote(NB.at[OWN], NB.at[1 + j], sn_sem, rn_sem.at[j // 2], d) for j, d in enumerate((tx, ty, pt))]

    x_loc = pltpu.make_async_copy(x_hbm, X.at[OWN], loc_sem.at[0])
    v_loc = pltpu.make_async_copy(v_hbm, VT.at[OWN], loc_sem.at[1])
    scalars = [pltpu.make_async_copy(src, dst, loc_sem.at[2 + i]) for i, (src, dst) in enumerate(((ell_hbm, ell_ref), (amp_hbm, amp_ref)))]
    for c in scalars + [v_loc, x_loc]:
        c.start()

    barrier = pltpu.get_barrier_semaphore()
    for d in (tx, ty, sx, sy, pt):
        pl.semaphore_signal(barrier, inc=1, device_id=d, device_id_type=MESH)
    with jax.named_scope("barrier"):
        pl.semaphore_wait(barrier, 5)

    for c in v_copies:
        c.start()
    for j in range(2):
        x_copy(j, 0).start()
    p_copy.start()

    for c in scalars:
        c.wait()
    ell = jnp.full((1, CHUNK), ell_ref[0], F32)
    half = LOG2E / (2.0 * ell * ell)
    top = jnp.log2(jnp.full((1, CHUNK), amp_ref[0], F32))
    CR[0:1, :] = 2.0 * half
    CR[1:2, :] = top
    h1, l1 = half[:, 0:128], top[:, 0:128]

    for s in range(3):
        YR[s] = jnp.zeros((STRIP + ROWS, 32), F32)
    for t in range(5):
        YT[t] = jnp.zeros((32, ROWS), F32)
    kr0[...] = jnp.zeros_like(kr0)
    kr1[...] = jnp.zeros_like(kr1)

    v_loc.wait()
    with jax.named_scope("x_local"):
        x_loc.wait()

    def own_norm(c, _):
        r = pl.ds(pl.multiple_of(c * CHUNK, CHUNK), CHUNK)
        x = X[OWN, r, :].astype(F32)
        n = jnp.broadcast_to(jnp.sum(x * x, axis=1, keepdims=True), (CHUNK, 128)) * h1
        NA[OWN, r, :] = l1 - n
        NB[OWN, :, cols_of(c)] = -jnp.transpose(n)[0:1, :]
        return 0

    with jax.named_scope("own_norm"):
        lax.fori_loop(0, N_CHUNK, own_norm, 0)
    for c in n_copies:
        c.start()

    def send_strip(n, _):
        for j in range(2):
            x_copy(j, n).start()
        return 0

    lax.fori_loop(1, N_STRIP, send_strip, 0)

    def left_norm(s):
        def one(c, _):
            r = pl.ds(pl.multiple_of(c * CHUNK, CHUNK), CHUNK)
            NA[s, r, :] = l1 + jnp.transpose(jnp.broadcast_to(NB[s, :, cols_of(c)], (128, CHUNK)))
            return 0

        lax.fori_loop(0, N_CHUNK, one, 0)

    def gram(tile):
        s, a, t, b, _ = tile
        return lax.dot_general(X[s, rows_of(a), :], X[t, cols_of(b), :], (((1,), (1,)), ((), ())), preferred_element_type=F32)

    def kern(tile, g):
        s, a, t, b, _ = tile
        na = NA[s, rows_of(a), :]
        e = (g * CR[0:1, :] + NB[t, :, cols_of(b)]) + jnp.concatenate([na] * (CHUNK // 128), axis=1)
        return jnp.exp2(jnp.minimum(e, CR[1:2, :])).astype(BF16)

    def apply(tile, k, vec):
        s, a, t, b, to = tile
        YR[s, rows_of(a + 1), :] += lax.dot_general(k, vec[t, :, cols_of(b)], (((1,), (1,)), ((), ())), preferred_element_type=F32)
        YT[to, :, cols_of(b)] += jnp.dot(vec[s, :, rows_of(jnp.maximum(a, 0))], k, preferred_element_type=F32)

    def k_out(seq, place, half):
        kr = (kr0, kr1)[half]
        row = pl.multiple_of(place * STEP_ROWS + half * HALF_ROWS, STRIP)
        return pltpu.make_async_copy(kr.at[seq & 1], k_hbm.at[pl.ds(row, HALF_ROWS)], ko_sem.at[seq & 1, half])

    def half_step(prev, cur, kr_new, d_new, kr_old, d_old):
        gs = [gram(t) for t in cur]
        for u in range(UNITS):
            apply(prev[u], kr_old[d_old, u * STRIP : (u + 1) * STRIP, :], VT)
        for u in range(UNITS):
            kr_new[d_new, u * STRIP : (u + 1) * STRIP, :] = kern(cur[u], gs[u])

    def flat(tiles):
        return tuple(x for t in tiles for x in t)

    def unflat(xs):
        return [tuple(xs[5 * u : 5 * u + 5]) for u in range(UNITS)]

    def begin(seq, before, place):
        @pl.when(seq >= 2)
        def _():
            for h in range(2):
                k_out(seq, place, h).wait()

        @pl.when(seq >= 1)
        def _():
            for h in range(2):
                k_out(seq - 1, before, h).start()

        return seq & 1

    def step_of(state, place, tile):
        seq, before, prev = state[0], state[1], state[2:]
        d = begin(seq, before, place)
        first = [tile(u) for u in range(UNITS)]
        second = [tile(UNITS + u) for u in range(UNITS)]
        half_step(unflat(prev), first, kr0, d, kr1, 1 - d)
        half_step(first, second, kr1, d, kr0, d)
        return (seq + 1, place) + flat(second)

    none = flat([i32(OWN, -1, OWN, 0, TRASH)] * UNITS)

    def own_step(o, state):
        @pl.when(o == N_OWN)
        def _():
            p_copy.wait_recv()
            v_copies[2].wait_recv()
            n_copies[2].wait_recv()

        return step_of(state, table(OWN_PLACE, o), lambda j: own_tile(o, j, core))

    def remote_step(p, state):
        return step_of(state, table(REMOTE_PLACE, p), lambda j: remote_tile(p, j))

    def cross_step(q, state):
        return step_of(state, CROSS_PLACE + q, lambda j: cross_tile(q, j))

    with jax.named_scope("pre"):
        state = lax.fori_loop(0, N_PAIR, own_step, i32(0, 0) + none)

    with jax.named_scope("left_norm"):
        remote(VT.at[1:3], VT.at[1:3], sv_sem, rv_sem.at[0], tx).wait_recv()
        remote(NB.at[1:3], NB.at[1:3], sn_sem, rn_sem.at[0], tx).wait_recv()
        for j in range(2):
            left_norm(1 + j)

    def strip(n, state):
        with jax.named_scope("wait_strip"):
            wait_strip(n)
        with jax.named_scope("strip"):
            state = lax.fori_loop(table(REMOTE_AT, n), table(REMOTE_AT, n + 1), remote_step, state)
            return lax.fori_loop(table(CROSS_AT, n), table(CROSS_AT, n + 1), cross_step, state)

    state = lax.fori_loop(0, N_STRIP - 1, strip, state)

    homes = ((XNB, sx), (YNB, sy), (PAR, pt))

    def part_copy(j, c, send, recv, ss, rs):
        return remote(send.at[j, :, cols_of(c)], recv.at[j, :, cols_of(c)], ss, rs.at[c] if send is SB else rs, homes[j][1])

    def finish(j, c, send):
        s = homes[j][0]
        part = YT[s, :, cols_of(c)]
        if j < 2:
            part = part + jnp.transpose(YR[s, sums_of(c), :])
        send[j, :, cols_of(c)] = part
        if send is SB:
            YT[s, :, cols_of(c)] = jnp.zeros((32, CHUNK), F32)
            if j < 2:
                YR[s, sums_of(c), :] = jnp.zeros((CHUNK, 32), F32)

    def finish_range(lo, hi, send, recv, ss, rs, js=(0, 1)):
        def one(c, _):
            for j in js:
                finish(j, c, send)
            return 0

        for c in range(lo, hi):
            one(c, 0)
            for j in js:
                part_copy(j, c, send, recv, ss, rs).start()

    def send_range(lo, hi, send, recv, ss, rs, js=(0, 1)):
        def go(c, _):
            for j in js:
                part_copy(j, c, send, recv, ss, rs).start()
            return 0

        lax.fori_loop(lo, hi, go, 0)

    def load_kb(d, slot):
        return pltpu.make_async_copy(k_hbm.at[pl.ds(pl.multiple_of(d * 2 * STEP_ROWS, STRIP), 2 * STEP_ROWS)], KB.at[slot], kb_sem.at[slot])

    def load_x(d, slot):
        src = k_hbm.at[pl.ds(pl.multiple_of(d * 2 * STEP_ROWS, STRIP), 2 * STEP_ROWS)]
        return pltpu.make_async_copy(src, X.at[slot, :, 0:CHUNK], kx_sem.at[slot])

    first_in = pltpu.make_async_copy(k_hbm.at[pl.ds(STEP_ROWS, STEP_ROWS)], KB.at[0, pl.ds(STEP_ROWS, STEP_ROWS)], kb_sem.at[0])
    first_in.start()
    for i in range(1, 4):
        load_kb(i, i).start()

    def y_copy(j, c):
        return remote(YV.at[OWN, :, cols_of(c)], YV.at[1 + j, :, cols_of(c)], sy_sem, ryp_sem.at[(c >= 3).astype(jnp.int32) + (c >= 4).astype(jnp.int32)] if j == 2 else ry_sem.at[c], (tx, ty, pt)[j])

    def middle(lo, hi):
        def one(c, _):
            with jax.named_scope("wait_part"):
                three = RB.at[:, :, cols_of(c)]
                remote(three, three, s1_sem, r1_sem.at[c], pt).wait_recv()
            y = YT[OWN, :, cols_of(c)] + jnp.transpose(YR[OWN, sums_of(c), :])
            y = y + RB[0, :, cols_of(c)] + RB[1, :, cols_of(c)] + RB[2, :, cols_of(c)]
            YV[OWN, :, cols_of(c)] = y.astype(BF16)
            YT[OWN, :, cols_of(c)] = jnp.zeros((32, CHUNK), F32)
            YR[OWN, sums_of(c), :] = jnp.zeros((CHUNK, 32), F32)
            for j in range(3):
                y_copy(j, c).start()
            return 0

        lax.fori_loop(lo, hi, one, 0)

    last = last_tiles()
    late = [remote_tile(jnp.int32(23), j) for j in range(6)]

    def rows_in(u, d):
        if d is None:
            return KL, (slice(u * STRIP, (u + 1) * STRIP), slice(None))
        return (kr0, kr1)[u % 6 // UNITS], (d, slice(u % UNITS * STRIP, (u % UNITS + 1) * STRIP), slice(None))

    def grams(tiles, first, d):
        gs = [gram(t) for t in tiles]

        def put():
            for u, (t, g) in enumerate(zip(tiles, gs), first):
                ref, at = rows_in(u, d)
                ref[at] = kern(t, g)

        return put

    def applies(tiles, first, d):
        for u, t in enumerate(tiles, first):
            ref, at = rows_in(u, d)
            apply(t, ref[at], VT)

    kl_out = pltpu.make_async_copy(KL, k_hbm.at[pl.ds(REMOTE_PLACE[23] * STEP_ROWS, STEP_ROWS)], loc_sem.at[0])
    seq, before, due = state[0], state[1], unflat(state[2:])
    d = begin(seq, before, before)
    put = grams(late[0:2], 0, None)
    applies(due, UNITS, 1 - d)
    put()
    applies(late[0:2], 0, None)
    finish_range(0, N_CHUNK, SB, RB, s1_sem, r1_sem, (2,))
    with jax.named_scope("wait_last"):
        wait_strip(N_STRIP - 1)
    with jax.named_scope("last"):
        for c in range(N_CHUNK):
            if c == 3:
                d = begin(seq + 1, jnp.int32(CROSS_PLACE + 10), before)
            put = grams(last[2 * c : 2 * c + 2], 2 * c, d)
            if c > 0:
                applies(last[2 * c - 2 : 2 * c], 2 * c - 2, 1 - d if c == 3 else d)
            put()
            if c > 0:
                finish_range(c - 1, c, SB, RB, s1_sem, r1_sem)
        put = grams(late[2:6], 2, None)
        applies(last[10:12], 10, d)
        put()
        kl_out.start()
        load_x(4, 0).start()
        middle(0, 1)
        applies(late[2:6], 2, None)
        finish_range(5, 6, SB, RB, s1_sem, r1_sem)

    for h in range(2):
        k_out(seq, 0, h).wait()
        k_out(seq + 1, CROSS_PLACE + 11, h).start()

    def use(k, slot, tile):
        for h in range(2):
            use_step(k, slot, h, functools.partial(tile, h))

    def use_step(k, slot, h, tile):
        for j in range(6):
            r = (6 * h + j) * STRIP
            apply(tile(j), k[slot, r : r + STRIP, 0:CHUNK], YV)

    def quad(t, tile, beside=None):
        slot = t & 3
        load_x(0, slot).wait()
        load_kb(0, slot).wait()

        t = jnp.int32(t)

        @pl.when(jnp.logical_and(t >= 1, t <= 7))
        def _():
            load_x(10 + 2 * t, (t - 1) & 3).start()

        @pl.when(jnp.logical_and(t >= 1, t <= 6))
        def _():
            load_kb(11 + 2 * t, (t - 1) & 3).start()

        if beside is not None:
            beside()
        use(X, slot, lambda h, j: tile(0, h, j))
        use(KB, slot, lambda h, j: tile(1, h, j))

    def wait_y(lo, hi):
        def one(c, _):
            two = YV.at[1:3, :, cols_of(c)]
            remote(two, two, sy_sem, ry_sem.at[c], tx).wait_recv()
            return 0

        lax.fori_loop(lo, hi, one, 0)

    def wait_y_par(late):
        part = YV.at[PAR, :, pl.ds((0, 3, 4)[late] * CHUNK, (3, 1, 2)[late] * CHUNK)]
        remote(part, part, sy_sem, ryp_sem.at[late], pt).wait_recv()

    with jax.named_scope("middle"):
        middle(1, 2)
    with jax.named_scope("second_own"):
        first_in.wait()
        for j in range(6):
            apply(own_tile(jnp.int32(0), j, core), KB[0, STEP_ROWS + j * STRIP : STEP_ROWS + (j + 1) * STRIP, :], YV)
        load_kb(5, 0).start()
        middle(2, 3)
        load_kb(0, 1).wait()
        use_step(KB, 1, 0, lambda j: own_tile(jnp.int32(1), j, core))
        wait_y_par(0)
        load_kb(0, 2).wait()
        use_step(KB, 2, 0, lambda j: own_tile(jnp.int32(N_OWN), j, core))
        middle(3, 4)
        use_step(KB, 1, 1, lambda j: own_tile(jnp.int32(2), j, core))
        load_x(6, 1).start()
        load_kb(7, 1).start()
        wait_y_par(1)
        use_step(KB, 2, 1, lambda j: own_tile(jnp.int32(N_OWN + 1), j, core))
        load_x(8, 2).start()
        load_kb(9, 2).start()
        middle(4, 5)
        load_kb(0, 3).wait()
        use(KB, 3, lambda h, j: own_tile(jnp.int32(3 + h), j, core))
        load_x(10, 3).start()
        kl_out.wait()
        for h in range(2):
            k_out(seq + 1, 0, h).wait()
        load_kb(11, 3).start()

    def remote_quad(step):
        ps = [step(i) for i in range(4)]
        return lambda d, h, j: remote_tile(ps[2 * d + h], j)

    with jax.named_scope("second_first"):
        wait_y(0, 1)
        quad(jnp.int32(0), remote_quad(jnp.int32))
        middle(5, 6)
    with jax.named_scope("second_cross"):

        def second_cross(t, _):
            with jax.named_scope("wait_y"):
                wait_y(table((1, 1) + Y_NEED[:-1], t), table((1,) + Y_NEED, t))

            def tile(d, h, j):
                cross = cross_tile(4 * (t - 1) + 2 * d + h, j)
                return pick(t < 3, cross, last[6 * h + j]) if d else cross

            quad(t, tile)
            return 0

        lax.fori_loop(1, 4, second_cross, 0)
        wait_y_par(2)

    for k, done in enumerate(((), (4, 5), (3,), (2,))):
        with jax.named_scope("second_chunk"):
            ps = REMOTE_ORDER[4 * k : 4 * k + 4]
            quad(4 + k, remote_quad(lambda i: jnp.int32(ps[i])), lambda: [finish(j, c, SB2) for c in done for j in range(2)])
        for c in done:
            send_range(c, c + 1, SB2, RB2, s2_sem, r2_sem)

    def finish_strip(n):
        cols = pl.ds(n * STRIP, STRIP)
        for j in range(2):
            s = homes[j][0]
            SB2[j, :, cols] = YT[s, :, cols] + jnp.transpose(YR[s, pl.ds((n + 1) * STRIP, STRIP), :])
        for j in range(2):
            remote(SB2.at[j, :, cols], RB2.at[j, :, cols], s2_sem, r2_sem, homes[j][1]).start()

    with jax.named_scope("second_chunk"):
        finish_range(0, 1, SB2, RB2, s2_sem, r2_sem)
        load_x(0, 0).wait()
        load_kb(0, 0).wait()
        use(X, 0, lambda h, j: remote_tile(jnp.int32(REMOTE_ORDER[16 + h]), j))
        finish_strip(2)
        use(KB, 0, lambda h, j: remote_tile(jnp.int32(REMOTE_ORDER[18 + h]), j))
        finish_strip(3)

    with jax.named_scope("second_par"):
        quad(jnp.int32(9), lambda d, h, j: own_tile(jnp.int32(N_OWN + 2 + 2 * d + h), j, core))
        remote(YT.at[PAR], RB2.at[2], s2_sem, r2_sem, pt).start()

    with jax.named_scope("second_end"):
        load_x(0, 2).wait()
        use(X, 2, lambda h, j: own_tile(jnp.int32(5 + h), j, core))

    with jax.named_scope("sent"):
        p_copy.wait_send()
        for j in range(2):
            remote(x_hbm, X.at[1 + j], sx_sem.at[j], rx_sem.at[0], tx).wait_send()
        for buf, sem in ((VT, sv_sem), (NB, sn_sem), (YV, sy_sem)):
            remote(buf.at[1:4], buf.at[1:4], sem, rx_sem.at[0], tx).wait_send()
        remote(SB, RB, s1_sem, rx_sem.at[0], tx).wait_send()

    def final(c, _):
        out_ref[:, cols_of(c)] = YT[OWN, :, cols_of(c)] + jnp.transpose(YR[OWN, sums_of(c), :])
        return 0

    with jax.named_scope("final"):
        for c in range(N_CHUNK):
            final(c, 0)
        all_sums = remote(SB2, RB2, s2_sem, r2_sem, pt)
        all_sums.wait_send()
        all_sums.wait_recv()


def solution(mesh):
    def local_program(x_loc, v_loc, length_scale, out_scale):
        dma = pltpu.SemaphoreType.DMA
        hbm = pl.BlockSpec(memory_space=pltpu.HBM)
        vmem = pl.BlockSpec(memory_space=pltpu.VMEM)
        own, parts, _ = pl.pallas_call(
            body,
            out_shape=(
                pltpu.VMEM((32, ROWS), F32),
                pltpu.VMEM((3, 32, ROWS), F32),
                jax.ShapeDtypeStruct((N_PLACE * STEP_ROWS, CHUNK), BF16),
            ),
            in_specs=[hbm, hbm, hbm, hbm],
            out_specs=(vmem, vmem, hbm),
            scratch_shapes=[
                pltpu.VMEM((4, ROWS, 768), BF16),
                pltpu.VMEM((4, 32, ROWS), BF16),
                pltpu.VMEM((4, 32, ROWS), BF16),
                pltpu.VMEM((3, ROWS, 128), F32),
                pltpu.VMEM((4, 1, ROWS), F32),
                pltpu.VMEM((8, CHUNK), F32),
                pltpu.VMEM((3, STRIP + ROWS, 32), F32),
                pltpu.VMEM((5, 32, ROWS), F32),
                pltpu.VMEM((3, 32, ROWS), F32),
                pltpu.VMEM((3, 32, ROWS), F32),
                pltpu.VMEM((3, 32, ROWS), F32),
                pltpu.VMEM((2, HALF_ROWS, CHUNK), BF16),
                pltpu.VMEM((2, HALF_ROWS, CHUNK), BF16),
                pltpu.VMEM((STEP_ROWS, CHUNK), BF16),
                pltpu.VMEM((4, 2 * STEP_ROWS, CHUNK), BF16),
                pltpu.SMEM((1,), F32), pltpu.SMEM((1,), F32),
                dma((2,)), dma((N_STRIP,)), dma, dma((2,)), dma, dma((2,)), dma, dma,
                dma((4,)), dma((2, 2)), dma((4,)), dma((4,)),
                dma, dma((N_CHUNK,)), dma, dma((N_CHUNK,)), dma((3,)), dma, dma,
            ],
            compiler_params=pltpu.CompilerParams(collective_id=0, has_side_effects=True, vmem_limit_bytes=58 * 2**20),
            name="products",
        )(x_loc, v_loc.T, length_scale, out_scale)
        return (own + parts[0] + parts[1] + parts[2]).T

    row_spec = P(("task", "row"), None)
    return jax.shard_map(local_program, mesh=mesh, in_specs=(row_spec, row_spec, P("task"), P("task")), out_specs=row_spec, check_vma=False)
```

```python
import functools

import jax
import jax.numpy as jnp
from jax import lax
from jax.experimental import pallas as pl
from jax.experimental.pallas import tpu as pltpu
from jax.sharding import PartitionSpec as P

MESH = pl.DeviceIdType.MESH
F32, BF16 = jnp.float32, jnp.bfloat16
LOG2E = 1.4426950408889634

ROWS = 3072
STRIP = 256
CHUNK = 512
N_STRIP = ROWS // STRIP
N_CHUNK = ROWS // CHUNK
UNITS = 3
OWN, XNB, YNB, PAR, TRASH = 0, 1, 2, 3, 4

N_OWN, N_PAIR = 7, 13
REMOTE_AT = (0, 7, 13, 18, 21, 21, 23, 23)
REMOTE_TILE = (0, 44, 80, 108, 128, 140)
CROSS_AT = (0, 0, 1, 3, 5, 6, 8, 10)
CROSS_TILE = (0, 0, 2, 4, 8, 12, 18, 24, 32, 40, 50, 60)
OWN_PLACE = (1, 2, 3, 6, 7, 48, 49, 4, 5, 44, 45, 46, 47)
REMOTE_ORDER = (20, 21, 22, 23, 16, 17, 18, 19, 10, 13, 14, 15, 8, 9, 11, 12)
REMOTE_PLACE = tuple(8 + p if p < 8 else 28 + REMOTE_ORDER.index(p) for p in range(24))
CROSS_PLACE = 16
N_PLACE = 50
STEP_ROWS = 6 * STRIP
HALF_ROWS = UNITS * STRIP
Y_NEED = (4, 5, 6)


def table(values, n):
    out = jnp.int32(values[0])
    for i in range(1, len(values)):
        if values[i] != values[i - 1]:
            out = out + (values[i] - values[i - 1]) * (n >= i).astype(jnp.int32)
    return out


def rank(bounds, x):
    out = jnp.int32(0)
    for b in bounds:
        out = out + (x >= b).astype(jnp.int32)
    return out


def pick(cond, a, b):
    return tuple(jnp.where(cond, x, y) for x, y in zip(a, b))


def i32(*xs):
    return tuple(jnp.int32(x) for x in xs)


def own_tile(o, j, core):
    p = 3 * o + j // 2
    c = rank((1, 3, 6, 10, 15), p)
    i = p - ((c * (c + 1)) >> 1)
    own = (jnp.int32(OWN), 2 * i + j % 2, jnp.int32(OWN), c, jnp.where(i == c, TRASH, OWN))
    p = 3 * (o - N_OWN) + j // 2
    c = 1 + rank((1, 3, 6, 10), p)
    i = p - ((c * (c - 1)) >> 1)
    same = core + 2 * (j // 2)
    i, c = pick(p < 15, (i, c), (same, same))
    par = (jnp.int32(OWN), 2 * i + j % 2, jnp.int32(PAR), c, jnp.int32(PAR))
    return pick(o < N_OWN, own, par)


def remote_tile(p, j):
    g = 6 * p + j
    d, first = jnp.int32(0), jnp.int32(0)
    for i in range(1, N_CHUNK):
        d, first = pick(g >= REMOTE_TILE[i], (i, REMOTE_TILE[i]), (d, first))
    r = g - first
    rest = r - (22 - 4 * d)
    k, side, odd = pick(rest >= 0, (rest >> 1, r & 1, 1), (r >> 1, r & 1, 0))
    k, side, odd = pick(d == 0, (r >> 2, (r >> 1) & 1, r & 1), (k, side, odd))
    t = jnp.where((k & 1) == (k > 0).astype(jnp.int32), OWN, PAR)
    return (1 + side, 2 * d + odd, t, d + ((k + 1) >> 1), t)


def cross_tile(q, j):
    g = 6 * q + j
    n = 1 + rank(CROSS_TILE[2:11], g)
    r = g - table(CROSS_TILE, n)
    m = n >> 1
    t = pick(r < m, (jnp.int32(XNB), n, jnp.int32(YNB), r, jnp.int32(YNB)), (jnp.int32(YNB), n, jnp.int32(XNB), r - m, jnp.int32(XNB)))
    return pick(r < 2 * m, t, (jnp.int32(XNB), n - 1 + (r - 2 * m), jnp.int32(YNB), m, jnp.int32(YNB)))


def last_tiles():
    n = N_STRIP - 1
    tiles = [t for c in range(N_CHUNK - 1) for t in ((YNB, n, XNB, c, XNB), (XNB, n, YNB, c, YNB))]
    tiles += [(XNB, n - 1, YNB, N_CHUNK - 1, YNB), (XNB, n, YNB, N_CHUNK - 1, YNB)]
    return [i32(*t) for t in tiles]


def span(start, size, unit):
    return pl.ds(start if isinstance(start, int) else pl.multiple_of(start, unit), size)


def rows_of(a):
    return span(a * STRIP, STRIP, STRIP)


def sums_of(c):
    return span(STRIP + c * CHUNK, CHUNK, STRIP)


def cols_of(b):
    return span(b * CHUNK, CHUNK, CHUNK)


def body(
    x_hbm, v_hbm, ell_ref, amp_ref, out_ref, RB2, k_hbm,
    X, VT, YV, NA, NB, CR, YR, YT, SB, RB, SB2, kr0, kr1, KL, KB,
    sx_sem, rx_sem, sv_sem, rv_sem, sn_sem, rn_sem, sp_sem, rp_sem, loc_sem, ko_sem, kb_sem, kx_sem,
    s1_sem, r1_sem, sy_sem, ry_sem, ryp_sem, s2_sem, r2_sem,
):
    me = lax.axis_index("row")
    core, cx, cy = me % 2, (me // 2) % 2, me // 4

    def dev(px, py, pc):
        return {"row": (py * 2 + px) * 2 + pc}

    tx = dev(1 - cx, cy, (core + 1 + cx) % 2)
    ty = dev(cx, 1 - cy, (core + 1 + cx + cy) % 2)
    sx = dev(1 - cx, cy, (core + cx) % 2)
    sy = dev(cx, 1 - cy, (core + cx + cy) % 2)
    pt = dev(cx, cy, 1 - core)

    def remote(src, dst, ss, rs, to):
        return pltpu.make_async_remote_copy(src_ref=src, dst_ref=dst, send_sem=ss, recv_sem=rs, device_id=to, device_id_type=MESH)

    def part_rows(i, late):
        return rows_of(i + 4) if late else cols_of(i)

    def x_copy(j, i, late):
        return remote(x_hbm.at[part_rows(i, late)], X.at[1 + j, part_rows(i, late)], sx_sem.at[j], rx_sem.at[i], (tx, ty)[j])

    def wait_x(i, late):
        two = X.at[1:3, part_rows(i, late)]
        remote(two, two, sx_sem.at[0], rx_sem.at[i], tx).wait_recv()

    p_copy = remote(x_hbm, X.at[PAR], sp_sem, rp_sem, pt)
    v_copies = [remote(v_hbm, VT.at[1 + j], sv_sem, rv_sem.at[j // 2], d) for j, d in enumerate((tx, ty, pt))]
    n_copies = [remote(NB.at[OWN], NB.at[1 + j], sn_sem, rn_sem.at[j // 2], d) for j, d in enumerate((tx, ty, pt))]

    x_loc = pltpu.make_async_copy(x_hbm, X.at[OWN], loc_sem.at[0])
    v_loc = pltpu.make_async_copy(v_hbm, VT.at[OWN], loc_sem.at[1])
    for c in (v_loc, x_loc):
        c.start()

    barrier = pltpu.get_barrier_semaphore()
    for d in (tx, ty, sx, sy, pt):
        pl.semaphore_signal(barrier, inc=1, device_id=d, device_id_type=MESH)
    with jax.named_scope("barrier"):
        pl.semaphore_wait(barrier, 5)

    for c in v_copies:
        c.start()
    for j in range(2):
        x_copy(j, 0, False).start()
    p_copy.start()

    ell = jnp.full((1, CHUNK), ell_ref[0], F32)
    half = LOG2E / (2.0 * ell * ell)
    top = jnp.log2(jnp.full((1, CHUNK), amp_ref[0], F32))
    CR[0:1, :] = 2.0 * half
    CR[1:2, :] = top

    for s in range(3):
        YR[s] = jnp.zeros((STRIP + ROWS, 32), F32)
    for t in range(5):
        YT[t] = jnp.zeros((32, ROWS), F32)
    kr0[...] = jnp.zeros_like(kr0)
    kr1[...] = jnp.zeros_like(kr1)

    v_loc.wait()
    with jax.named_scope("x_local"):
        x_loc.wait()

    def own_norm(c, _):
        r = pl.ds(pl.multiple_of(c * CHUNK, CHUNK), CHUNK)
        x = X[OWN, r, :].astype(F32)
        n = jnp.broadcast_to(0.5 * jnp.sum(x * x, axis=1, keepdims=True), (CHUNK, 128))
        NA[OWN, r, :] = n
        NB[OWN, :, cols_of(c)] = jnp.transpose(n)[0:1, :]
        return 0

    with jax.named_scope("own_norm"):
        lax.fori_loop(0, N_CHUNK, own_norm, 0)
    for c in n_copies:
        c.start()

    for i in range(1, 8):
        for j in range(2):
            x_copy(j, i, i >= 4).start()

    def left_norm(s):
        def one(c, _):
            r = pl.ds(pl.multiple_of(c * CHUNK, CHUNK), CHUNK)
            NA[s, r, :] = jnp.transpose(jnp.broadcast_to(NB[s, :, cols_of(c)], (128, CHUNK)))
            return 0

        lax.fori_loop(0, N_CHUNK, one, 0)

    def gram(tile):
        s, a, t, b, _ = tile
        return lax.dot_general(X[s, rows_of(a), :], X[t, cols_of(b), :], (((1,), (1,)), ((), ())), preferred_element_type=F32)

    def kern(tile, g):
        s, a, t, b, _ = tile
        na = NA[s, rows_of(a), :]
        d = (jnp.concatenate([na] * (CHUNK // 128), axis=1) + NB[t, :, cols_of(b)]) - g
        return jnp.exp2(CR[1:2, :] - jnp.maximum(d, 0.0) * CR[0:1, :]).astype(BF16)

    def apply(tile, k, vec):
        s, a, t, b, to = tile
        YR[s, rows_of(a + 1), :] += lax.dot_general(k, vec[t, :, cols_of(b)], (((1,), (1,)), ((), ())), preferred_element_type=F32)
        YT[to, :, cols_of(b)] += jnp.dot(vec[s, :, rows_of(jnp.maximum(a, 0))], k, preferred_element_type=F32)

    def k_out(seq, place, half):
        kr = (kr0, kr1)[half]
        row = pl.multiple_of(place * STEP_ROWS + half * HALF_ROWS, STRIP)
        return pltpu.make_async_copy(kr.at[seq & 1], k_hbm.at[pl.ds(row, HALF_ROWS)], ko_sem.at[seq & 1, half])

    def half_step(prev, cur, kr_new, d_new, kr_old, d_old):
        gs = [gram(t) for t in cur]
        for u in range(UNITS):
            apply(prev[u], kr_old[d_old, u * STRIP : (u + 1) * STRIP, :], VT)
        for u in range(UNITS):
            kr_new[d_new, u * STRIP : (u + 1) * STRIP, :] = kern(cur[u], gs[u])

    def flat(tiles):
        return tuple(x for t in tiles for x in t)

    def unflat(xs):
        return [tuple(xs[5 * u : 5 * u + 5]) for u in range(UNITS)]

    def begin(seq, before, place):
        @pl.when(seq >= 2)
        def _():
            for h in range(2):
                k_out(seq, place, h).wait()

        @pl.when(seq >= 1)
        def _():
            for h in range(2):
                k_out(seq - 1, before, h).start()

        return seq & 1

    def step_of(state, place, tile):
        seq, before, prev = state[0], state[1], state[2:]
        d = begin(seq, before, place)
        first = [tile(u) for u in range(UNITS)]
        second = [tile(UNITS + u) for u in range(UNITS)]
        half_step(unflat(prev), first, kr0, d, kr1, 1 - d)
        half_step(first, second, kr1, d, kr0, d)
        return (seq + 1, place) + flat(second)

    none = flat([i32(OWN, -1, OWN, 0, TRASH)] * UNITS)

    def own_step(o, state):
        @pl.when(o == N_OWN)
        def _():
            p_copy.wait_recv()
            v_copies[2].wait_recv()
            n_copies[2].wait_recv()

        return step_of(state, table(OWN_PLACE, o), lambda j: own_tile(o, j, core))

    def remote_step(p, state):
        return step_of(state, table(REMOTE_PLACE, p), lambda j: remote_tile(p, j))

    def cross_step(q, state):
        return step_of(state, CROSS_PLACE + q, lambda j: cross_tile(q, j))

    with jax.named_scope("pre"):
        state = lax.fori_loop(0, N_PAIR, own_step, i32(0, 0) + none)

    with jax.named_scope("left_norm"):
        remote(VT.at[1:3], VT.at[1:3], sv_sem, rv_sem.at[0], tx).wait_recv()
        remote(NB.at[1:3], NB.at[1:3], sn_sem, rn_sem.at[0], tx).wait_recv()
        for j in range(2):
            left_norm(1 + j)

    def landed(i, state):
        with jax.named_scope("wait_strip"):

            @pl.when(i < 4)
            def _():
                wait_x(i, False)

            @pl.when(i >= 4)
            def _():
                wait_x(i, True)

        with jax.named_scope("strip"):
            state = lax.fori_loop(table(REMOTE_AT, i), table(REMOTE_AT, i + 1), remote_step, state)
            return lax.fori_loop(table(CROSS_AT, i), table(CROSS_AT, i + 1), cross_step, state)

    state = lax.fori_loop(0, 7, landed, state)

    homes = ((XNB, sx), (YNB, sy), (PAR, pt))

    def part_copy(j, c, send, recv, ss, rs):
        return remote(send.at[j, :, cols_of(c)], recv.at[j, :, cols_of(c)], ss, rs.at[c] if send is SB else rs, homes[j][1])

    def finish(j, c, send):
        s = homes[j][0]
        part = YT[s, :, cols_of(c)]
        if j < 2:
            part = part + jnp.transpose(YR[s, sums_of(c), :])
        send[j, :, cols_of(c)] = part
        if send is SB:
            YT[s, :, cols_of(c)] = jnp.zeros((32, CHUNK), F32)
            if j < 2:
                YR[s, sums_of(c), :] = jnp.zeros((CHUNK, 32), F32)

    def finish_range(lo, hi, send, recv, ss, rs, js=(0, 1)):
        for c in range(lo, hi):
            for j in js:
                finish(j, c, send)
            for j in js:
                part_copy(j, c, send, recv, ss, rs).start()

    def load_kb(d, slot):
        return pltpu.make_async_copy(k_hbm.at[pl.ds(pl.multiple_of(d * 2 * STEP_ROWS, STRIP), 2 * STEP_ROWS)], KB.at[slot], kb_sem.at[slot])

    def load_x(d, slot):
        src = k_hbm.at[pl.ds(pl.multiple_of(d * 2 * STEP_ROWS, STRIP), 2 * STEP_ROWS)]
        return pltpu.make_async_copy(src, X.at[slot, :, 0:CHUNK], kx_sem.at[slot])

    first_in = pltpu.make_async_copy(k_hbm.at[pl.ds(STEP_ROWS, STEP_ROWS)], KB.at[0, pl.ds(STEP_ROWS, STEP_ROWS)], kb_sem.at[0])
    first_in.start()
    for i in range(1, 4):
        load_kb(i, i).start()

    def y_copy(j, c):
        return remote(YV.at[OWN, :, cols_of(c)], YV.at[1 + j, :, cols_of(c)], sy_sem, ryp_sem.at[(c >= 3).astype(jnp.int32) + (c >= 4).astype(jnp.int32)] if j == 2 else ry_sem.at[c], (tx, ty, pt)[j])

    def middle(lo, hi):
        def one(c, _):
            with jax.named_scope("wait_part"):
                three = RB.at[:, :, cols_of(c)]
                remote(three, three, s1_sem, r1_sem.at[c], pt).wait_recv()
            y = YT[OWN, :, cols_of(c)] + jnp.transpose(YR[OWN, sums_of(c), :])
            y = y + RB[0, :, cols_of(c)] + RB[1, :, cols_of(c)] + RB[2, :, cols_of(c)]
            YV[OWN, :, cols_of(c)] = y.astype(BF16)
            YT[OWN, :, cols_of(c)] = jnp.zeros((32, CHUNK), F32)
            YR[OWN, sums_of(c), :] = jnp.zeros((CHUNK, 32), F32)
            for j in range(3):
                y_copy(j, c).start()
            return 0

        lax.fori_loop(lo, hi, one, 0)

    last = last_tiles()
    late = [remote_tile(jnp.int32(23), j) for j in range(6)]

    def rows_in(u, d):
        if d is None:
            return KL, (slice(u * STRIP, (u + 1) * STRIP), slice(None))
        return (kr0, kr1)[u % 6 // UNITS], (d, slice(u % UNITS * STRIP, (u % UNITS + 1) * STRIP), slice(None))

    def grams(tiles, first, d):
        gs = [gram(t) for t in tiles]

        def put():
            for u, (t, g) in enumerate(zip(tiles, gs), first):
                ref, at = rows_in(u, d)
                ref[at] = kern(t, g)

        return put

    def applies(tiles, first, d):
        for u, t in enumerate(tiles, first):
            ref, at = rows_in(u, d)
            apply(t, ref[at], VT)

    kl_out = pltpu.make_async_copy(KL, k_hbm.at[pl.ds(REMOTE_PLACE[23] * STEP_ROWS, STEP_ROWS)], loc_sem.at[0])
    seq, before, due = state[0], state[1], unflat(state[2:])
    d = begin(seq, before, before)
    put = grams(late[0:2], 0, None)
    applies(due, UNITS, 1 - d)
    put()
    applies(late[0:2], 0, None)
    finish_range(0, N_CHUNK, SB, RB, s1_sem, r1_sem, (2,))
    with jax.named_scope("wait_last"):
        wait_x(7, True)
    with jax.named_scope("last"):
        for c in range(N_CHUNK):
            if c == 3:
                d = begin(seq + 1, jnp.int32(CROSS_PLACE + 10), before)
            put = grams(last[2 * c : 2 * c + 2], 2 * c, d)
            if c > 1:
                applies(last[2 * c - 2 : 2 * c], 2 * c - 2, 1 - d if c == 3 else d)
            put()
            if c == 0:
                applies(last[0:2], 0, d)
            if c != 1:
                finish_range(max(c - 1, 0), max(c, 1), SB, RB, s1_sem, r1_sem)
        put = grams(late[2:6], 2, None)
        applies(last[10:12], 10, d)
        put()
        kl_out.start()
        load_x(4, 0).start()
        middle(0, 1)
        applies(late[2:6], 2, None)
        finish_range(5, 6, SB, RB, s1_sem, r1_sem)

    for h in range(2):
        k_out(seq, 0, h).wait()
        k_out(seq + 1, CROSS_PLACE + 11, h).start()

    def use(k, slot, tile):
        for h in range(2):
            use_step(k, slot, h, functools.partial(tile, h))

    def use_step(k, slot, h, tile):
        for j in range(6):
            r = (6 * h + j) * STRIP
            apply(tile(j), k[slot, r : r + STRIP, 0:CHUNK], YV)

    def quad(t, tile):
        slot = t & 3
        load_x(0, slot).wait()
        load_kb(0, slot).wait()
        t = jnp.int32(t)

        @pl.when(jnp.logical_and(t >= 1, t <= 7))
        def _():
            load_x(10 + 2 * t, (t - 1) & 3).start()

        @pl.when(jnp.logical_and(t >= 1, t <= 6))
        def _():
            load_kb(11 + 2 * t, (t - 1) & 3).start()

        use(X, slot, lambda h, j: tile(0, h, j))
        use(KB, slot, lambda h, j: tile(1, h, j))

    def wait_y(lo, hi):
        def one(c, _):
            two = YV.at[1:3, :, cols_of(c)]
            remote(two, two, sy_sem, ry_sem.at[c], tx).wait_recv()
            return 0

        lax.fori_loop(lo, hi, one, 0)

    def wait_y_par(late):
        part = YV.at[PAR, :, pl.ds((0, 3, 4)[late] * CHUNK, (3, 1, 2)[late] * CHUNK)]
        remote(part, part, sy_sem, ryp_sem.at[late], pt).wait_recv()

    with jax.named_scope("middle"):
        middle(1, 2)
    with jax.named_scope("second_own"):
        first_in.wait()
        for j in range(6):
            apply(own_tile(jnp.int32(0), j, core), KB[0, STEP_ROWS + j * STRIP : STEP_ROWS + (j + 1) * STRIP, :], YV)
        load_kb(5, 0).start()
        middle(2, 3)
        load_kb(0, 1).wait()
        use_step(KB, 1, 0, lambda j: own_tile(jnp.int32(1), j, core))
        wait_y_par(0)
        load_kb(0, 2).wait()
        use_step(KB, 2, 0, lambda j: own_tile(jnp.int32(N_OWN), j, core))
        middle(3, 4)
        use_step(KB, 1, 1, lambda j: own_tile(jnp.int32(2), j, core))
        load_x(6, 1).start()
        load_kb(7, 1).start()
        wait_y_par(1)
        use_step(KB, 2, 1, lambda j: own_tile(jnp.int32(N_OWN + 1), j, core))
        load_x(8, 2).start()
        load_kb(9, 2).start()
        kl_out.wait()
        for h in range(2):
            k_out(seq + 1, 0, h).wait()
        load_x(10, 3).start()
        middle(4, 5)

    def remote_quad(step):
        ps = [step(i) for i in range(4)]
        return lambda d, h, j: remote_tile(ps[2 * d + h], j)

    with jax.named_scope("second_first"):

        wait_y(0, 1)
        quad(0, remote_quad(jnp.int32))
        middle(5, 6)
        load_kb(0, 3).wait()
        use(KB, 3, lambda h, j: own_tile(jnp.int32(3 + h), j, core))
        load_kb(11, 3).start()
        wait_y_par(2)
        wait_y(1, 2)
        quad(1, remote_quad(lambda i: jnp.int32(4 + i)))
    with jax.named_scope("second_cross"):

        def second_cross(t, _):
            with jax.named_scope("wait_y"):
                wait_y(table((2, 2, 2) + Y_NEED[:-1], t), table((2, 2) + Y_NEED, t))

            def tile(d, h, j):
                cross = cross_tile(4 * (t - 2) + 2 * d + h, j)
                return pick(t < 4, cross, last[6 * h + j]) if d else cross

            quad(t, tile)
            return 0

        lax.fori_loop(2, 5, second_cross, 0)

    for k, done in enumerate(((0,), (4, 5), (3,))):
        for c in done:
            finish_range(c, c + 1, SB2, RB2, s2_sem, r2_sem)
        with jax.named_scope("second_chunk"):
            ps = REMOTE_ORDER[4 * k : 4 * k + 4]
            quad(5 + k, remote_quad(lambda i: jnp.int32(ps[i])))

    def finish_strip(n):
        cols = pl.ds(n * STRIP, STRIP)
        for j in range(2):
            s = homes[j][0]
            SB2[j, :, cols] = YT[s, :, cols] + jnp.transpose(YR[s, pl.ds((n + 1) * STRIP, STRIP), :])
        for j in range(2):
            remote(SB2.at[j, :, cols], RB2.at[j, :, cols], s2_sem, r2_sem, homes[j][1]).start()

    with jax.named_scope("second_chunk"):
        finish_range(2, 3, SB2, RB2, s2_sem, r2_sem)
        load_x(0, 0).wait()
        load_kb(0, 0).wait()
        use(X, 0, lambda h, j: remote_tile(jnp.int32(REMOTE_ORDER[12 + h]), j))
        finish_strip(2)
        use(KB, 0, lambda h, j: remote_tile(jnp.int32(REMOTE_ORDER[14 + h]), j))
        finish_strip(3)

    with jax.named_scope("second_par"):
        quad(9, lambda d, h, j: own_tile(jnp.int32(N_OWN + 2 + 2 * d + h), j, core))
        remote(YT.at[PAR], RB2.at[2], s2_sem, r2_sem, pt).start()

    with jax.named_scope("second_end"):
        load_x(0, 2).wait()
        use(X, 2, lambda h, j: own_tile(jnp.int32(5 + h), j, core))

    with jax.named_scope("sent"):
        p_copy.wait_send()
        for j in range(2):
            remote(x_hbm, X.at[1 + j], sx_sem.at[j], rx_sem.at[0], tx).wait_send()
        for buf, sem in ((VT, sv_sem), (NB, sn_sem), (YV, sy_sem)):
            remote(buf.at[1:4], buf.at[1:4], sem, rx_sem.at[0], tx).wait_send()
        remote(SB, RB, s1_sem, rx_sem.at[0], tx).wait_send()

    with jax.named_scope("final"):
        for c in range(N_CHUNK):
            out_ref[:, cols_of(c)] = YT[OWN, :, cols_of(c)] + jnp.transpose(YR[OWN, sums_of(c), :])
        all_sums = remote(SB2, RB2, s2_sem, r2_sem, pt)
        all_sums.wait_send()
        all_sums.wait_recv()


def solution(mesh):
    def local_program(x_loc, v_loc, length_scale, out_scale):
        dma = pltpu.SemaphoreType.DMA
        hbm = pl.BlockSpec(memory_space=pltpu.HBM)
        vmem = pl.BlockSpec(memory_space=pltpu.VMEM)
        smem = pl.BlockSpec(memory_space=pltpu.SMEM)
        own, parts, _ = pl.pallas_call(
            body,
            out_shape=(
                pltpu.VMEM((32, ROWS), F32),
                pltpu.VMEM((3, 32, ROWS), F32),
                jax.ShapeDtypeStruct((N_PLACE * STEP_ROWS, CHUNK), BF16),
            ),
            in_specs=[hbm, hbm, smem, smem],
            out_specs=(vmem, vmem, hbm),
            scratch_shapes=[
                pltpu.VMEM((4, ROWS, 768), BF16),
                pltpu.VMEM((4, 32, ROWS), BF16),
                pltpu.VMEM((4, 32, ROWS), BF16),
                pltpu.VMEM((3, ROWS, 128), F32),
                pltpu.VMEM((4, 1, ROWS), F32),
                pltpu.VMEM((8, CHUNK), F32),
                pltpu.VMEM((3, STRIP + ROWS, 32), F32),
                pltpu.VMEM((5, 32, ROWS), F32),
                pltpu.VMEM((3, 32, ROWS), F32),
                pltpu.VMEM((3, 32, ROWS), F32),
                pltpu.VMEM((3, 32, ROWS), F32),
                pltpu.VMEM((2, HALF_ROWS, CHUNK), BF16),
                pltpu.VMEM((2, HALF_ROWS, CHUNK), BF16),
                pltpu.VMEM((STEP_ROWS, CHUNK), BF16),
                pltpu.VMEM((4, 2 * STEP_ROWS, CHUNK), BF16),
                dma((2,)), dma((8,)), dma, dma((2,)), dma, dma((2,)), dma, dma,
                dma((2,)), dma((2, 2)), dma((4,)), dma((4,)),
                dma, dma((N_CHUNK,)), dma, dma((N_CHUNK,)), dma((3,)), dma, dma,
            ],
            compiler_params=pltpu.CompilerParams(collective_id=0, has_side_effects=True, vmem_limit_bytes=58 * 2**20),
            name="products",
        )(x_loc, v_loc.T, length_scale, out_scale)
        return (own + parts[0] + parts[1] + parts[2]).T

    row_spec = P(("task", "row"), None)
    return jax.shard_map(local_program, mesh=mesh, in_specs=(row_spec, row_spec, P("task"), P("task")), out_specs=row_spec, check_vma=False)
```

```python
import functools

import jax
import jax.numpy as jnp
from jax import lax
from jax.experimental import pallas as pl
from jax.experimental.pallas import tpu as pltpu
from jax.sharding import PartitionSpec as P

MESH = pl.DeviceIdType.MESH
F32, BF16 = jnp.float32, jnp.bfloat16
LOG2E = 1.4426950408889634

ROWS = 3072
STRIP = 256
CHUNK = 512
N_STRIP = ROWS // STRIP
N_CHUNK = ROWS // CHUNK
UNITS = 3
OWN, XNB, YNB, PAR, TRASH = 0, 1, 2, 3, 4

N_OWN, N_PAIR = 7, 13
REMOTE_AT = (0, 7, 13, 18, 21, 21, 23, 23)
REMOTE_TILE = (0, 44, 80, 108, 128, 140)
CROSS_AT = (0, 0, 1, 3, 5, 6, 8, 10)
CROSS_TILE = (0, 0, 2, 4, 8, 12, 18, 24, 32, 40, 50, 60)
OWN_PLACE = (1, 2, 3, 6, 7, 48, 49, 4, 5, 44, 45, 46, 47)
REMOTE_ORDER = (20, 21, 22, 23, 16, 17, 18, 19, 10, 13, 14, 15, 8, 9, 11, 12)
REMOTE_PLACE = tuple(8 + p if p < 8 else 28 + REMOTE_ORDER.index(p) for p in range(24))
CROSS_PLACE = 16
N_PLACE = 50
STEP_ROWS = 6 * STRIP
HALF_ROWS = UNITS * STRIP
Y_NEED = (4, 5, 6)


def table(values, n):
    out = jnp.int32(values[0])
    for i in range(1, len(values)):
        if values[i] != values[i - 1]:
            out = out + (values[i] - values[i - 1]) * (n >= i).astype(jnp.int32)
    return out


def rank(bounds, x):
    out = jnp.int32(0)
    for b in bounds:
        out = out + (x >= b).astype(jnp.int32)
    return out


def pick(cond, a, b):
    return tuple(jnp.where(cond, x, y) for x, y in zip(a, b))


def i32(*xs):
    return tuple(jnp.int32(x) for x in xs)


def own_tile(o, j, core):
    p = 3 * o + j // 2
    c = rank((1, 3, 6, 10, 15), p)
    i = p - ((c * (c + 1)) >> 1)
    own = (jnp.int32(OWN), 2 * i + j % 2, jnp.int32(OWN), c, jnp.where(i == c, TRASH, OWN))
    p = 3 * (o - N_OWN) + j // 2
    c = 1 + rank((1, 3, 6, 10), p)
    i = p - ((c * (c - 1)) >> 1)
    same = core + 2 * (j // 2)
    i, c = pick(p < 15, (i, c), (same, same))
    par = (jnp.int32(OWN), 2 * i + j % 2, jnp.int32(PAR), c, jnp.int32(PAR))
    return pick(o < N_OWN, own, par)


def remote_tile(p, j):
    g = 6 * p + j
    d, first = jnp.int32(0), jnp.int32(0)
    for i in range(1, N_CHUNK):
        d, first = pick(g >= REMOTE_TILE[i], (i, REMOTE_TILE[i]), (d, first))
    r = g - first
    rest = r - (22 - 4 * d)
    k, side, odd = pick(rest >= 0, (rest >> 1, r & 1, 1), (r >> 1, r & 1, 0))
    k, side, odd = pick(d == 0, (r >> 2, (r >> 1) & 1, r & 1), (k, side, odd))
    t = jnp.where((k & 1) == (k > 0).astype(jnp.int32), OWN, PAR)
    return (1 + side, 2 * d + odd, t, d + ((k + 1) >> 1), t)


def cross_tile(q, j):
    g = 6 * q + j
    n, first = jnp.int32(1), jnp.int32(0)
    for i in range(2, N_STRIP - 1):
        n, first = pick(g >= CROSS_TILE[i], (i, CROSS_TILE[i]), (n, first))
    r = g - first
    m = n >> 1
    t = pick(r < m, (jnp.int32(XNB), n, jnp.int32(YNB), r, jnp.int32(YNB)), (jnp.int32(YNB), n, jnp.int32(XNB), r - m, jnp.int32(XNB)))
    return pick(r < 2 * m, t, (jnp.int32(XNB), n - 1 + (r - 2 * m), jnp.int32(YNB), m, jnp.int32(YNB)))


def last_tiles():
    n = N_STRIP - 1
    tiles = [t for c in range(N_CHUNK - 1) for t in ((YNB, n, XNB, c, XNB), (XNB, n, YNB, c, YNB))]
    tiles += [(XNB, n - 1, YNB, N_CHUNK - 1, YNB), (XNB, n, YNB, N_CHUNK - 1, YNB)]
    return [i32(*t) for t in tiles]


def span(start, size, unit):
    return pl.ds(start if isinstance(start, int) else pl.multiple_of(start, unit), size)


def rows_of(a):
    return span(a * STRIP, STRIP, STRIP)


def sums_of(c):
    return span(STRIP + c * CHUNK, CHUNK, STRIP)


def cols_of(b):
    return span(b * CHUNK, CHUNK, CHUNK)


def body(
    x_hbm, v_hbm, ell_ref, amp_ref, out_ref, RB2, k_hbm,
    X, VT, YV, NA, NB, CR, YR, YT, SB, RB, SB2, kr0, kr1, KL, KB,
    sx_sem, rx_sem, sv_sem, rv_sem, sn_sem, rn_sem, sp_sem, rp_sem, loc_sem, ko_sem, kb_sem, kx_sem,
    s1_sem, r1_sem, sy_sem, ry_sem, ryp_sem, s2_sem, r2_sem,
):
    me = lax.axis_index("row")
    core, cx, cy = me % 2, (me // 2) % 2, me // 4

    def dev(px, py, pc):
        return {"row": (py * 2 + px) * 2 + pc}

    tx = dev(1 - cx, cy, (core + 1 + cx) % 2)
    ty = dev(cx, 1 - cy, (core + 1 + cx + cy) % 2)
    sx = dev(1 - cx, cy, (core + cx) % 2)
    sy = dev(cx, 1 - cy, (core + cx + cy) % 2)
    pt = dev(cx, cy, 1 - core)

    def remote(src, dst, ss, rs, to):
        return pltpu.make_async_remote_copy(src_ref=src, dst_ref=dst, send_sem=ss, recv_sem=rs, device_id=to, device_id_type=MESH)

    def part_rows(i, late):
        return rows_of(i + 4) if late else cols_of(i)

    def x_copy(j, i, late):
        return remote(x_hbm.at[part_rows(i, late)], X.at[1 + j, part_rows(i, late)], sx_sem.at[j], rx_sem.at[i], (tx, ty)[j])

    def wait_x(i, late):
        two = X.at[1:3, part_rows(i, late)]
        remote(two, two, sx_sem.at[0], rx_sem.at[i], tx).wait_recv()

    p_copy = remote(x_hbm, X.at[PAR], sp_sem, rp_sem, pt)
    v_copies = [remote(v_hbm, VT.at[1 + j], sv_sem, rv_sem.at[j // 2], d) for j, d in enumerate((tx, ty, pt))]
    n_copies = [remote(NB.at[OWN], NB.at[1 + j], sn_sem, rn_sem.at[j // 2], d) for j, d in enumerate((tx, ty, pt))]

    x_loc = pltpu.make_async_copy(x_hbm, X.at[OWN], loc_sem.at[0])
    v_loc = pltpu.make_async_copy(v_hbm, VT.at[OWN], loc_sem.at[1])
    for c in (v_loc, x_loc):
        c.start()

    barrier = pltpu.get_barrier_semaphore()
    for d in (tx, ty, sx, sy, pt):
        pl.semaphore_signal(barrier, inc=1, device_id=d, device_id_type=MESH)
    with jax.named_scope("barrier"):
        pl.semaphore_wait(barrier, 5)

    for c in v_copies:
        c.start()
    for j in range(2):
        x_copy(j, 0, False).start()
    p_copy.start()

    ell = jnp.full((1, CHUNK), ell_ref[0], F32)
    half = LOG2E / (2.0 * ell * ell)
    top = jnp.log2(jnp.full((1, CHUNK), amp_ref[0], F32))
    CR[0:1, :] = 2.0 * half
    CR[1:2, :] = top

    for s in range(3):
        YR[s] = jnp.zeros((STRIP + ROWS, 32), F32)
    for t in range(5):
        YT[t] = jnp.zeros((32, ROWS), F32)
    kr0[...] = jnp.zeros_like(kr0)
    kr1[...] = jnp.zeros_like(kr1)

    v_loc.wait()
    with jax.named_scope("x_local"):
        x_loc.wait()

    def own_norm(c, _):
        r = pl.ds(pl.multiple_of(c * CHUNK, CHUNK), CHUNK)
        x = X[OWN, r, :].astype(F32)
        n = jnp.broadcast_to(0.5 * jnp.sum(x * x, axis=1, keepdims=True), (CHUNK, 128))
        NA[OWN, r, :] = n
        NB[OWN, :, cols_of(c)] = jnp.transpose(n)[0:1, :]
        return 0

    with jax.named_scope("own_norm"):
        lax.fori_loop(0, N_CHUNK, own_norm, 0)
    for c in n_copies:
        c.start()

    for i in range(1, 8):
        for j in range(2):
            x_copy(j, i, i >= 4).start()

    def left_norm(s):
        def one(c, _):
            r = pl.ds(pl.multiple_of(c * CHUNK, CHUNK), CHUNK)
            NA[s, r, :] = jnp.transpose(jnp.broadcast_to(NB[s, :, cols_of(c)], (128, CHUNK)))
            return 0

        lax.fori_loop(0, N_CHUNK, one, 0)

    def gram(tile):
        s, a, t, b, _ = tile
        return lax.dot_general(X[s, rows_of(a), :], X[t, cols_of(b), :], (((1,), (1,)), ((), ())), preferred_element_type=F32)

    def kern(tile, g):
        s, a, t, b, _ = tile
        na = NA[s, rows_of(a), :]
        d = (jnp.concatenate([na] * (CHUNK // 128), axis=1) + NB[t, :, cols_of(b)]) - g
        return jnp.exp2(CR[1:2, :] - jnp.maximum(d, 0.0) * CR[0:1, :]).astype(BF16)

    def apply(tile, k, vec):
        s, a, t, b, to = tile
        YR[s, rows_of(a + 1), :] += lax.dot_general(k, vec[t, :, cols_of(b)], (((1,), (1,)), ((), ())), preferred_element_type=F32)
        YT[to, :, cols_of(b)] += jnp.dot(vec[s, :, rows_of(jnp.maximum(a, 0))], k, preferred_element_type=F32)

    def k_out(seq, place, half):
        kr = (kr0, kr1)[half]
        row = pl.multiple_of(place * STEP_ROWS + half * HALF_ROWS, STRIP)
        return pltpu.make_async_copy(kr.at[seq & 1], k_hbm.at[pl.ds(row, HALF_ROWS)], ko_sem.at[seq & 1, half])

    def half_step(prev, cur, kr_new, d_new, kr_old, d_old):
        gs = [gram(t) for t in cur]
        for u in range(UNITS):
            apply(prev[u], kr_old[d_old, u * STRIP : (u + 1) * STRIP, :], VT)
        for u in range(UNITS):
            kr_new[d_new, u * STRIP : (u + 1) * STRIP, :] = kern(cur[u], gs[u])

    def flat(tiles):
        return tuple(x for t in tiles for x in t)

    def unflat(xs):
        return [tuple(xs[5 * u : 5 * u + 5]) for u in range(UNITS)]

    def begin(seq, before, place):
        @pl.when(seq >= 2)
        def _():
            for h in range(2):
                k_out(seq, place, h).wait()

        @pl.when(seq >= 1)
        def _():
            for h in range(2):
                k_out(seq - 1, before, h).start()

        return seq & 1

    def step_of(state, place, tile):
        seq, before, prev = state[0], state[1], state[2:]
        d = begin(seq, before, place)
        first = [tile(u) for u in range(UNITS)]
        second = [tile(UNITS + u) for u in range(UNITS)]
        half_step(unflat(prev), first, kr0, d, kr1, 1 - d)
        half_step(first, second, kr1, d, kr0, d)
        return (seq + 1, place) + flat(second)

    none = flat([i32(OWN, -1, OWN, 0, TRASH)] * UNITS)

    def own_step(o, state):
        @pl.when(o == N_OWN)
        def _():
            p_copy.wait_recv()
            v_copies[2].wait_recv()
            n_copies[2].wait_recv()

        return step_of(state, table(OWN_PLACE, o), lambda j: own_tile(o, j, core))

    def remote_step(p, state):
        return step_of(state, table(REMOTE_PLACE, p), lambda j: remote_tile(p, j))

    def cross_step(q, state):
        return step_of(state, CROSS_PLACE + q, lambda j: cross_tile(q, j))

    with jax.named_scope("pre"):
        state = lax.fori_loop(0, N_PAIR, own_step, i32(0, 0) + none)

    with jax.named_scope("left_norm"):
        remote(VT.at[1:3], VT.at[1:3], sv_sem, rv_sem.at[0], tx).wait_recv()
        remote(NB.at[1:3], NB.at[1:3], sn_sem, rn_sem.at[0], tx).wait_recv()
        for j in range(2):
            left_norm(1 + j)

    def landed(i, state):
        with jax.named_scope("wait_strip"):

            @pl.when(i < 4)
            def _():
                wait_x(i, False)

            @pl.when(i >= 4)
            def _():
                wait_x(i, True)

        with jax.named_scope("strip"):
            state = lax.fori_loop(table(REMOTE_AT, i), table(REMOTE_AT, i + 1), remote_step, state)
            return lax.fori_loop(table(CROSS_AT, i), table(CROSS_AT, i + 1), cross_step, state)

    state = lax.fori_loop(0, 7, landed, state)

    homes = ((XNB, sx), (YNB, sy), (PAR, pt))

    def part_copy(j, c, send, recv, ss, rs):
        return remote(send.at[j, :, cols_of(c)], recv.at[j, :, cols_of(c)], ss, rs.at[c] if send is SB else rs, homes[j][1])

    def finish(j, c, send):
        s = homes[j][0]
        part = YT[s, :, cols_of(c)]
        if j < 2:
            part = part + jnp.transpose(YR[s, sums_of(c), :])
        send[j, :, cols_of(c)] = part
        if send is SB:
            YT[s, :, cols_of(c)] = jnp.zeros((32, CHUNK), F32)
            if j < 2:
                YR[s, sums_of(c), :] = jnp.zeros((CHUNK, 32), F32)

    def finish_range(lo, hi, send, recv, ss, rs, js=(0, 1)):
        for c in range(lo, hi):
            for j in js:
                finish(j, c, send)
            for j in js:
                part_copy(j, c, send, recv, ss, rs).start()

    def load_kb(d, slot):
        return pltpu.make_async_copy(k_hbm.at[pl.ds(pl.multiple_of(d * 2 * STEP_ROWS, STRIP), 2 * STEP_ROWS)], KB.at[slot], kb_sem.at[slot])

    def load_x(d, slot):
        src = k_hbm.at[pl.ds(pl.multiple_of(d * 2 * STEP_ROWS, STRIP), 2 * STEP_ROWS)]
        return pltpu.make_async_copy(src, X.at[slot, :, 0:CHUNK], kx_sem.at[slot])

    first_in = pltpu.make_async_copy(k_hbm.at[pl.ds(STEP_ROWS, STEP_ROWS)], KB.at[0, pl.ds(STEP_ROWS, STEP_ROWS)], kb_sem.at[0])
    first_in.start()
    for i in range(1, 4):
        load_kb(i, i).start()

    def y_copy(j, c):
        return remote(YV.at[OWN, :, cols_of(c)], YV.at[1 + j, :, cols_of(c)], sy_sem, ryp_sem.at[(c >= 3).astype(jnp.int32) + (c >= 4).astype(jnp.int32)] if j == 2 else ry_sem.at[c], (tx, ty, pt)[j])

    def middle(lo, hi):
        def one(c, _):
            with jax.named_scope("wait_part"):
                three = RB.at[:, :, cols_of(c)]
                remote(three, three, s1_sem, r1_sem.at[c], pt).wait_recv()
            y = YT[OWN, :, cols_of(c)] + jnp.transpose(YR[OWN, sums_of(c), :])
            y = y + RB[0, :, cols_of(c)] + RB[1, :, cols_of(c)] + RB[2, :, cols_of(c)]
            YV[OWN, :, cols_of(c)] = y.astype(BF16)
            YT[OWN, :, cols_of(c)] = jnp.zeros((32, CHUNK), F32)
            YR[OWN, sums_of(c), :] = jnp.zeros((CHUNK, 32), F32)
            for j in range(3):
                y_copy(j, c).start()
            return 0

        lax.fori_loop(lo, hi, one, 0)

    last = last_tiles()
    late = [remote_tile(jnp.int32(23), j) for j in range(6)]

    def rows_in(u, d):
        if d is None:
            return KL, (slice(u * STRIP, (u + 1) * STRIP), slice(None))
        return (kr0, kr1)[u % 6 // UNITS], (d, slice(u % UNITS * STRIP, (u % UNITS + 1) * STRIP), slice(None))

    def grams(tiles, first, d):
        gs = [gram(t) for t in tiles]

        def put():
            for u, (t, g) in enumerate(zip(tiles, gs), first):
                ref, at = rows_in(u, d)
                ref[at] = kern(t, g)

        return put

    def applies(tiles, first, d):
        for u, t in enumerate(tiles, first):
            ref, at = rows_in(u, d)
            apply(t, ref[at], VT)

    kl_out = pltpu.make_async_copy(KL, k_hbm.at[pl.ds(REMOTE_PLACE[23] * STEP_ROWS, STEP_ROWS)], loc_sem.at[0])
    seq, before, due = state[0], state[1], unflat(state[2:])
    d = begin(seq, before, before)
    put = grams(late[0:2], 0, None)
    applies(due, UNITS, 1 - d)
    put()
    applies(late[0:2], 0, None)
    finish_range(0, N_CHUNK, SB, RB, s1_sem, r1_sem, (2,))
    with jax.named_scope("wait_last"):
        wait_x(7, True)
    with jax.named_scope("last"):
        for c in range(N_CHUNK):
            if c == 3:
                d = begin(seq + 1, jnp.int32(CROSS_PLACE + 10), before)
            put = grams(last[2 * c : 2 * c + 2], 2 * c, d)
            if c > 1:
                applies(last[2 * c - 2 : 2 * c], 2 * c - 2, 1 - d if c == 3 else d)
            put()
            if c == 0:
                applies(last[0:2], 0, d)
            if c != 1:
                finish_range(max(c - 1, 0), max(c, 1), SB, RB, s1_sem, r1_sem)
        put = grams(late[2:6], 2, None)
        applies(last[10:12], 10, d)
        put()
        kl_out.start()
        load_x(4, 0).start()
        middle(0, 1)
        applies(late[2:6], 2, None)
        finish_range(5, 6, SB, RB, s1_sem, r1_sem)

    for h in range(2):
        k_out(seq, 0, h).wait()
        k_out(seq + 1, CROSS_PLACE + 11, h).start()

    def use(k, slot, tile):
        for h in range(2):
            use_step(k, slot, h, functools.partial(tile, h))

    def use_step(k, slot, h, tile):
        for j in range(6):
            r = (6 * h + j) * STRIP
            apply(tile(j), k[slot, r : r + STRIP, 0:CHUNK], YV)

    def quad(t, tile):
        slot = t & 3
        load_x(0, slot).wait()
        load_kb(0, slot).wait()
        t = jnp.int32(t)

        @pl.when(jnp.logical_and(t >= 1, t <= 7))
        def _():
            load_x(10 + 2 * t, (t - 1) & 3).start()

        @pl.when(jnp.logical_and(t >= 1, t <= 6))
        def _():
            load_kb(11 + 2 * t, (t - 1) & 3).start()

        use(X, slot, lambda h, j: tile(0, h, j))
        use(KB, slot, lambda h, j: tile(1, h, j))

    def wait_y(lo, hi):
        def one(c, _):
            two = YV.at[1:3, :, cols_of(c)]
            remote(two, two, sy_sem, ry_sem.at[c], tx).wait_recv()
            return 0

        lax.fori_loop(lo, hi, one, 0)

    def wait_y_par(late):
        part = YV.at[PAR, :, pl.ds((0, 3, 4)[late] * CHUNK, (3, 1, 2)[late] * CHUNK)]
        remote(part, part, sy_sem, ryp_sem.at[late], pt).wait_recv()

    with jax.named_scope("middle"):
        middle(1, 2)
    with jax.named_scope("second_own"):
        first_in.wait()
        for j in range(6):
            apply(own_tile(jnp.int32(0), j, core), KB[0, STEP_ROWS + j * STRIP : STEP_ROWS + (j + 1) * STRIP, :], YV)
        load_kb(5, 0).start()
        middle(2, 3)
        load_kb(0, 1).wait()
        use_step(KB, 1, 0, lambda j: own_tile(jnp.int32(1), j, core))
        wait_y_par(0)
        load_kb(0, 2).wait()
        use_step(KB, 2, 0, lambda j: own_tile(jnp.int32(N_OWN), j, core))
        middle(3, 4)
        use_step(KB, 1, 1, lambda j: own_tile(jnp.int32(2), j, core))
        load_x(6, 1).start()
        load_kb(7, 1).start()
        wait_y_par(1)
        use_step(KB, 2, 1, lambda j: own_tile(jnp.int32(N_OWN + 1), j, core))
        load_x(8, 2).start()
        load_kb(9, 2).start()
        kl_out.wait()
        for h in range(2):
            k_out(seq + 1, 0, h).wait()
        load_x(10, 3).start()
        middle(4, 5)

    def remote_quad(step):
        ps = [step(i) for i in range(4)]
        return lambda d, h, j: remote_tile(ps[2 * d + h], j)

    with jax.named_scope("second_first"):

        wait_y(0, 1)
        quad(0, remote_quad(jnp.int32))
        middle(5, 6)
        load_kb(0, 3).wait()
        use(KB, 3, lambda h, j: own_tile(jnp.int32(3 + h), j, core))
        load_kb(11, 3).start()
        wait_y_par(2)
        wait_y(1, 2)
        quad(1, remote_quad(lambda i: jnp.int32(4 + i)))
    with jax.named_scope("second_cross"):

        def second_cross(t, _):
            with jax.named_scope("wait_y"):
                wait_y(table((2, 2, 2) + Y_NEED[:-1], t), table((2, 2) + Y_NEED, t))

            def tile(d, h, j):
                cross = cross_tile(4 * (t - 2) + 2 * d + h, j)
                return pick(t < 4, cross, last[6 * h + j]) if d else cross

            quad(t, tile)
            return 0

        lax.fori_loop(2, 5, second_cross, 0)

    for k, done in enumerate(((0,), (4, 5), (3,))):
        for c in done:
            finish_range(c, c + 1, SB2, RB2, s2_sem, r2_sem)
        with jax.named_scope("second_chunk"):
            ps = REMOTE_ORDER[4 * k : 4 * k + 4]
            quad(5 + k, remote_quad(lambda i: jnp.int32(ps[i])))

    def finish_strip(n):
        cols = pl.ds(n * STRIP, STRIP)
        for j in range(2):
            s = homes[j][0]
            SB2[j, :, cols] = YT[s, :, cols] + jnp.transpose(YR[s, pl.ds((n + 1) * STRIP, STRIP), :])
        for j in range(2):
            remote(SB2.at[j, :, cols], RB2.at[j, :, cols], s2_sem, r2_sem, homes[j][1]).start()

    with jax.named_scope("second_chunk"):
        finish_range(2, 3, SB2, RB2, s2_sem, r2_sem)
        load_x(0, 0).wait()
        load_kb(0, 0).wait()
        use(X, 0, lambda h, j: remote_tile(jnp.int32(REMOTE_ORDER[12 + h]), j))
        finish_strip(2)
        use(KB, 0, lambda h, j: remote_tile(jnp.int32(REMOTE_ORDER[14 + h]), j))
        finish_strip(3)

    with jax.named_scope("second_par"):
        quad(9, lambda d, h, j: own_tile(jnp.int32(N_OWN + 2 + 2 * d + h), j, core))
        remote(YT.at[PAR], RB2.at[2], s2_sem, r2_sem, pt).start()

    with jax.named_scope("second_end"):
        load_x(0, 2).wait()
        use(X, 2, lambda h, j: own_tile(jnp.int32(5 + h), j, core))

    with jax.named_scope("sent"):
        p_copy.wait_send()
        for j in range(2):
            remote(x_hbm, X.at[1 + j], sx_sem.at[j], rx_sem.at[0], tx).wait_send()
        for buf, sem in ((VT, sv_sem), (NB, sn_sem), (YV, sy_sem)):
            remote(buf.at[1:4], buf.at[1:4], sem, rx_sem.at[0], tx).wait_send()
        remote(SB, RB, s1_sem, rx_sem.at[0], tx).wait_send()

    with jax.named_scope("final"):
        for c in range(N_CHUNK):
            out_ref[:, cols_of(c)] = YT[OWN, :, cols_of(c)] + jnp.transpose(YR[OWN, sums_of(c), :])
        all_sums = remote(SB2, RB2, s2_sem, r2_sem, pt)
        all_sums.wait_send()
        all_sums.wait_recv()


def solution(mesh):
    def local_program(x_loc, v_loc, length_scale, out_scale):
        dma = pltpu.SemaphoreType.DMA
        hbm = pl.BlockSpec(memory_space=pltpu.HBM)
        vmem = pl.BlockSpec(memory_space=pltpu.VMEM)
        smem = pl.BlockSpec(memory_space=pltpu.SMEM)
        own, parts, _ = pl.pallas_call(
            body,
            out_shape=(
                pltpu.VMEM((32, ROWS), F32),
                pltpu.VMEM((3, 32, ROWS), F32),
                jax.ShapeDtypeStruct((N_PLACE * STEP_ROWS, CHUNK), BF16),
            ),
            in_specs=[hbm, hbm, smem, smem],
            out_specs=(vmem, vmem, hbm),
            scratch_shapes=[
                pltpu.VMEM((4, ROWS, 768), BF16),
                pltpu.VMEM((4, 32, ROWS), BF16),
                pltpu.VMEM((4, 32, ROWS), BF16),
                pltpu.VMEM((3, ROWS, 128), F32),
                pltpu.VMEM((4, 1, ROWS), F32),
                pltpu.VMEM((8, CHUNK), F32),
                pltpu.VMEM((3, STRIP + ROWS, 32), F32),
                pltpu.VMEM((5, 32, ROWS), F32),
                pltpu.VMEM((3, 32, ROWS), F32),
                pltpu.VMEM((3, 32, ROWS), F32),
                pltpu.VMEM((3, 32, ROWS), F32),
                pltpu.VMEM((2, HALF_ROWS, CHUNK), BF16),
                pltpu.VMEM((2, HALF_ROWS, CHUNK), BF16),
                pltpu.VMEM((STEP_ROWS, CHUNK), BF16),
                pltpu.VMEM((4, 2 * STEP_ROWS, CHUNK), BF16),
                dma((2,)), dma((8,)), dma, dma((2,)), dma, dma((2,)), dma, dma,
                dma((2,)), dma((2, 2)), dma((4,)), dma((4,)),
                dma, dma((N_CHUNK,)), dma, dma((N_CHUNK,)), dma((3,)), dma, dma,
            ],
            compiler_params=pltpu.CompilerParams(collective_id=0, has_side_effects=True, vmem_limit_bytes=58 * 2**20),
            name="products",
        )(x_loc, v_loc.T, length_scale, out_scale)
        return (own + parts[0] + parts[1] + parts[2]).T

    row_spec = P(("task", "row"), None)
    return jax.shard_map(local_program, mesh=mesh, in_specs=(row_spec, row_spec, P("task"), P("task")), out_specs=row_spec, check_vma=False)
```

```python
import functools

import jax
import jax.numpy as jnp
from jax import lax
from jax.experimental import pallas as pl
from jax.experimental.pallas import tpu as pltpu
from jax.sharding import PartitionSpec as P

MESH = pl.DeviceIdType.MESH
F32, BF16 = jnp.float32, jnp.bfloat16
LOG2E = 1.4426950408889634

ROWS = 3072
STRIP = 256
CHUNK = 512
N_STRIP = ROWS // STRIP
N_CHUNK = ROWS // CHUNK
UNITS = 3
OWN, XNB, YNB, PAR, TRASH = 0, 1, 2, 3, 4

N_OWN, N_PAIR = 7, 13
REMOTE_AT = (0, 7, 13, 18, 21, 21, 23, 23)
REMOTE_TILE = (0, 44, 80, 108, 128, 140)
CROSS_AT = (0, 0, 1, 3, 5, 6, 8, 10)
CROSS_TILE = (0, 0, 2, 4, 8, 12, 18, 24, 32, 40, 50, 60)
OWN_PLACE = (1, 2, 3, 6, 7, 48, 49, 4, 5, 44, 45, 46, 47)
REMOTE_ORDER = (23, 22, 21, 20, 19, 18, 17, 16, 15, 14, 13, 10, 8, 9, 11, 12)
REMOTE_PLACE = tuple(8 + p if p < 8 else 28 + REMOTE_ORDER.index(p) for p in range(24))
CROSS_PLACE = 16
N_PLACE = 50
STEP_ROWS = 6 * STRIP
HALF_ROWS = UNITS * STRIP
Y_NEED = (4, 5, 6)


def table(values, n):
    out = jnp.int32(values[0])
    for i in range(1, len(values)):
        if values[i] != values[i - 1]:
            out = out + (values[i] - values[i - 1]) * (n >= i).astype(jnp.int32)
    return out


def rank(bounds, x):
    out = jnp.int32(0)
    for b in bounds:
        out = out + (x >= b).astype(jnp.int32)
    return out


def pick(cond, a, b):
    return tuple(jnp.where(cond, x, y) for x, y in zip(a, b))


def i32(*xs):
    return tuple(jnp.int32(x) for x in xs)


def own_tile(o, j, core):
    p = 3 * o + j // 2
    c = rank((1, 3, 6, 10, 15), p)
    i = p - ((c * (c + 1)) >> 1)
    own = (jnp.int32(OWN), 2 * i + j % 2, jnp.int32(OWN), c, jnp.where(i == c, TRASH, OWN))
    p = 3 * (o - N_OWN) + j // 2
    c = 1 + rank((1, 3, 6, 10), p)
    i = p - ((c * (c - 1)) >> 1)
    same = core + 2 * (j // 2)
    i, c = pick(p < 15, (i, c), (same, same))
    par = (jnp.int32(OWN), 2 * i + j % 2, jnp.int32(PAR), c, jnp.int32(PAR))
    return pick(o < N_OWN, own, par)


def own_ints(o, j):
    if o < N_OWN:
        pairs = [(i, c) for c in range(N_CHUNK) for i in range(c + 1)]
        i, c = pairs[3 * o + j // 2]
        return (OWN, 2 * i + j % 2, OWN, c, TRASH if i == c else OWN)
    pairs = [(i, c) for c in range(N_CHUNK) for i in range(c)]
    i, c = pairs[3 * (o - N_OWN) + j // 2]
    return (OWN, 2 * i + j % 2, PAR, c, PAR)


def remote_tile(p, j):
    g = 6 * p + j
    d, first = jnp.int32(0), jnp.int32(0)
    for i in range(1, N_CHUNK):
        d, first = pick(g >= REMOTE_TILE[i], (i, REMOTE_TILE[i]), (d, first))
    r = g - first
    rest = r - (22 - 4 * d)
    k, side, odd = pick(rest >= 0, (rest >> 1, r & 1, 1), (r >> 1, r & 1, 0))
    k, side, odd = pick(d == 0, (r >> 2, (r >> 1) & 1, r & 1), (k, side, odd))
    t = jnp.where((k & 1) == (k > 0).astype(jnp.int32), OWN, PAR)
    return (1 + side, 2 * d + odd, t, d + ((k + 1) >> 1), t)


def cross_tile(q, j):
    g = 6 * q + j
    n, first = jnp.int32(1), jnp.int32(0)
    for i in range(2, N_STRIP - 1):
        n, first = pick(g >= CROSS_TILE[i], (i, CROSS_TILE[i]), (n, first))
    r = g - first
    m = n >> 1
    t = pick(r < m, (jnp.int32(XNB), n, jnp.int32(YNB), r, jnp.int32(YNB)), (jnp.int32(YNB), n, jnp.int32(XNB), r - m, jnp.int32(XNB)))
    return pick(r < 2 * m, t, (jnp.int32(XNB), n - 1 + (r - 2 * m), jnp.int32(YNB), m, jnp.int32(YNB)))


def last_tiles():
    n = N_STRIP - 1
    tiles = [t for c in range(N_CHUNK - 1) for t in ((YNB, n, XNB, c, XNB), (XNB, n, YNB, c, YNB))]
    tiles += [(XNB, n - 1, YNB, N_CHUNK - 1, YNB), (XNB, n, YNB, N_CHUNK - 1, YNB)]
    return [i32(*t) for t in tiles]


def span(start, size, unit):
    return pl.ds(start if isinstance(start, int) else pl.multiple_of(start, unit), size)


def rows_of(a):
    return span(a * STRIP, STRIP, STRIP)


def sums_of(c):
    return span(STRIP + c * CHUNK, CHUNK, STRIP)


def cols_of(b):
    return span(b * CHUNK, CHUNK, CHUNK)


def body(
    x_hbm, v_hbm, ell_ref, amp_ref, out_ref, RB2, k_hbm,
    X, VT, YV, NA, NB, CR, YR, YT, SB, RB, SB2, kr0, kr1, KL, KB,
    sx_sem, rx_sem, sv_sem, rv_sem, sn_sem, rn_sem, sp_sem, rp_sem, loc_sem, ko_sem, kb_sem, kx_sem,
    s1_sem, r1_sem, sy_sem, ry_sem, ryp_sem, s2_sem, r2_sem,
):
    me = lax.axis_index("row")
    core, cx, cy = me % 2, (me // 2) % 2, me // 4

    def dev(px, py, pc):
        return {"row": (py * 2 + px) * 2 + pc}

    tx = dev(1 - cx, cy, (core + 1 + cx) % 2)
    ty = dev(cx, 1 - cy, (core + 1 + cx + cy) % 2)
    sx = dev(1 - cx, cy, (core + cx) % 2)
    sy = dev(cx, 1 - cy, (core + cx + cy) % 2)
    pt = dev(cx, cy, 1 - core)

    def remote(src, dst, ss, rs, to):
        return pltpu.make_async_remote_copy(src_ref=src, dst_ref=dst, send_sem=ss, recv_sem=rs, device_id=to, device_id_type=MESH)

    def part_rows(i, late):
        return rows_of(i + 4) if late else cols_of(i)

    def x_copy(j, i, late):
        return remote(x_hbm.at[part_rows(i, late)], X.at[1 + j, part_rows(i, late)], sx_sem.at[j], rx_sem.at[i], (tx, ty)[j])

    def wait_x(i, late):
        two = X.at[1:3, part_rows(i, late)]
        remote(two, two, sx_sem.at[0], rx_sem.at[i], tx).wait_recv()

    p_copy = remote(x_hbm, X.at[PAR], sp_sem, rp_sem, pt)
    v_copies = [remote(v_hbm, VT.at[1 + j], sv_sem, rv_sem.at[j // 2], d) for j, d in enumerate((tx, ty, pt))]
    n_copies = [remote(NB.at[OWN], NB.at[1 + j], sn_sem, rn_sem.at[j // 2], d) for j, d in enumerate((tx, ty, pt))]

    x_loc = pltpu.make_async_copy(x_hbm, X.at[OWN], loc_sem.at[0])
    v_loc = pltpu.make_async_copy(v_hbm, VT.at[OWN], loc_sem.at[1])
    for c in (v_loc, x_loc):
        c.start()

    barrier = pltpu.get_barrier_semaphore()
    for d in (tx, ty, sx, sy, pt):
        pl.semaphore_signal(barrier, inc=1, device_id=d, device_id_type=MESH)
    with jax.named_scope("barrier"):
        pl.semaphore_wait(barrier, 5)

    for c in v_copies:
        c.start()
    for j in range(2):
        x_copy(j, 0, False).start()
    p_copy.start()

    ell = jnp.full((1, CHUNK), ell_ref[0], F32)
    half = LOG2E / (2.0 * ell * ell)
    top = jnp.log2(jnp.full((1, CHUNK), amp_ref[0], F32))
    CR[0:1, :] = 2.0 * half
    CR[1:2, :] = top

    for s in range(3):
        YR[s] = jnp.zeros((STRIP + ROWS, 32), F32)
    for t in range(5):
        YT[t] = jnp.zeros((32, ROWS), F32)
    kr0[...] = jnp.zeros_like(kr0)
    kr1[...] = jnp.zeros_like(kr1)

    v_loc.wait()
    with jax.named_scope("x_local"):
        x_loc.wait()

    def own_norm(c, _):
        r = pl.ds(pl.multiple_of(c * CHUNK, CHUNK), CHUNK)
        x = X[OWN, r, :].astype(F32)
        n = jnp.broadcast_to(0.5 * jnp.sum(x * x, axis=1, keepdims=True), (CHUNK, 128))
        NA[OWN, r, :] = n
        NB[OWN, :, cols_of(c)] = jnp.transpose(n)[0:1, :]
        return 0

    with jax.named_scope("own_norm"):
        lax.fori_loop(0, N_CHUNK, own_norm, 0)
    for c in n_copies:
        c.start()

    for i in range(1, 8):
        for j in range(2):
            x_copy(j, i, i >= 4).start()

    def left_norm(s):
        def one(c, _):
            r = pl.ds(pl.multiple_of(c * CHUNK, CHUNK), CHUNK)
            NA[s, r, :] = jnp.transpose(jnp.broadcast_to(NB[s, :, cols_of(c)], (128, CHUNK)))
            return 0

        lax.fori_loop(0, N_CHUNK, one, 0)

    def gram(tile):
        s, a, t, b, _ = tile
        return lax.dot_general(X[s, rows_of(a), :], X[t, cols_of(b), :], (((1,), (1,)), ((), ())), preferred_element_type=F32)

    def kern(tile, g):
        s, a, t, b, _ = tile
        na = NA[s, rows_of(a), :]
        d = (jnp.concatenate([na] * (CHUNK // 128), axis=1) + NB[t, :, cols_of(b)]) - g
        return jnp.exp2(CR[1:2, :] - jnp.maximum(d, 0.0) * CR[0:1, :]).astype(BF16)

    def apply(tile, k, vec):
        s, a, t, b, to = tile
        YR[s, rows_of(a + 1), :] += lax.dot_general(k, vec[t, :, cols_of(b)], (((1,), (1,)), ((), ())), preferred_element_type=F32)
        if isinstance(to, int) and to == TRASH:
            return
        left = a if isinstance(a, int) else jnp.maximum(a, 0)
        YT[to, :, cols_of(b)] += jnp.dot(vec[s, :, rows_of(left)], k, preferred_element_type=F32)

    def k_out(seq, place, half):
        kr = (kr0, kr1)[half]
        row = pl.multiple_of(place * STEP_ROWS + half * HALF_ROWS, STRIP)
        return pltpu.make_async_copy(kr.at[seq & 1], k_hbm.at[pl.ds(row, HALF_ROWS)], ko_sem.at[seq & 1, half])

    def half_step(prev, cur, kr_new, d_new, kr_old, d_old):
        gs = [gram(t) for t in cur]
        for u in range(UNITS):
            apply(prev[u], kr_old[d_old, u * STRIP : (u + 1) * STRIP, :], VT)
        for u in range(UNITS):
            kr_new[d_new, u * STRIP : (u + 1) * STRIP, :] = kern(cur[u], gs[u])

    def flat(tiles):
        return tuple(x for t in tiles for x in t)

    def unflat(xs):
        return [tuple(xs[5 * u : 5 * u + 5]) for u in range(UNITS)]

    def begin(seq, before, place):
        @pl.when(seq >= 2)
        def _():
            for h in range(2):
                k_out(seq, place, h).wait()

        @pl.when(seq >= 1)
        def _():
            for h in range(2):
                k_out(seq - 1, before, h).start()

        return seq & 1

    def step_of(state, place, tile):
        seq, before, prev = state[0], state[1], state[2:]
        d = begin(seq, before, place)
        first = [tile(u) for u in range(UNITS)]
        second = [tile(UNITS + u) for u in range(UNITS)]
        half_step(unflat(prev), first, kr0, d, kr1, 1 - d)
        half_step(first, second, kr1, d, kr0, d)
        return (seq + 1, place) + flat(second)

    none = flat([i32(OWN, -1, OWN, 0, TRASH)] * UNITS)

    def own_step(o, state):
        @pl.when(o == N_OWN)
        def _():
            p_copy.wait_recv()
            v_copies[2].wait_recv()
            n_copies[2].wait_recv()

        return step_of(state, table(OWN_PLACE, o), lambda j: own_tile(o, j, core))

    def remote_step(p, state):
        return step_of(state, table(REMOTE_PLACE, p), lambda j: remote_tile(p, j))

    def cross_step(q, state):
        return step_of(state, CROSS_PLACE + q, lambda j: cross_tile(q, j))

    with jax.named_scope("pre"):
        state = lax.fori_loop(0, N_PAIR, own_step, i32(0, 0) + none)

    with jax.named_scope("left_norm"):
        remote(VT.at[1:3], VT.at[1:3], sv_sem, rv_sem.at[0], tx).wait_recv()
        remote(NB.at[1:3], NB.at[1:3], sn_sem, rn_sem.at[0], tx).wait_recv()
        for j in range(2):
            left_norm(1 + j)

    def landed(i, state):
        with jax.named_scope("wait_strip"):

            @pl.when(i < 4)
            def _():
                wait_x(i, False)

            @pl.when(i >= 4)
            def _():
                wait_x(i, True)

        with jax.named_scope("strip"):
            state = lax.fori_loop(table(REMOTE_AT, i), table(REMOTE_AT, i + 1), remote_step, state)
            return lax.fori_loop(table(CROSS_AT, i), table(CROSS_AT, i + 1), cross_step, state)

    state = lax.fori_loop(0, 7, landed, state)

    homes = ((XNB, sx), (YNB, sy), (PAR, pt))

    def part_copy(j, c, send, recv, ss, rs):
        return remote(send.at[j, :, cols_of(c)], recv.at[j, :, cols_of(c)], ss, rs.at[c] if send is SB else rs, homes[j][1])

    def finish(j, c, send):
        s = homes[j][0]
        part = YT[s, :, cols_of(c)]
        if j < 2:
            part = part + jnp.transpose(YR[s, sums_of(c), :])
        send[j, :, cols_of(c)] = part
        if send is SB:
            YT[s, :, cols_of(c)] = jnp.zeros((32, CHUNK), F32)
            if j < 2:
                YR[s, sums_of(c), :] = jnp.zeros((CHUNK, 32), F32)

    def finish_range(lo, hi, send, recv, ss, rs, js=(0, 1)):
        for c in range(lo, hi):
            for j in js:
                finish(j, c, send)
            for j in js:
                part_copy(j, c, send, recv, ss, rs).start()

    def load_kb(d, slot):
        return pltpu.make_async_copy(k_hbm.at[pl.ds(pl.multiple_of(d * 2 * STEP_ROWS, STRIP), 2 * STEP_ROWS)], KB.at[slot], kb_sem.at[slot])

    def load_x(d, slot):
        src = k_hbm.at[pl.ds(pl.multiple_of(d * 2 * STEP_ROWS, STRIP), 2 * STEP_ROWS)]
        return pltpu.make_async_copy(src, X.at[slot, :, 0:CHUNK], kx_sem.at[slot])

    first_in = pltpu.make_async_copy(k_hbm.at[pl.ds(STEP_ROWS, STEP_ROWS)], KB.at[0, pl.ds(STEP_ROWS, STEP_ROWS)], kb_sem.at[0])
    first_in.start()
    for i in range(1, 4):
        load_kb(i, i).start()

    def y_copy(j, c):
        done = ryp_sem.at[(c >= 3) + (c >= 4)] if j == 2 else ry_sem.at[c]
        return remote(YV.at[OWN, :, cols_of(c)], YV.at[1 + j, :, cols_of(c)], sy_sem, done, (tx, ty, pt)[j])

    def middle(c):
        with jax.named_scope("wait_part"):
            three = RB.at[:, :, cols_of(c)]
            remote(three, three, s1_sem, r1_sem.at[c], pt).wait_recv()
        y = YT[OWN, :, cols_of(c)] + jnp.transpose(YR[OWN, sums_of(c), :])
        y = y + RB[0, :, cols_of(c)] + RB[1, :, cols_of(c)] + RB[2, :, cols_of(c)]
        YV[OWN, :, cols_of(c)] = y.astype(BF16)
        YT[OWN, :, cols_of(c)] = jnp.zeros((32, CHUNK), F32)
        YR[OWN, sums_of(c), :] = jnp.zeros((CHUNK, 32), F32)
        for j in range(3):
            y_copy(j, c).start()

    last = last_tiles()
    late = [remote_tile(jnp.int32(23), j) for j in range(6)]

    def rows_in(u, d):
        if d is None:
            return KL, (slice(u * STRIP, (u + 1) * STRIP), slice(None))
        return (kr0, kr1)[u % 6 // UNITS], (d, slice(u % UNITS * STRIP, (u % UNITS + 1) * STRIP), slice(None))

    def grams(tiles, first, d):
        gs = [gram(t) for t in tiles]

        def put():
            for u, (t, g) in enumerate(zip(tiles, gs), first):
                ref, at = rows_in(u, d)
                ref[at] = kern(t, g)

        return put

    def applies(tiles, first, d):
        for u, t in enumerate(tiles, first):
            ref, at = rows_in(u, d)
            apply(t, ref[at], VT)

    kl_out = pltpu.make_async_copy(KL, k_hbm.at[pl.ds(REMOTE_PLACE[23] * STEP_ROWS, STEP_ROWS)], loc_sem.at[0])
    seq, before, due = state[0], state[1], unflat(state[2:])
    d = begin(seq, before, before)
    put = grams(late[0:2], 0, None)
    applies(due, UNITS, 1 - d)
    put()
    applies(late[0:2], 0, None)
    finish_range(0, N_CHUNK, SB, RB, s1_sem, r1_sem, (2,))
    with jax.named_scope("wait_last"):
        wait_x(7, True)
    with jax.named_scope("last"):
        for c in range(N_CHUNK):
            if c == 3:
                d = begin(seq + 1, jnp.int32(CROSS_PLACE + 10), before)
            put = grams(last[2 * c : 2 * c + 2], 2 * c, d)
            if c > 1:
                applies(last[2 * c - 2 : 2 * c], 2 * c - 2, 1 - d if c == 3 else d)
            put()
            if c == 0:
                applies(last[0:2], 0, d)
            if c != 1:
                finish_range(max(c - 1, 0), max(c, 1), SB, RB, s1_sem, r1_sem)
        put = grams(late[2:6], 2, None)
        applies(last[10:12], 10, d)
        put()
        kl_out.start()
        load_x(4, 0).start()
        middle(0)
        applies(late[2:6], 2, None)
        finish_range(5, 6, SB, RB, s1_sem, r1_sem)

    for h in range(2):
        k_out(seq, 0, h).wait()
        k_out(seq + 1, CROSS_PLACE + 11, h).start()

    def use(k, slot, tile):
        for h in range(2):
            use_step(k, slot, h, functools.partial(tile, h))

    def use_step(k, slot, h, tile):
        for j in range(6):
            r = (6 * h + j) * STRIP
            apply(tile(j), k[slot, r : r + STRIP, 0:CHUNK], YV)

    def quad(t, tile):
        slot = t & 3
        load_x(0, slot).wait()
        load_kb(0, slot).wait()
        t = jnp.int32(t)

        @pl.when(jnp.logical_and(t >= 1, t <= 7))
        def _():
            load_x(10 + 2 * t, (t - 1) & 3).start()

        @pl.when(jnp.logical_and(t >= 1, t <= 6))
        def _():
            load_kb(11 + 2 * t, (t - 1) & 3).start()

        use(X, slot, lambda h, j: tile(0, h, j))
        use(KB, slot, lambda h, j: tile(1, h, j))

    def wait_y_one(c):
        two = YV.at[1:3, :, cols_of(c)]
        remote(two, two, sy_sem, ry_sem.at[c], tx).wait_recv()

    def wait_y(lo, hi):
        def one(c, _):
            wait_y_one(c)
            return 0

        lax.fori_loop(lo, hi, one, 0)

    def wait_y_par(late):
        part = YV.at[PAR, :, pl.ds((0, 3, 4)[late] * CHUNK, (3, 1, 2)[late] * CHUNK)]
        remote(part, part, sy_sem, ryp_sem.at[late], pt).wait_recv()

    with jax.named_scope("middle"):
        middle(1)
    with jax.named_scope("second_own"):
        first_in.wait()
        for j in range(6):
            apply(own_ints(0, j), KB[0, STEP_ROWS + j * STRIP : STEP_ROWS + (j + 1) * STRIP, :], YV)
        load_kb(5, 0).start()
        middle(2)
        load_kb(0, 1).wait()
        use_step(KB, 1, 0, lambda j: own_ints(1, j))
        wait_y_par(0)
        load_kb(0, 2).wait()
        use_step(KB, 2, 0, lambda j: own_ints(N_OWN, j))
        middle(3)
        use_step(KB, 1, 1, lambda j: own_ints(2, j))
        load_x(6, 1).start()
        load_kb(7, 1).start()
        wait_y_par(1)
        use_step(KB, 2, 1, lambda j: own_ints(N_OWN + 1, j))
        load_x(8, 2).start()
        load_kb(9, 2).start()
        kl_out.wait()
        for h in range(2):
            k_out(seq + 1, 0, h).wait()
        load_x(10, 3).start()
        middle(4)

    def remote_quad(step):
        ps = [step(i) for i in range(4)]
        return lambda d, h, j: remote_tile(ps[2 * d + h], j)

    with jax.named_scope("second_first"):

        wait_y_one(0)
        quad(0, remote_quad(jnp.int32))
        middle(5)
        load_kb(0, 3).wait()
        use(KB, 3, lambda h, j: own_ints(3 + h, j))
        load_kb(11, 3).start()
        wait_y_par(2)
        wait_y_one(1)
        quad(1, remote_quad(lambda i: jnp.int32(4 + i)))
    with jax.named_scope("second_cross"):

        def second_cross(t, _):
            with jax.named_scope("wait_y"):
                wait_y(table((2, 2, 2) + Y_NEED[:-1], t), table((2, 2) + Y_NEED, t))

            def tile(d, h, j):
                cross = cross_tile(4 * (t - 2) + 2 * d + h, j)
                return pick(t < 4, cross, last[6 * h + j]) if d else cross

            quad(t, tile)
            return 0

        lax.fori_loop(2, 5, second_cross, 0)

    for k, done in enumerate(((0,), (4, 5), (3,))):
        for c in done:
            finish_range(c, c + 1, SB2, RB2, s2_sem, r2_sem)
        with jax.named_scope("second_chunk"):
            ps = REMOTE_ORDER[4 * k : 4 * k + 4]
            quad(5 + k, remote_quad(lambda i: jnp.int32(ps[i])))

    def finish_strip(n):
        cols = pl.ds(n * STRIP, STRIP)
        for j in range(2):
            s = homes[j][0]
            SB2[j, :, cols] = YT[s, :, cols] + jnp.transpose(YR[s, pl.ds((n + 1) * STRIP, STRIP), :])
        for j in range(2):
            remote(SB2.at[j, :, cols], RB2.at[j, :, cols], s2_sem, r2_sem, homes[j][1]).start()

    with jax.named_scope("second_chunk"):
        finish_range(2, 3, SB2, RB2, s2_sem, r2_sem)
        load_x(0, 0).wait()
        load_kb(0, 0).wait()
        use(X, 0, lambda h, j: remote_tile(jnp.int32(REMOTE_ORDER[12 + h]), j))
        finish_strip(2)
        use(KB, 0, lambda h, j: remote_tile(jnp.int32(REMOTE_ORDER[14 + h]), j))
        finish_strip(3)

    with jax.named_scope("second_par"):
        quad(9, lambda d, h, j: own_tile(jnp.int32(N_PAIR - 1), j, core) if d and h else own_ints(N_OWN + 2 + 2 * d + h, j))
        remote(YT.at[PAR], RB2.at[2], s2_sem, r2_sem, pt).start()

    with jax.named_scope("sent"):
        p_copy.wait_send()
        for j in range(2):
            remote(x_hbm, X.at[1 + j], sx_sem.at[j], rx_sem.at[0], tx).wait_send()
        for buf, sem in ((VT, sv_sem), (NB, sn_sem), (YV, sy_sem)):
            remote(buf.at[1:4], buf.at[1:4], sem, rx_sem.at[0], tx).wait_send()
        remote(SB, RB, s1_sem, rx_sem.at[0], tx).wait_send()

    with jax.named_scope("second_end"):
        load_x(0, 2).wait()
        use(X, 2, lambda h, j: own_ints(5 + h, j))

    with jax.named_scope("final"):
        for c in range(N_CHUNK):
            out_ref[:, cols_of(c)] = YT[OWN, :, cols_of(c)] + jnp.transpose(YR[OWN, sums_of(c), :])
        all_sums = remote(SB2, RB2, s2_sem, r2_sem, pt)
        all_sums.wait_send()
        all_sums.wait_recv()


def solution(mesh):
    def local_program(x_loc, v_loc, length_scale, out_scale):
        dma = pltpu.SemaphoreType.DMA
        hbm = pl.BlockSpec(memory_space=pltpu.HBM)
        vmem = pl.BlockSpec(memory_space=pltpu.VMEM)
        smem = pl.BlockSpec(memory_space=pltpu.SMEM)
        own, parts, _ = pl.pallas_call(
            body,
            out_shape=(
                pltpu.VMEM((32, ROWS), F32),
                pltpu.VMEM((3, 32, ROWS), F32),
                jax.ShapeDtypeStruct((N_PLACE * STEP_ROWS, CHUNK), BF16),
            ),
            in_specs=[hbm, hbm, smem, smem],
            out_specs=(vmem, vmem, hbm),
            scratch_shapes=[
                pltpu.VMEM((4, ROWS, 768), BF16),
                pltpu.VMEM((4, 32, ROWS), BF16),
                pltpu.VMEM((4, 32, ROWS), BF16),
                pltpu.VMEM((3, ROWS, 128), F32),
                pltpu.VMEM((4, 1, ROWS), F32),
                pltpu.VMEM((8, CHUNK), F32),
                pltpu.VMEM((3, STRIP + ROWS, 32), F32),
                pltpu.VMEM((5, 32, ROWS), F32),
                pltpu.VMEM((3, 32, ROWS), F32),
                pltpu.VMEM((3, 32, ROWS), F32),
                pltpu.VMEM((3, 32, ROWS), F32),
                pltpu.VMEM((2, HALF_ROWS, CHUNK), BF16),
                pltpu.VMEM((2, HALF_ROWS, CHUNK), BF16),
                pltpu.VMEM((STEP_ROWS, CHUNK), BF16),
                pltpu.VMEM((4, 2 * STEP_ROWS, CHUNK), BF16),
                dma((2,)), dma((8,)), dma, dma((2,)), dma, dma((2,)), dma, dma,
                dma((2,)), dma((2, 2)), dma((4,)), dma((4,)),
                dma, dma((N_CHUNK,)), dma, dma((N_CHUNK,)), dma((3,)), dma, dma,
            ],
            compiler_params=pltpu.CompilerParams(collective_id=0, has_side_effects=True, vmem_limit_bytes=58 * 2**20),
            name="products",
        )(x_loc, v_loc.T, length_scale, out_scale)
        return (own + parts[0] + parts[1] + parts[2]).T

    row_spec = P(("task", "row"), None)
    return jax.shard_map(local_program, mesh=mesh, in_specs=(row_spec, row_spec, P("task"), P("task")), out_specs=row_spec, check_vma=False)
```

```python
import functools

import jax
import jax.numpy as jnp
from jax import lax
from jax.experimental import pallas as pl
from jax.experimental.pallas import tpu as pltpu
from jax.sharding import PartitionSpec as P

MESH = pl.DeviceIdType.MESH
F32, BF16 = jnp.float32, jnp.bfloat16
LOG2E = 1.4426950408889634

ROWS = 3072
STRIP = 256
CHUNK = 512
N_STRIP = ROWS // STRIP
N_CHUNK = ROWS // CHUNK
UNITS = 3
OWN, XNB, YNB, PAR, TRASH = 0, 1, 2, 3, 4

N_OWN, N_PAIR = 7, 13
REMOTE_AT = (0, 7, 13, 18, 21, 21, 23, 23)
REMOTE_TILE = (0, 44, 80, 108, 128, 140)
CROSS_AT = (0, 0, 1, 3, 5, 6, 8, 10)
CROSS_TILE = (0, 0, 2, 4, 8, 12, 18, 24, 32, 40, 50, 60)
OWN_PLACE = (1, 2, 3, 6, 7, 48, 49, 4, 5, 44, 45, 46, 47)
REMOTE_ORDER = (23, 22, 21, 20, 19, 18, 17, 16, 15, 14, 13, 10, 8, 9, 11, 12)
REMOTE_PLACE = tuple(8 + p if p < 8 else 28 + REMOTE_ORDER.index(p) for p in range(24))
CROSS_PLACE = 16
N_PLACE = 50
STEP_ROWS = 6 * STRIP
HALF_ROWS = UNITS * STRIP
Y_NEED = (4, 5, 6)


def table(values, n):
    out = jnp.int32(values[0])
    for i in range(1, len(values)):
        if values[i] != values[i - 1]:
            out = out + (values[i] - values[i - 1]) * (n >= i).astype(jnp.int32)
    return out


def rank(bounds, x):
    out = jnp.int32(0)
    for b in bounds:
        out = out + (x >= b).astype(jnp.int32)
    return out


def pick(cond, a, b):
    return tuple(jnp.where(cond, x, y) for x, y in zip(a, b))


def i32(*xs):
    return tuple(jnp.int32(x) for x in xs)


def own_tile(o, j, core):
    p = 3 * o + j // 2
    c = rank((1, 3, 6, 10, 15), p)
    i = p - ((c * (c + 1)) >> 1)
    own = (jnp.int32(OWN), 2 * i + j % 2, jnp.int32(OWN), c, jnp.where(i == c, TRASH, OWN))
    p = 3 * (o - N_OWN) + j // 2
    c = 1 + rank((1, 3, 6, 10), p)
    i = p - ((c * (c - 1)) >> 1)
    same = core + 2 * (j // 2)
    i, c = pick(p < 15, (i, c), (same, same))
    par = (jnp.int32(OWN), 2 * i + j % 2, jnp.int32(PAR), c, jnp.int32(PAR))
    return pick(o < N_OWN, own, par)


def own_ints(o, j):
    if o < N_OWN:
        pairs = [(i, c) for c in range(N_CHUNK) for i in range(c + 1)]
        i, c = pairs[3 * o + j // 2]
        return (OWN, 2 * i + j % 2, OWN, c, TRASH if i == c else OWN)
    pairs = [(i, c) for c in range(N_CHUNK) for i in range(c)]
    i, c = pairs[3 * (o - N_OWN) + j // 2]
    return (OWN, 2 * i + j % 2, PAR, c, PAR)


def remote_tile(p, j):
    g = 6 * p + j
    d, first = jnp.int32(0), jnp.int32(0)
    for i in range(1, N_CHUNK):
        d, first = pick(g >= REMOTE_TILE[i], (i, REMOTE_TILE[i]), (d, first))
    r = g - first
    rest = r - (22 - 4 * d)
    k, side, odd = pick(rest >= 0, (rest >> 1, r & 1, 1), (r >> 1, r & 1, 0))
    k, side, odd = pick(d == 0, (r >> 2, (r >> 1) & 1, r & 1), (k, side, odd))
    t = jnp.where((k & 1) == (k > 0).astype(jnp.int32), OWN, PAR)
    return (1 + side, 2 * d + odd, t, d + ((k + 1) >> 1), t)


def cross_tile(q, j):
    g = 6 * q + j
    n, first = jnp.int32(1), jnp.int32(0)
    for i in range(2, N_STRIP - 1):
        n, first = pick(g >= CROSS_TILE[i], (i, CROSS_TILE[i]), (n, first))
    r = g - first
    m = n >> 1
    t = pick(r < m, (jnp.int32(XNB), n, jnp.int32(YNB), r, jnp.int32(YNB)), (jnp.int32(YNB), n, jnp.int32(XNB), r - m, jnp.int32(XNB)))
    return pick(r < 2 * m, t, (jnp.int32(XNB), n - 1 + (r - 2 * m), jnp.int32(YNB), m, jnp.int32(YNB)))


def last_tiles():
    n = N_STRIP - 1
    tiles = [t for c in range(N_CHUNK - 1) for t in ((YNB, n, XNB, c, XNB), (XNB, n, YNB, c, YNB))]
    tiles += [(XNB, n - 1, YNB, N_CHUNK - 1, YNB), (XNB, n, YNB, N_CHUNK - 1, YNB)]
    return [i32(*t) for t in tiles]


def span(start, size, unit):
    return pl.ds(start if isinstance(start, int) else pl.multiple_of(start, unit), size)


def rows_of(a):
    return span(a * STRIP, STRIP, STRIP)


def sums_of(c):
    return span(STRIP + c * CHUNK, CHUNK, STRIP)


def cols_of(b):
    return span(b * CHUNK, CHUNK, CHUNK)


def body(
    x_hbm, v_hbm, ell_ref, amp_ref, out_ref, RB2, k_hbm,
    X, VT, YV, NA, NB, CR, YR, YT, SB, RB, SB2, kr0, kr1, KL, KB,
    sx_sem, rx_sem, sv_sem, rv_sem, sn_sem, rn_sem, sp_sem, rp_sem, loc_sem, ko_sem, kb_sem, kx_sem,
    s1_sem, r1_sem, sy_sem, ry_sem, ryp_sem, s2_sem, r2_sem,
):
    me = lax.axis_index("row")
    core, cx, cy = me % 2, (me // 2) % 2, me // 4

    def dev(px, py, pc):
        return {"row": (py * 2 + px) * 2 + pc}

    tx = dev(1 - cx, cy, (core + 1 + cx) % 2)
    ty = dev(cx, 1 - cy, (core + 1 + cx + cy) % 2)
    sx = dev(1 - cx, cy, (core + cx) % 2)
    sy = dev(cx, 1 - cy, (core + cx + cy) % 2)
    pt = dev(cx, cy, 1 - core)

    def remote(src, dst, ss, rs, to):
        return pltpu.make_async_remote_copy(src_ref=src, dst_ref=dst, send_sem=ss, recv_sem=rs, device_id=to, device_id_type=MESH)

    def part_rows(i, late):
        return rows_of(i + 4) if late else cols_of(i)

    def x_copy(j, i, late):
        return remote(x_hbm.at[part_rows(i, late)], X.at[1 + j, part_rows(i, late)], sx_sem.at[j], rx_sem.at[i], (tx, ty)[j])

    def wait_x(i, late):
        two = X.at[1:3, part_rows(i, late)]
        remote(two, two, sx_sem.at[0], rx_sem.at[i], tx).wait_recv()

    p_copy = remote(x_hbm, X.at[PAR], sp_sem, rp_sem, pt)
    v_copies = [remote(v_hbm, VT.at[1 + j], sv_sem, rv_sem.at[j // 2], d) for j, d in enumerate((tx, ty, pt))]
    n_copies = [remote(NB.at[OWN], NB.at[1 + j], sn_sem, rn_sem.at[j // 2], d) for j, d in enumerate((tx, ty, pt))]

    x_loc = pltpu.make_async_copy(x_hbm, X.at[OWN], loc_sem.at[0])
    v_loc = pltpu.make_async_copy(v_hbm, VT.at[OWN], loc_sem.at[1])
    for c in (v_loc, x_loc):
        c.start()

    barrier = pltpu.get_barrier_semaphore()
    for d in (tx, ty, sx, sy, pt):
        pl.semaphore_signal(barrier, inc=1, device_id=d, device_id_type=MESH)
    with jax.named_scope("barrier"):
        pl.semaphore_wait(barrier, 5)

    for c in v_copies:
        c.start()
    for j in range(2):
        x_copy(j, 0, False).start()
    p_copy.start()

    ell = jnp.full((1, CHUNK), ell_ref[0], F32)
    half = LOG2E / (2.0 * ell * ell)
    top = jnp.log2(jnp.full((1, CHUNK), amp_ref[0], F32))
    CR[0:1, :] = 2.0 * half
    CR[1:2, :] = top

    for s in range(3):
        YR[s] = jnp.zeros((STRIP + ROWS, 32), F32)
    for t in range(5):
        YT[t] = jnp.zeros((32, ROWS), F32)
    kr0[...] = jnp.zeros_like(kr0)
    kr1[...] = jnp.zeros_like(kr1)

    v_loc.wait()
    with jax.named_scope("x_local"):
        x_loc.wait()

    def own_norm(c, _):
        r = pl.ds(pl.multiple_of(c * CHUNK, CHUNK), CHUNK)
        x = X[OWN, r, :].astype(F32)
        n = jnp.broadcast_to(0.5 * jnp.sum(x * x, axis=1, keepdims=True), (CHUNK, 128))
        NA[OWN, r, :] = n
        NB[OWN, :, cols_of(c)] = jnp.transpose(n)[0:1, :]
        return 0

    with jax.named_scope("own_norm"):
        lax.fori_loop(0, N_CHUNK, own_norm, 0)
    for c in n_copies:
        c.start()

    for i in range(1, 8):
        for j in range(2):
            x_copy(j, i, i >= 4).start()

    def left_norm(s):
        def one(c, _):
            r = pl.ds(pl.multiple_of(c * CHUNK, CHUNK), CHUNK)
            NA[s, r, :] = jnp.transpose(jnp.broadcast_to(NB[s, :, cols_of(c)], (128, CHUNK)))
            return 0

        lax.fori_loop(0, N_CHUNK, one, 0)

    def gram(tile):
        s, a, t, b, _ = tile
        return lax.dot_general(X[s, rows_of(a), :], X[t, cols_of(b), :], (((1,), (1,)), ((), ())), preferred_element_type=F32)

    def kern(tile, g):
        s, a, t, b, _ = tile
        na = NA[s, rows_of(a), :]
        d = (jnp.concatenate([na] * (CHUNK // 128), axis=1) + NB[t, :, cols_of(b)]) - g
        return jnp.exp2(CR[1:2, :] - jnp.maximum(d, 0.0) * CR[0:1, :]).astype(BF16)

    def apply(tile, k, vec):
        s, a, t, b, to = tile
        YR[s, rows_of(a + 1), :] += lax.dot_general(k, vec[t, :, cols_of(b)], (((1,), (1,)), ((), ())), preferred_element_type=F32)
        if isinstance(to, int) and to == TRASH:
            return
        left = a if isinstance(a, int) else jnp.maximum(a, 0)
        YT[to, :, cols_of(b)] += jnp.dot(vec[s, :, rows_of(left)], k, preferred_element_type=F32)

    def k_out(seq, place, half):
        kr = (kr0, kr1)[half]
        row = pl.multiple_of(place * STEP_ROWS + half * HALF_ROWS, STRIP)
        return pltpu.make_async_copy(kr.at[seq & 1], k_hbm.at[pl.ds(row, HALF_ROWS)], ko_sem.at[seq & 1, half])

    def half_step(prev, cur, kr_new, d_new, kr_old, d_old):
        gs = [gram(t) for t in cur]
        for u in range(UNITS):
            apply(prev[u], kr_old[d_old, u * STRIP : (u + 1) * STRIP, :], VT)
        for u in range(UNITS):
            kr_new[d_new, u * STRIP : (u + 1) * STRIP, :] = kern(cur[u], gs[u])

    def flat(tiles):
        return tuple(x for t in tiles for x in t)

    def unflat(xs):
        return [tuple(xs[5 * u : 5 * u + 5]) for u in range(UNITS)]

    def begin(seq, before, place):
        @pl.when(seq >= 2)
        def _():
            for h in range(2):
                k_out(seq, place, h).wait()

        @pl.when(seq >= 1)
        def _():
            for h in range(2):
                k_out(seq - 1, before, h).start()

        return seq & 1

    def step_of(state, place, tile):
        seq, before, prev = state[0], state[1], state[2:]
        d = begin(seq, before, place)
        first = [tile(u) for u in range(UNITS)]
        second = [tile(UNITS + u) for u in range(UNITS)]
        half_step(unflat(prev), first, kr0, d, kr1, 1 - d)
        half_step(first, second, kr1, d, kr0, d)
        return (seq + 1, place) + flat(second)

    none = flat([i32(OWN, -1, OWN, 0, TRASH)] * UNITS)

    def own_step(o, state):
        @pl.when(o == N_OWN)
        def _():
            p_copy.wait_recv()
            v_copies[2].wait_recv()
            n_copies[2].wait_recv()

        return step_of(state, table(OWN_PLACE, o), lambda j: own_tile(o, j, core))

    def remote_step(p, state):
        return step_of(state, table(REMOTE_PLACE, p), lambda j: remote_tile(p, j))

    def cross_step(q, state):
        return step_of(state, CROSS_PLACE + q, lambda j: cross_tile(q, j))

    with jax.named_scope("pre"):
        state = lax.fori_loop(0, N_PAIR, own_step, i32(0, 0) + none)

    with jax.named_scope("left_norm"):
        remote(VT.at[1:3], VT.at[1:3], sv_sem, rv_sem.at[0], tx).wait_recv()
        remote(NB.at[1:3], NB.at[1:3], sn_sem, rn_sem.at[0], tx).wait_recv()
        for j in range(2):
            left_norm(1 + j)

    def landed(i, state):
        with jax.named_scope("wait_strip"):

            @pl.when(i < 4)
            def _():
                wait_x(i, False)

            @pl.when(i >= 4)
            def _():
                wait_x(i, True)

        with jax.named_scope("strip"):
            state = lax.fori_loop(table(REMOTE_AT, i), table(REMOTE_AT, i + 1), remote_step, state)
            return lax.fori_loop(table(CROSS_AT, i), table(CROSS_AT, i + 1), cross_step, state)

    state = lax.fori_loop(0, 7, landed, state)

    homes = ((XNB, sx), (YNB, sy), (PAR, pt))

    def part_copy(j, c, send, recv, ss, rs):
        return remote(send.at[j, :, cols_of(c)], recv.at[j, :, cols_of(c)], ss, rs.at[c] if send is SB else rs, homes[j][1])

    def finish(j, c, send):
        s = homes[j][0]
        part = YT[s, :, cols_of(c)]
        if j < 2:
            part = part + jnp.transpose(YR[s, sums_of(c), :])
        send[j, :, cols_of(c)] = part
        if send is SB:
            YT[s, :, cols_of(c)] = jnp.zeros((32, CHUNK), F32)
            if j < 2:
                YR[s, sums_of(c), :] = jnp.zeros((CHUNK, 32), F32)

    def finish_range(lo, hi, send, recv, ss, rs, js=(0, 1)):
        for c in range(lo, hi):
            for j in js:
                finish(j, c, send)
            for j in js:
                part_copy(j, c, send, recv, ss, rs).start()

    def load_kb(d, slot):
        return pltpu.make_async_copy(k_hbm.at[pl.ds(pl.multiple_of(d * 2 * STEP_ROWS, STRIP), 2 * STEP_ROWS)], KB.at[slot], kb_sem.at[slot])

    def load_x(d, slot):
        src = k_hbm.at[pl.ds(pl.multiple_of(d * 2 * STEP_ROWS, STRIP), 2 * STEP_ROWS)]
        return pltpu.make_async_copy(src, X.at[slot, :, 0:CHUNK], kx_sem.at[slot])

    first_in = pltpu.make_async_copy(k_hbm.at[pl.ds(STEP_ROWS, STEP_ROWS)], KB.at[0, pl.ds(STEP_ROWS, STEP_ROWS)], kb_sem.at[0])
    first_in.start()
    for i in range(1, 4):
        load_kb(i, i).start()

    def y_copy(j, c):
        done = ryp_sem.at[(c >= 3) + (c >= 4)] if j == 2 else ry_sem.at[c]
        return remote(YV.at[OWN, :, cols_of(c)], YV.at[1 + j, :, cols_of(c)], sy_sem, done, (tx, ty, pt)[j])

    def middle(c):
        with jax.named_scope("wait_part"):
            three = RB.at[:, :, cols_of(c)]
            remote(three, three, s1_sem, r1_sem.at[c], pt).wait_recv()
        y = YT[OWN, :, cols_of(c)] + jnp.transpose(YR[OWN, sums_of(c), :])
        y = y + RB[0, :, cols_of(c)] + RB[1, :, cols_of(c)] + RB[2, :, cols_of(c)]
        YV[OWN, :, cols_of(c)] = y.astype(BF16)
        YT[OWN, :, cols_of(c)] = jnp.zeros((32, CHUNK), F32)
        YR[OWN, sums_of(c), :] = jnp.zeros((CHUNK, 32), F32)
        for j in range(3):
            y_copy(j, c).start()

    last = last_tiles()
    late = [remote_tile(jnp.int32(23), j) for j in range(6)]

    def rows_in(u, d):
        if d is None:
            return KL, (slice(u * STRIP, (u + 1) * STRIP), slice(None))
        return (kr0, kr1)[u % 6 // UNITS], (d, slice(u % UNITS * STRIP, (u % UNITS + 1) * STRIP), slice(None))

    def grams(tiles, first, d):
        gs = [gram(t) for t in tiles]

        def put():
            for u, (t, g) in enumerate(zip(tiles, gs), first):
                ref, at = rows_in(u, d)
                ref[at] = kern(t, g)

        return put

    def applies(tiles, first, d):
        for u, t in enumerate(tiles, first):
            ref, at = rows_in(u, d)
            apply(t, ref[at], VT)

    kl_out = pltpu.make_async_copy(KL, k_hbm.at[pl.ds(REMOTE_PLACE[23] * STEP_ROWS, STEP_ROWS)], loc_sem.at[0])
    seq, before, due = state[0], state[1], unflat(state[2:])
    d = begin(seq, before, before)
    put = grams(late[0:2], 0, None)
    applies(due, UNITS, 1 - d)
    put()
    put = grams(late[2:4], 2, None)
    applies(late[0:2], 0, None)
    put()
    applies(late[2:4], 2, None)
    finish_range(0, N_CHUNK, SB, RB, s1_sem, r1_sem, (2,))
    with jax.named_scope("wait_last"):
        wait_x(7, True)
    with jax.named_scope("last"):
        for c in range(N_CHUNK):
            if c == 3:
                d = begin(seq + 1, jnp.int32(CROSS_PLACE + 10), before)
            put = grams(last[2 * c : 2 * c + 2], 2 * c, d)
            if c > 1:
                applies(last[2 * c - 2 : 2 * c], 2 * c - 2, 1 - d if c == 3 else d)
            put()
            if c == 0:
                applies(last[0:2], 0, d)
            if c != 1:
                finish_range(max(c - 1, 0), max(c, 1), SB, RB, s1_sem, r1_sem)
        put = grams(late[4:6], 4, None)
        applies(last[10:12], 10, d)
        put()
        kl_out.start()
        load_x(4, 0).start()
        middle(0)
        applies(late[4:6], 4, None)
        finish_range(5, 6, SB, RB, s1_sem, r1_sem)

    for h in range(2):
        k_out(seq, 0, h).wait()
        k_out(seq + 1, CROSS_PLACE + 11, h).start()

    def use(k, slot, tile):
        for h in range(2):
            use_step(k, slot, h, functools.partial(tile, h))

    def use_step(k, slot, h, tile):
        for j in range(6):
            r = (6 * h + j) * STRIP
            apply(tile(j), k[slot, r : r + STRIP, 0:CHUNK], YV)

    def quad(t, tile):
        slot = t & 3
        load_x(0, slot).wait()
        load_kb(0, slot).wait()
        t = jnp.int32(t)

        @pl.when(jnp.logical_and(t >= 1, t <= 7))
        def _():
            load_x(10 + 2 * t, (t - 1) & 3).start()

        @pl.when(jnp.logical_and(t >= 1, t <= 6))
        def _():
            load_kb(11 + 2 * t, (t - 1) & 3).start()

        use(X, slot, lambda h, j: tile(0, h, j))
        use(KB, slot, lambda h, j: tile(1, h, j))

    def wait_y_one(c):
        two = YV.at[1:3, :, cols_of(c)]
        remote(two, two, sy_sem, ry_sem.at[c], tx).wait_recv()

    def wait_y(lo, hi):
        def one(c, _):
            wait_y_one(c)
            return 0

        lax.fori_loop(lo, hi, one, 0)

    def wait_y_par(late):
        part = YV.at[PAR, :, pl.ds((0, 3, 4)[late] * CHUNK, (3, 1, 2)[late] * CHUNK)]
        remote(part, part, sy_sem, ryp_sem.at[late], pt).wait_recv()

    with jax.named_scope("middle"):
        middle(1)
    with jax.named_scope("second_own"):
        first_in.wait()
        for j in range(6):
            apply(own_ints(0, j), KB[0, STEP_ROWS + j * STRIP : STEP_ROWS + (j + 1) * STRIP, :], YV)
        load_kb(5, 0).start()
        middle(2)
        load_kb(0, 1).wait()
        use_step(KB, 1, 0, lambda j: own_ints(1, j))
        wait_y_par(0)
        load_kb(0, 2).wait()
        use_step(KB, 2, 0, lambda j: own_ints(N_OWN, j))
        middle(3)
        use_step(KB, 1, 1, lambda j: own_ints(2, j))
        load_x(6, 1).start()
        load_kb(7, 1).start()
        wait_y_par(1)
        use_step(KB, 2, 1, lambda j: own_ints(N_OWN + 1, j))
        load_x(8, 2).start()
        load_kb(9, 2).start()
        kl_out.wait()
        for h in range(2):
            k_out(seq + 1, 0, h).wait()
        load_x(10, 3).start()
        middle(4)

    def remote_quad(step):
        ps = [step(i) for i in range(4)]
        return lambda d, h, j: remote_tile(ps[2 * d + h], j)

    with jax.named_scope("second_first"):

        wait_y_one(0)
        quad(0, remote_quad(jnp.int32))
        middle(5)
        load_kb(0, 3).wait()
        use(KB, 3, lambda h, j: own_ints(3 + h, j))
        load_kb(11, 3).start()
        wait_y_par(2)
        wait_y_one(1)
        quad(1, remote_quad(lambda i: jnp.int32(4 + i)))
    with jax.named_scope("second_cross"):

        def second_cross(t, _):
            with jax.named_scope("wait_y"):
                wait_y(table((2, 2, 2) + Y_NEED[:-1], t), table((2, 2) + Y_NEED, t))

            def tile(d, h, j):
                cross = cross_tile(4 * (t - 2) + 2 * d + h, j)
                return pick(t < 4, cross, last[6 * h + j]) if d else cross

            quad(t, tile)
            return 0

        lax.fori_loop(2, 5, second_cross, 0)

    for k, done in enumerate(((0,), (4, 5), (3,))):
        for c in done:
            finish_range(c, c + 1, SB2, RB2, s2_sem, r2_sem)
        with jax.named_scope("second_chunk"):
            ps = REMOTE_ORDER[4 * k : 4 * k + 4]
            quad(5 + k, remote_quad(lambda i: jnp.int32(ps[i])))

    def finish_strip(n):
        cols = pl.ds(n * STRIP, STRIP)
        for j in range(2):
            s = homes[j][0]
            SB2[j, :, cols] = YT[s, :, cols] + jnp.transpose(YR[s, pl.ds((n + 1) * STRIP, STRIP), :])
        for j in range(2):
            remote(SB2.at[j, :, cols], RB2.at[j, :, cols], s2_sem, r2_sem, homes[j][1]).start()

    with jax.named_scope("second_chunk"):
        finish_range(2, 3, SB2, RB2, s2_sem, r2_sem)
        load_x(0, 0).wait()
        load_kb(0, 0).wait()
        use(X, 0, lambda h, j: remote_tile(jnp.int32(REMOTE_ORDER[12 + h]), j))
        finish_strip(2)
        use(KB, 0, lambda h, j: remote_tile(jnp.int32(REMOTE_ORDER[14 + h]), j))
        finish_strip(3)

    with jax.named_scope("second_par"):
        quad(9, lambda d, h, j: own_tile(jnp.int32(N_PAIR - 1), j, core) if d and h else own_ints(N_OWN + 2 + 2 * d + h, j))
        remote(YT.at[PAR], RB2.at[2], s2_sem, r2_sem, pt).start()

    with jax.named_scope("sent"):
        p_copy.wait_send()
        for j in range(2):
            remote(x_hbm, X.at[1 + j], sx_sem.at[j], rx_sem.at[0], tx).wait_send()
        for buf, sem in ((VT, sv_sem), (NB, sn_sem), (YV, sy_sem)):
            remote(buf.at[1:4], buf.at[1:4], sem, rx_sem.at[0], tx).wait_send()
        remote(SB, RB, s1_sem, rx_sem.at[0], tx).wait_send()

    with jax.named_scope("second_end"):
        load_x(0, 2).wait()
        use(X, 2, lambda h, j: own_ints(5 + h, j))

    with jax.named_scope("final"):
        for c in range(N_CHUNK):
            out_ref[:, cols_of(c)] = YT[OWN, :, cols_of(c)] + jnp.transpose(YR[OWN, sums_of(c), :])
        all_sums = remote(SB2, RB2, s2_sem, r2_sem, pt)
        all_sums.wait_send()
        all_sums.wait_recv()


def solution(mesh):
    def local_program(x_loc, v_loc, length_scale, out_scale):
        dma = pltpu.SemaphoreType.DMA
        hbm = pl.BlockSpec(memory_space=pltpu.HBM)
        vmem = pl.BlockSpec(memory_space=pltpu.VMEM)
        smem = pl.BlockSpec(memory_space=pltpu.SMEM)
        own, parts, _ = pl.pallas_call(
            body,
            out_shape=(
                pltpu.VMEM((32, ROWS), F32),
                pltpu.VMEM((3, 32, ROWS), F32),
                jax.ShapeDtypeStruct((N_PLACE * STEP_ROWS, CHUNK), BF16),
            ),
            in_specs=[hbm, hbm, smem, smem],
            out_specs=(vmem, vmem, hbm),
            scratch_shapes=[
                pltpu.VMEM((4, ROWS, 768), BF16),
                pltpu.VMEM((4, 32, ROWS), BF16),
                pltpu.VMEM((4, 32, ROWS), BF16),
                pltpu.VMEM((3, ROWS, 128), F32),
                pltpu.VMEM((4, 1, ROWS), F32),
                pltpu.VMEM((8, CHUNK), F32),
                pltpu.VMEM((3, STRIP + ROWS, 32), F32),
                pltpu.VMEM((5, 32, ROWS), F32),
                pltpu.VMEM((3, 32, ROWS), F32),
                pltpu.VMEM((3, 32, ROWS), F32),
                pltpu.VMEM((3, 32, ROWS), F32),
                pltpu.VMEM((2, HALF_ROWS, CHUNK), BF16),
                pltpu.VMEM((2, HALF_ROWS, CHUNK), BF16),
                pltpu.VMEM((STEP_ROWS, CHUNK), BF16),
                pltpu.VMEM((4, 2 * STEP_ROWS, CHUNK), BF16),
                dma((2,)), dma((8,)), dma, dma((2,)), dma, dma((2,)), dma, dma,
                dma((2,)), dma((2, 2)), dma((4,)), dma((4,)),
                dma, dma((N_CHUNK,)), dma, dma((N_CHUNK,)), dma((3,)), dma, dma,
            ],
            compiler_params=pltpu.CompilerParams(collective_id=0, has_side_effects=True, vmem_limit_bytes=58 * 2**20),
            name="products",
        )(x_loc, v_loc.T, length_scale, out_scale)
        return (own + parts[0] + parts[1] + parts[2]).T

    row_spec = P(("task", "row"), None)
    return jax.shard_map(local_program, mesh=mesh, in_specs=(row_spec, row_spec, P("task"), P("task")), out_specs=row_spec, check_vma=False)
```

```python
import functools

import jax
import jax.numpy as jnp
from jax import lax
from jax.experimental import pallas as pl
from jax.experimental.pallas import tpu as pltpu
from jax.sharding import PartitionSpec as P

MESH = pl.DeviceIdType.MESH
F32, BF16 = jnp.float32, jnp.bfloat16
LOG2E = 1.4426950408889634

ROWS = 3072
STRIP = 256
CHUNK = 512
N_STRIP = ROWS // STRIP
N_CHUNK = ROWS // CHUNK
UNITS = 3
OWN, XNB, YNB, PAR, TRASH = 0, 1, 2, 3, 4

N_OWN, N_PAIR = 7, 13
REMOTE_AT = (0, 7, 13, 18, 21, 21, 23, 23)
REMOTE_TILE = (0, 44, 80, 108, 128, 140)
CROSS_AT = (0, 0, 1, 3, 5, 6, 8, 10)
CROSS_TILE = (0, 0, 2, 4, 8, 12, 18, 24, 32, 40, 50, 60)
OWN_PLACE = (1, 2, 3, 6, 7, 48, 49, 4, 5, 44, 45, 46, 47)
REMOTE_ORDER = (23, 22, 21, 20, 19, 18, 17, 16, 15, 14, 13, 10, 8, 9, 11, 12)
REMOTE_PLACE = tuple(8 + p if p < 8 else 28 + REMOTE_ORDER.index(p) for p in range(24))
CROSS_PLACE = 16
N_PLACE = 50
STEP_ROWS = 6 * STRIP
HALF_ROWS = UNITS * STRIP
Y_NEED = (4, 5, 6)


def table(values, n):
    out = jnp.int32(values[0])
    for i in range(1, len(values)):
        if values[i] != values[i - 1]:
            out = out + (values[i] - values[i - 1]) * (n >= i).astype(jnp.int32)
    return out


def rank(bounds, x):
    out = jnp.int32(0)
    for b in bounds:
        out = out + (x >= b).astype(jnp.int32)
    return out


def pick(cond, a, b):
    return tuple(jnp.where(cond, x, y) for x, y in zip(a, b))


def i32(*xs):
    return tuple(jnp.int32(x) for x in xs)


def own_tile(o, j, core):
    p = 3 * o + j // 2
    c = rank((1, 3, 6, 10, 15), p)
    i = p - ((c * (c + 1)) >> 1)
    own = (jnp.int32(OWN), 2 * i + j % 2, jnp.int32(OWN), c, jnp.where(i == c, TRASH, OWN))
    p = 3 * (o - N_OWN) + j // 2
    c = 1 + rank((1, 3, 6, 10), p)
    i = p - ((c * (c - 1)) >> 1)
    same = core + 2 * (j // 2)
    i, c = pick(p < 15, (i, c), (same, same))
    par = (jnp.int32(OWN), 2 * i + j % 2, jnp.int32(PAR), c, jnp.int32(PAR))
    return pick(o < N_OWN, own, par)


def own_ints(o, j):
    if o < N_OWN:
        pairs = [(i, c) for c in range(N_CHUNK) for i in range(c + 1)]
        i, c = pairs[3 * o + j // 2]
        return (OWN, 2 * i + j % 2, OWN, c, TRASH if i == c else OWN)
    pairs = [(i, c) for c in range(N_CHUNK) for i in range(c)]
    i, c = pairs[3 * (o - N_OWN) + j // 2]
    return (OWN, 2 * i + j % 2, PAR, c, PAR)


def remote_tile(p, j):
    g = 6 * p + j
    d, first = jnp.int32(0), jnp.int32(0)
    for i in range(1, N_CHUNK):
        d, first = pick(g >= REMOTE_TILE[i], (i, REMOTE_TILE[i]), (d, first))
    r = g - first
    rest = r - (22 - 4 * d)
    k, side, odd = pick(rest >= 0, (rest >> 1, r & 1, 1), (r >> 1, r & 1, 0))
    k, side, odd = pick(d == 0, (r >> 2, (r >> 1) & 1, r & 1), (k, side, odd))
    t = jnp.where((k & 1) == (k > 0).astype(jnp.int32), OWN, PAR)
    return (1 + side, 2 * d + odd, t, d + ((k + 1) >> 1), t)


def cross_tile(q, j):
    g = 6 * q + j
    n, first = jnp.int32(1), jnp.int32(0)
    for i in range(2, N_STRIP - 1):
        n, first = pick(g >= CROSS_TILE[i], (i, CROSS_TILE[i]), (n, first))
    r = g - first
    m = n >> 1
    t = pick(r < m, (jnp.int32(XNB), n, jnp.int32(YNB), r, jnp.int32(YNB)), (jnp.int32(YNB), n, jnp.int32(XNB), r - m, jnp.int32(XNB)))
    return pick(r < 2 * m, t, (jnp.int32(XNB), n - 1 + (r - 2 * m), jnp.int32(YNB), m, jnp.int32(YNB)))


def last_tiles():
    n = N_STRIP - 1
    tiles = [t for c in range(N_CHUNK - 1) for t in ((YNB, n, XNB, c, XNB), (XNB, n, YNB, c, YNB))]
    tiles += [(XNB, n - 1, YNB, N_CHUNK - 1, YNB), (XNB, n, YNB, N_CHUNK - 1, YNB)]
    return [i32(*t) for t in tiles]


def span(start, size, unit):
    return pl.ds(start if isinstance(start, int) else pl.multiple_of(start, unit), size)


def rows_of(a):
    return span(a * STRIP, STRIP, STRIP)


def sums_of(c):
    return span(STRIP + c * CHUNK, CHUNK, STRIP)


def cols_of(b):
    return span(b * CHUNK, CHUNK, CHUNK)


def body(
    x_hbm, v_hbm, ell_ref, amp_ref, out_ref, RB2, k_hbm,
    X, VT, YV, NA, NB, CR, YR, YT, SB, RB, SB2, kr0, kr1, KL, KB,
    sx_sem, rx_sem, sv_sem, rv_sem, sn_sem, rn_sem, sp_sem, rp_sem, loc_sem, ko_sem, kb_sem, kx_sem,
    s1_sem, r1_sem, sy_sem, ry_sem, ryp_sem, s2_sem, r2_sem,
):
    me = lax.axis_index("row")
    core, cx, cy = me % 2, (me // 2) % 2, me // 4

    def dev(px, py, pc):
        return {"row": (py * 2 + px) * 2 + pc}

    tx = dev(1 - cx, cy, (core + 1 + cx) % 2)
    ty = dev(cx, 1 - cy, (core + 1 + cx + cy) % 2)
    sx = dev(1 - cx, cy, (core + cx) % 2)
    sy = dev(cx, 1 - cy, (core + cx + cy) % 2)
    pt = dev(cx, cy, 1 - core)

    def remote(src, dst, ss, rs, to):
        return pltpu.make_async_remote_copy(src_ref=src, dst_ref=dst, send_sem=ss, recv_sem=rs, device_id=to, device_id_type=MESH)

    def part_rows(i, late):
        return rows_of(i + 4) if late else cols_of(i)

    def x_copy(j, i, late):
        return remote(x_hbm.at[part_rows(i, late)], X.at[1 + j, part_rows(i, late)], sx_sem.at[j], rx_sem.at[i], (tx, ty)[j])

    def wait_x(i, late):
        two = X.at[1:3, part_rows(i, late)]
        remote(two, two, sx_sem.at[0], rx_sem.at[i], tx).wait_recv()

    p_copy = remote(x_hbm, X.at[PAR], sp_sem, rp_sem, pt)
    v_copies = [remote(v_hbm, VT.at[1 + j], sv_sem, rv_sem.at[j // 2], d) for j, d in enumerate((tx, ty, pt))]
    tail_cols = pl.ds(4 * CHUNK, 2 * CHUNK)
    n_copies = [remote(NB.at[OWN, :, tail_cols], NB.at[1 + j, :, tail_cols], sn_sem.at[0], rn_sem.at[0], d) for j, d in enumerate((tx, ty))]
    n_copies.append(remote(NB.at[OWN], NB.at[PAR], sn_sem.at[1], rn_sem.at[1], pt))

    x_loc = pltpu.make_async_copy(x_hbm, X.at[OWN], loc_sem.at[0])
    v_loc = pltpu.make_async_copy(v_hbm, VT.at[OWN], loc_sem.at[1])
    for c in (v_loc, x_loc):
        c.start()

    barrier = pltpu.get_barrier_semaphore()
    for d in (tx, ty, sx, sy, pt):
        pl.semaphore_signal(barrier, inc=1, device_id=d, device_id_type=MESH)
    with jax.named_scope("barrier"):
        pl.semaphore_wait(barrier, 5)

    for c in v_copies:
        c.start()
    for j in range(2):
        x_copy(j, 0, False).start()
    p_copy.start()

    ell = jnp.full((1, CHUNK), ell_ref[0], F32)
    half = LOG2E / (2.0 * ell * ell)
    top = jnp.log2(jnp.full((1, CHUNK), amp_ref[0], F32))
    CR[0:1, :] = 2.0 * half
    CR[1:2, :] = top

    for s in range(3):
        YR[s] = jnp.zeros((STRIP + ROWS, 32), F32)
    for t in range(5):
        YT[t] = jnp.zeros((32, ROWS), F32)
    kr0[...] = jnp.zeros_like(kr0)
    kr1[...] = jnp.zeros_like(kr1)

    v_loc.wait()
    with jax.named_scope("x_local"):
        x_loc.wait()

    def norm_of(s, c):
        r = pl.ds(pl.multiple_of(c * CHUNK, CHUNK), CHUNK)
        x = X[s, r, :].astype(F32)
        n = jnp.broadcast_to(0.5 * jnp.sum(x * x, axis=1, keepdims=True), (CHUNK, 128))
        NA[s, r, :] = n
        NB[s, :, cols_of(c)] = jnp.transpose(n)[0:1, :]

    def own_norm(c, _):
        norm_of(OWN, c)
        return 0

    with jax.named_scope("own_norm"):
        lax.fori_loop(0, N_CHUNK, own_norm, 0)
    for c in n_copies:
        c.start()

    for i in range(1, 8):
        for j in range(2):
            x_copy(j, i, i >= 4).start()

    def left_norm(s):
        def one(c, _):
            r = pl.ds(pl.multiple_of(c * CHUNK, CHUNK), CHUNK)
            NA[s, r, :] = jnp.transpose(jnp.broadcast_to(NB[s, :, cols_of(c)], (128, CHUNK)))
            return 0

        lax.fori_loop(4, N_CHUNK, one, 0)

    def gram(tile):
        s, a, t, b, _ = tile
        return lax.dot_general(X[s, rows_of(a), :], X[t, cols_of(b), :], (((1,), (1,)), ((), ())), preferred_element_type=F32)

    def kern(tile, g):
        s, a, t, b, _ = tile
        na = NA[s, rows_of(a), :]
        d = (jnp.concatenate([na] * (CHUNK // 128), axis=1) + NB[t, :, cols_of(b)]) - g
        return jnp.exp2(CR[1:2, :] - jnp.maximum(d, 0.0) * CR[0:1, :]).astype(BF16)

    def apply(tile, k, vec):
        s, a, t, b, to = tile
        YR[s, rows_of(a + 1), :] += lax.dot_general(k, vec[t, :, cols_of(b)], (((1,), (1,)), ((), ())), preferred_element_type=F32)
        if isinstance(to, int) and to == TRASH:
            return
        left = a if isinstance(a, int) else jnp.maximum(a, 0)
        YT[to, :, cols_of(b)] += jnp.dot(vec[s, :, rows_of(left)], k, preferred_element_type=F32)

    def k_out(seq, place, half):
        kr = (kr0, kr1)[half]
        row = pl.multiple_of(place * STEP_ROWS + half * HALF_ROWS, STRIP)
        return pltpu.make_async_copy(kr.at[seq & 1], k_hbm.at[pl.ds(row, HALF_ROWS)], ko_sem.at[seq & 1, half])

    def half_step(prev, cur, kr_new, d_new, kr_old, d_old):
        gs = [gram(t) for t in cur]
        for u in range(UNITS):
            apply(prev[u], kr_old[d_old, u * STRIP : (u + 1) * STRIP, :], VT)
        for u in range(UNITS):
            kr_new[d_new, u * STRIP : (u + 1) * STRIP, :] = kern(cur[u], gs[u])

    def flat(tiles):
        return tuple(x for t in tiles for x in t)

    def unflat(xs):
        return [tuple(xs[5 * u : 5 * u + 5]) for u in range(UNITS)]

    def begin(seq, before, place):
        @pl.when(seq >= 2)
        def _():
            for h in range(2):
                k_out(seq, place, h).wait()

        @pl.when(seq >= 1)
        def _():
            for h in range(2):
                k_out(seq - 1, before, h).start()

        return seq & 1

    def step_of(state, place, tile):
        seq, before, prev = state[0], state[1], state[2:]
        d = begin(seq, before, place)
        first = [tile(u) for u in range(UNITS)]
        second = [tile(UNITS + u) for u in range(UNITS)]
        half_step(unflat(prev), first, kr0, d, kr1, 1 - d)
        half_step(first, second, kr1, d, kr0, d)
        return (seq + 1, place) + flat(second)

    none = flat([i32(OWN, -1, OWN, 0, TRASH)] * UNITS)

    def own_step(o, state):
        @pl.when(o == N_OWN)
        def _():
            p_copy.wait_recv()
            v_copies[2].wait_recv()
            n_copies[2].wait_recv()

        return step_of(state, table(OWN_PLACE, o), lambda j: own_tile(o, j, core))

    def remote_step(p, state):
        return step_of(state, table(REMOTE_PLACE, p), lambda j: remote_tile(p, j))

    def cross_step(q, state):
        return step_of(state, CROSS_PLACE + q, lambda j: cross_tile(q, j))

    with jax.named_scope("pre"):
        state = lax.fori_loop(0, N_PAIR, own_step, i32(0, 0) + none)

    with jax.named_scope("left_norm"):
        remote(VT.at[1:3], VT.at[1:3], sv_sem, rv_sem.at[0], tx).wait_recv()
        remote(NB.at[1:3, :, tail_cols], NB.at[1:3, :, tail_cols], sn_sem.at[0], rn_sem.at[0], tx).wait_recv()
        for j in range(2):
            left_norm(1 + j)

    def landed(i, state):
        with jax.named_scope("wait_strip"):

            @pl.when(i < 4)
            def _():
                wait_x(i, False)
                for s in range(1, 3):
                    norm_of(s, i)

            @pl.when(i >= 4)
            def _():
                wait_x(i, True)

        with jax.named_scope("strip"):
            state = lax.fori_loop(table(REMOTE_AT, i), table(REMOTE_AT, i + 1), remote_step, state)
            return lax.fori_loop(table(CROSS_AT, i), table(CROSS_AT, i + 1), cross_step, state)

    state = lax.fori_loop(0, 7, landed, state)

    homes = ((XNB, sx), (YNB, sy), (PAR, pt))

    def part_copy(j, c, send, recv, ss, rs):
        return remote(send.at[j, :, cols_of(c)], recv.at[j, :, cols_of(c)], ss, rs.at[c] if send is SB else rs, homes[j][1])

    def finish(j, c, send):
        s = homes[j][0]
        part = YT[s, :, cols_of(c)]
        if j < 2:
            part = part + jnp.transpose(YR[s, sums_of(c), :])
        send[j, :, cols_of(c)] = part
        if send is SB:
            YT[s, :, cols_of(c)] = jnp.zeros((32, CHUNK), F32)
            if j < 2:
                YR[s, sums_of(c), :] = jnp.zeros((CHUNK, 32), F32)

    def finish_range(lo, hi, send, recv, ss, rs, js=(0, 1)):
        for c in range(lo, hi):
            for j in js:
                finish(j, c, send)
            for j in js:
                part_copy(j, c, send, recv, ss, rs).start()

    def load_kb(d, slot):
        return pltpu.make_async_copy(k_hbm.at[pl.ds(pl.multiple_of(d * 2 * STEP_ROWS, STRIP), 2 * STEP_ROWS)], KB.at[slot], kb_sem.at[slot])

    def load_x(d, slot):
        src = k_hbm.at[pl.ds(pl.multiple_of(d * 2 * STEP_ROWS, STRIP), 2 * STEP_ROWS)]
        return pltpu.make_async_copy(src, X.at[slot, :, 0:CHUNK], kx_sem.at[slot])

    first_in = pltpu.make_async_copy(k_hbm.at[pl.ds(STEP_ROWS, STEP_ROWS)], KB.at[0, pl.ds(STEP_ROWS, STEP_ROWS)], kb_sem.at[0])
    first_in.start()
    for i in range(1, 4):
        load_kb(i, i).start()

    def y_copy(j, c):
        done = ryp_sem.at[(c >= 3) + (c >= 4)] if j == 2 else ry_sem.at[c]
        return remote(YV.at[OWN, :, cols_of(c)], YV.at[1 + j, :, cols_of(c)], sy_sem, done, (tx, ty, pt)[j])

    def middle(c):
        with jax.named_scope("wait_part"):
            three = RB.at[:, :, cols_of(c)]
            remote(three, three, s1_sem, r1_sem.at[c], pt).wait_recv()
        y = YT[OWN, :, cols_of(c)] + jnp.transpose(YR[OWN, sums_of(c), :])
        y = y + RB[0, :, cols_of(c)] + RB[1, :, cols_of(c)] + RB[2, :, cols_of(c)]
        YV[OWN, :, cols_of(c)] = y.astype(BF16)
        YT[OWN, :, cols_of(c)] = jnp.zeros((32, CHUNK), F32)
        YR[OWN, sums_of(c), :] = jnp.zeros((CHUNK, 32), F32)
        for j in range(3):
            y_copy(j, c).start()

    last = last_tiles()
    late = [remote_tile(jnp.int32(23), j) for j in range(6)]

    def rows_in(u, d):
        if d is None:
            return KL, (slice(u * STRIP, (u + 1) * STRIP), slice(None))
        return (kr0, kr1)[u % 6 // UNITS], (d, slice(u % UNITS * STRIP, (u % UNITS + 1) * STRIP), slice(None))

    def grams(tiles, first, d):
        gs = [gram(t) for t in tiles]

        def put():
            for u, (t, g) in enumerate(zip(tiles, gs), first):
                ref, at = rows_in(u, d)
                ref[at] = kern(t, g)

        return put

    def applies(tiles, first, d):
        for u, t in enumerate(tiles, first):
            ref, at = rows_in(u, d)
            apply(t, ref[at], VT)

    kl_out = pltpu.make_async_copy(KL, k_hbm.at[pl.ds(REMOTE_PLACE[23] * STEP_ROWS, STEP_ROWS)], loc_sem.at[0])
    seq, before, due = state[0], state[1], unflat(state[2:])
    d = begin(seq, before, before)
    put = grams(late[0:2], 0, None)
    applies(due, UNITS, 1 - d)
    put()
    put = grams(late[2:4], 2, None)
    applies(late[0:2], 0, None)
    put()
    applies(late[2:4], 2, None)
    finish_range(0, N_CHUNK, SB, RB, s1_sem, r1_sem, (2,))
    with jax.named_scope("wait_last"):
        wait_x(7, True)
    with jax.named_scope("last"):
        for c in range(N_CHUNK):
            if c == 3:
                d = begin(seq + 1, jnp.int32(CROSS_PLACE + 10), before)
            put = grams(last[2 * c : 2 * c + 2], 2 * c, d)
            if c > 1:
                applies(last[2 * c - 2 : 2 * c], 2 * c - 2, 1 - d if c == 3 else d)
            put()
            if c == 0:
                applies(last[0:2], 0, d)
            if c != 1:
                finish_range(max(c - 1, 0), max(c, 1), SB, RB, s1_sem, r1_sem)
        put = grams(late[4:6], 4, None)
        applies(last[10:12], 10, d)
        put()
        kl_out.start()
        load_x(4, 0).start()
        middle(0)
        applies(late[4:6], 4, None)
        finish_range(5, 6, SB, RB, s1_sem, r1_sem)

    for h in range(2):
        k_out(seq, 0, h).wait()
        k_out(seq + 1, CROSS_PLACE + 11, h).start()

    def use(k, slot, tile):
        for h in range(2):
            use_step(k, slot, h, functools.partial(tile, h))

    def use_step(k, slot, h, tile):
        for j in range(6):
            r = (6 * h + j) * STRIP
            apply(tile(j), k[slot, r : r + STRIP, 0:CHUNK], YV)

    def quad(t, tile):
        slot = t & 3
        load_x(0, slot).wait()
        load_kb(0, slot).wait()
        t = jnp.int32(t)

        @pl.when(jnp.logical_and(t >= 1, t <= 7))
        def _():
            load_x(10 + 2 * t, (t - 1) & 3).start()

        @pl.when(jnp.logical_and(t >= 1, t <= 6))
        def _():
            load_kb(11 + 2 * t, (t - 1) & 3).start()

        use(X, slot, lambda h, j: tile(0, h, j))
        use(KB, slot, lambda h, j: tile(1, h, j))

    def wait_y_one(c):
        two = YV.at[1:3, :, cols_of(c)]
        remote(two, two, sy_sem, ry_sem.at[c], tx).wait_recv()

    def wait_y(lo, hi):
        def one(c, _):
            wait_y_one(c)
            return 0

        lax.fori_loop(lo, hi, one, 0)

    def wait_y_par(late):
        part = YV.at[PAR, :, pl.ds((0, 3, 4)[late] * CHUNK, (3, 1, 2)[late] * CHUNK)]
        remote(part, part, sy_sem, ryp_sem.at[late], pt).wait_recv()

    with jax.named_scope("middle"):
        middle(1)
    with jax.named_scope("second_own"):
        first_in.wait()
        for j in range(6):
            apply(own_ints(0, j), KB[0, STEP_ROWS + j * STRIP : STEP_ROWS + (j + 1) * STRIP, :], YV)
        load_kb(5, 0).start()
        middle(2)
        load_kb(0, 1).wait()
        use_step(KB, 1, 0, lambda j: own_ints(1, j))
        wait_y_par(0)
        load_kb(0, 2).wait()
        use_step(KB, 2, 0, lambda j: own_ints(N_OWN, j))
        middle(3)
        use_step(KB, 1, 1, lambda j: own_ints(2, j))
        load_x(6, 1).start()
        load_kb(7, 1).start()
        wait_y_par(1)
        use_step(KB, 2, 1, lambda j: own_ints(N_OWN + 1, j))
        load_x(8, 2).start()
        load_kb(9, 2).start()
        kl_out.wait()
        for h in range(2):
            k_out(seq + 1, 0, h).wait()
        load_x(10, 3).start()
        middle(4)

    def remote_quad(step):
        ps = [step(i) for i in range(4)]
        return lambda d, h, j: remote_tile(ps[2 * d + h], j)

    with jax.named_scope("second_first"):

        wait_y_one(0)
        quad(0, remote_quad(jnp.int32))
        middle(5)
        load_kb(0, 3).wait()
        use(KB, 3, lambda h, j: own_ints(3 + h, j))
        load_kb(11, 3).start()
        wait_y_par(2)
        wait_y_one(1)
        quad(1, remote_quad(lambda i: jnp.int32(4 + i)))
    with jax.named_scope("second_cross"):

        def second_cross(t, _):
            with jax.named_scope("wait_y"):
                wait_y(table((2, 2, 2) + Y_NEED[:-1], t), table((2, 2) + Y_NEED, t))

            def tile(d, h, j):
                cross = cross_tile(4 * (t - 2) + 2 * d + h, j)
                return pick(t < 4, cross, last[6 * h + j]) if d else cross

            quad(t, tile)
            return 0

        lax.fori_loop(2, 5, second_cross, 0)

    for k, done in enumerate(((0,), (4, 5), (3,))):
        for c in done:
            finish_range(c, c + 1, SB2, RB2, s2_sem, r2_sem)
        with jax.named_scope("second_chunk"):
            ps = REMOTE_ORDER[4 * k : 4 * k + 4]
            quad(5 + k, remote_quad(lambda i: jnp.int32(ps[i])))

    def finish_strip(n):
        cols = pl.ds(n * STRIP, STRIP)
        for j in range(2):
            s = homes[j][0]
            SB2[j, :, cols] = YT[s, :, cols] + jnp.transpose(YR[s, pl.ds((n + 1) * STRIP, STRIP), :])
        for j in range(2):
            remote(SB2.at[j, :, cols], RB2.at[j, :, cols], s2_sem, r2_sem, homes[j][1]).start()

    with jax.named_scope("second_chunk"):
        finish_range(2, 3, SB2, RB2, s2_sem, r2_sem)
        load_x(0, 0).wait()
        load_kb(0, 0).wait()
        use(X, 0, lambda h, j: remote_tile(jnp.int32(REMOTE_ORDER[12 + h]), j))
        finish_strip(2)
        use(KB, 0, lambda h, j: remote_tile(jnp.int32(REMOTE_ORDER[14 + h]), j))
        finish_strip(3)

    with jax.named_scope("second_par"):
        quad(9, lambda d, h, j: own_tile(jnp.int32(N_PAIR - 1), j, core) if d and h else own_ints(N_OWN + 2 + 2 * d + h, j))
        remote(YT.at[PAR], RB2.at[2], s2_sem, r2_sem, pt).start()

    with jax.named_scope("sent"):
        p_copy.wait_send()
        for j in range(2):
            remote(x_hbm, X.at[1 + j], sx_sem.at[j], rx_sem.at[0], tx).wait_send()
        remote(NB.at[1:3, :, tail_cols], NB.at[1:3, :, tail_cols], sn_sem.at[0], rx_sem.at[0], tx).wait_send()
        n_copies[2].wait_send()
        for buf, sem in ((VT, sv_sem), (YV, sy_sem)):
            remote(buf.at[1:4], buf.at[1:4], sem, rx_sem.at[0], tx).wait_send()
        remote(SB, RB, s1_sem, rx_sem.at[0], tx).wait_send()

    with jax.named_scope("second_end"):
        load_x(0, 2).wait()
        use(X, 2, lambda h, j: own_ints(5 + h, j))

    with jax.named_scope("final"):
        for c in range(N_CHUNK):
            out_ref[:, cols_of(c)] = YT[OWN, :, cols_of(c)] + jnp.transpose(YR[OWN, sums_of(c), :])
        all_sums = remote(SB2, RB2, s2_sem, r2_sem, pt)
        all_sums.wait_send()
        all_sums.wait_recv()


def solution(mesh):
    def local_program(x_loc, v_loc, length_scale, out_scale):
        dma = pltpu.SemaphoreType.DMA
        hbm = pl.BlockSpec(memory_space=pltpu.HBM)
        vmem = pl.BlockSpec(memory_space=pltpu.VMEM)
        smem = pl.BlockSpec(memory_space=pltpu.SMEM)
        own, parts, _ = pl.pallas_call(
            body,
            out_shape=(
                pltpu.VMEM((32, ROWS), F32),
                pltpu.VMEM((3, 32, ROWS), F32),
                jax.ShapeDtypeStruct((N_PLACE * STEP_ROWS, CHUNK), BF16),
            ),
            in_specs=[hbm, hbm, smem, smem],
            out_specs=(vmem, vmem, hbm),
            scratch_shapes=[
                pltpu.VMEM((4, ROWS, 768), BF16),
                pltpu.VMEM((4, 32, ROWS), BF16),
                pltpu.VMEM((4, 32, ROWS), BF16),
                pltpu.VMEM((3, ROWS, 128), F32),
                pltpu.VMEM((4, 1, ROWS), F32),
                pltpu.VMEM((8, CHUNK), F32),
                pltpu.VMEM((3, STRIP + ROWS, 32), F32),
                pltpu.VMEM((5, 32, ROWS), F32),
                pltpu.VMEM((3, 32, ROWS), F32),
                pltpu.VMEM((3, 32, ROWS), F32),
                pltpu.VMEM((3, 32, ROWS), F32),
                pltpu.VMEM((2, HALF_ROWS, CHUNK), BF16),
                pltpu.VMEM((2, HALF_ROWS, CHUNK), BF16),
                pltpu.VMEM((STEP_ROWS, CHUNK), BF16),
                pltpu.VMEM((4, 2 * STEP_ROWS, CHUNK), BF16),
                dma((2,)), dma((8,)), dma, dma((2,)), dma((2,)), dma((2,)), dma, dma,
                dma((2,)), dma((2, 2)), dma((4,)), dma((4,)),
                dma, dma((N_CHUNK,)), dma, dma((N_CHUNK,)), dma((3,)), dma, dma,
            ],
            compiler_params=pltpu.CompilerParams(collective_id=0, has_side_effects=True, vmem_limit_bytes=58 * 2**20),
            name="products",
        )(x_loc, v_loc.T, length_scale, out_scale)
        return (own + parts[0] + parts[1] + parts[2]).T

    row_spec = P(("task", "row"), None)
    return jax.shard_map(local_program, mesh=mesh, in_specs=(row_spec, row_spec, P("task"), P("task")), out_specs=row_spec, check_vma=False)
```

```python
import functools

import jax
import jax.numpy as jnp
from jax import lax
from jax.experimental import pallas as pl
from jax.experimental.pallas import tpu as pltpu
from jax.sharding import PartitionSpec as P

MESH = pl.DeviceIdType.MESH
F32, BF16 = jnp.float32, jnp.bfloat16
LOG2E = 1.4426950408889634

ROWS = 3072
STRIP = 256
CHUNK = 512
N_STRIP = ROWS // STRIP
N_CHUNK = ROWS // CHUNK
UNITS = 3
OWN, XNB, YNB, PAR, TRASH = 0, 1, 2, 3, 4

N_OWN, N_PAIR = 7, 13
REMOTE_AT = (0, 7, 13, 18, 21, 21, 23, 23)
REMOTE_TILE = (0, 44, 80, 108, 128, 140)
CROSS_AT = (0, 0, 1, 3, 5, 6, 8, 10)
CROSS_TILE = (0, 0, 2, 4, 8, 12, 18, 24, 32, 40, 50, 60)
OWN_PLACE = (1, 2, 3, 6, 7, 48, 49, 4, 5, 44, 45, 46, 47)
REMOTE_ORDER = (23, 22, 21, 20, 19, 18, 17, 16, 15, 14, 13, 10, 8, 9, 11, 12)
REMOTE_PLACE = tuple(8 + p if p < 8 else 28 + REMOTE_ORDER.index(p) for p in range(24))
CROSS_PLACE = 16
N_PLACE = 50
STEP_ROWS = 6 * STRIP
HALF_ROWS = UNITS * STRIP
Y_NEED = (4, 5, 6)


def table(values, n):
    out = jnp.int32(values[0])
    for i in range(1, len(values)):
        if values[i] != values[i - 1]:
            out = out + (values[i] - values[i - 1]) * (n >= i).astype(jnp.int32)
    return out


def rank(bounds, x):
    out = jnp.int32(0)
    for b in bounds:
        out = out + (x >= b).astype(jnp.int32)
    return out


def pick(cond, a, b):
    return tuple(jnp.where(cond, x, y) for x, y in zip(a, b))


def i32(*xs):
    return tuple(jnp.int32(x) for x in xs)


def own_tile(o, j, core):
    p = 3 * o + j // 2
    c = rank((1, 3, 6, 10, 15), p)
    i = p - ((c * (c + 1)) >> 1)
    own = (jnp.int32(OWN), 2 * i + j % 2, jnp.int32(OWN), c, jnp.where(i == c, TRASH, OWN))
    p = 3 * (o - N_OWN) + j // 2
    c = 1 + rank((1, 3, 6, 10), p)
    i = p - ((c * (c - 1)) >> 1)
    same = core + 2 * (j // 2)
    i, c = pick(p < 15, (i, c), (same, same))
    par = (jnp.int32(OWN), 2 * i + j % 2, jnp.int32(PAR), c, jnp.int32(PAR))
    return pick(o < N_OWN, own, par)


def own_ints(o, j):
    if o < N_OWN:
        pairs = [(i, c) for c in range(N_CHUNK) for i in range(c + 1)]
        i, c = pairs[3 * o + j // 2]
        return (OWN, 2 * i + j % 2, OWN, c, TRASH if i == c else OWN)
    pairs = [(i, c) for c in range(N_CHUNK) for i in range(c)]
    i, c = pairs[3 * (o - N_OWN) + j // 2]
    return (OWN, 2 * i + j % 2, PAR, c, PAR)


def remote_tile(p, j):
    g = 6 * p + j
    d, first = jnp.int32(0), jnp.int32(0)
    for i in range(1, N_CHUNK):
        d, first = pick(g >= REMOTE_TILE[i], (i, REMOTE_TILE[i]), (d, first))
    r = g - first
    rest = r - (22 - 4 * d)
    k, side, odd = pick(rest >= 0, (rest >> 1, r & 1, 1), (r >> 1, r & 1, 0))
    k, side, odd = pick(d == 0, (r >> 2, (r >> 1) & 1, r & 1), (k, side, odd))
    t = jnp.where((k & 1) == (k > 0).astype(jnp.int32), OWN, PAR)
    return (1 + side, 2 * d + odd, t, d + ((k + 1) >> 1), t)


def cross_tile(q, j):
    g = 6 * q + j
    n, first = jnp.int32(1), jnp.int32(0)
    for i in range(2, N_STRIP - 1):
        n, first = pick(g >= CROSS_TILE[i], (i, CROSS_TILE[i]), (n, first))
    r = g - first
    m = n >> 1
    t = pick(r < m, (jnp.int32(XNB), n, jnp.int32(YNB), r, jnp.int32(YNB)), (jnp.int32(YNB), n, jnp.int32(XNB), r - m, jnp.int32(XNB)))
    return pick(r < 2 * m, t, (jnp.int32(XNB), n - 1 + (r - 2 * m), jnp.int32(YNB), m, jnp.int32(YNB)))


def last_tiles():
    n = N_STRIP - 1
    tiles = [t for c in range(N_CHUNK - 1) for t in ((YNB, n, XNB, c, XNB), (XNB, n, YNB, c, YNB))]
    tiles += [(XNB, n - 1, YNB, N_CHUNK - 1, YNB), (XNB, n, YNB, N_CHUNK - 1, YNB)]
    return [i32(*t) for t in tiles]


def span(start, size, unit):
    return pl.ds(start if isinstance(start, int) else pl.multiple_of(start, unit), size)


def rows_of(a):
    return span(a * STRIP, STRIP, STRIP)


def sums_of(c):
    return span(STRIP + c * CHUNK, CHUNK, STRIP)


def cols_of(b):
    return span(b * CHUNK, CHUNK, CHUNK)


def body(
    x_hbm, v_hbm, ell_ref, amp_ref, out_ref, RB2, k_hbm,
    X, VT, YV, NA, NB, CR, YR, YT, SB, RB, SB2, kr0, kr1, KL, KB,
    sx_sem, rx_sem, sv_sem, rv_sem, sn_sem, rn_sem, sp_sem, rp_sem, loc_sem, ko_sem, kb_sem, kx_sem,
    s1_sem, r1_sem, sy_sem, ry_sem, ryp_sem, s2_sem, r2_sem,
):
    me = lax.axis_index("row")
    core, cx, cy = me % 2, (me // 2) % 2, me // 4

    def dev(px, py, pc):
        return {"row": (py * 2 + px) * 2 + pc}

    tx = dev(1 - cx, cy, (core + 1 + cx) % 2)
    ty = dev(cx, 1 - cy, (core + 1 + cx + cy) % 2)
    sx = dev(1 - cx, cy, (core + cx) % 2)
    sy = dev(cx, 1 - cy, (core + cx + cy) % 2)
    pt = dev(cx, cy, 1 - core)

    def remote(src, dst, ss, rs, to):
        return pltpu.make_async_remote_copy(src_ref=src, dst_ref=dst, send_sem=ss, recv_sem=rs, device_id=to, device_id_type=MESH)

    def part_rows(i, late):
        return rows_of(i + 4) if late else cols_of(i)

    def x_copy(j, i, late):
        return remote(x_hbm.at[part_rows(i, late)], X.at[1 + j, part_rows(i, late)], sx_sem.at[j], rx_sem.at[i], (tx, ty)[j])

    def wait_x(i, late):
        two = X.at[1:3, part_rows(i, late)]
        remote(two, two, sx_sem.at[0], rx_sem.at[i], tx).wait_recv()

    p_copy = remote(x_hbm, X.at[PAR], sp_sem, rp_sem, pt)
    v_copies = [remote(v_hbm, VT.at[1 + j], sv_sem, rv_sem.at[j // 2], d) for j, d in enumerate((tx, ty, pt))]
    tail_cols = pl.ds(5 * CHUNK, CHUNK)
    n_copies = [remote(NB.at[OWN, :, tail_cols], NB.at[1 + j, :, tail_cols], sn_sem.at[0], rn_sem.at[0], d) for j, d in enumerate((tx, ty))]
    n_copies.append(remote(NB.at[OWN], NB.at[PAR], sn_sem.at[1], rn_sem.at[1], pt))

    x_loc = pltpu.make_async_copy(x_hbm, X.at[OWN], loc_sem.at[0])
    v_loc = pltpu.make_async_copy(v_hbm, VT.at[OWN], loc_sem.at[1])
    for c in (v_loc, x_loc):
        c.start()

    barrier = pltpu.get_barrier_semaphore()
    for d in (tx, ty, sx, sy, pt):
        pl.semaphore_signal(barrier, inc=1, device_id=d, device_id_type=MESH)
    with jax.named_scope("barrier"):
        pl.semaphore_wait(barrier, 5)

    for c in v_copies:
        c.start()
    for j in range(2):
        x_copy(j, 0, False).start()
    p_copy.start()

    ell = jnp.full((1, CHUNK), ell_ref[0], F32)
    half = LOG2E / (2.0 * ell * ell)
    top = jnp.log2(jnp.full((1, CHUNK), amp_ref[0], F32))
    CR[0:1, :] = 2.0 * half
    CR[1:2, :] = top

    for s in range(3):
        YR[s] = jnp.zeros((STRIP + ROWS, 32), F32)
    for t in range(5):
        YT[t] = jnp.zeros((32, ROWS), F32)
    kr0[...] = jnp.zeros_like(kr0)
    kr1[...] = jnp.zeros_like(kr1)

    v_loc.wait()
    with jax.named_scope("x_local"):
        x_loc.wait()

    def norm_of(s, i, size=CHUNK):
        r = pl.ds(pl.multiple_of(i * size, size), size)
        x = X[s, r, :].astype(F32)
        n = jnp.broadcast_to(0.5 * jnp.sum(x * x, axis=1, keepdims=True), (size, 128))
        NA[s, r, :] = n
        NB[s, :, r] = jnp.transpose(n)[0:1, :]

    def own_norm(c, _):
        norm_of(OWN, c)
        return 0

    with jax.named_scope("own_norm"):
        lax.fori_loop(0, N_CHUNK, own_norm, 0)
    for c in n_copies:
        c.start()

    for i in range(1, 8):
        for j in range(2):
            x_copy(j, i, i >= 4).start()

    def left_norm(s):
        def one(c, _):
            r = pl.ds(pl.multiple_of(c * CHUNK, CHUNK), CHUNK)
            NA[s, r, :] = jnp.transpose(jnp.broadcast_to(NB[s, :, cols_of(c)], (128, CHUNK)))
            return 0

        lax.fori_loop(5, N_CHUNK, one, 0)

    def gram(tile):
        s, a, t, b, _ = tile
        return lax.dot_general(X[s, rows_of(a), :], X[t, cols_of(b), :], (((1,), (1,)), ((), ())), preferred_element_type=F32)

    def kern(tile, g):
        s, a, t, b, _ = tile
        na = NA[s, rows_of(a), :]
        d = (jnp.concatenate([na] * (CHUNK // 128), axis=1) + NB[t, :, cols_of(b)]) - g
        return jnp.exp2(CR[1:2, :] - jnp.maximum(d, 0.0) * CR[0:1, :]).astype(BF16)

    def apply(tile, k, vec):
        s, a, t, b, to = tile
        YR[s, rows_of(a + 1), :] += lax.dot_general(k, vec[t, :, cols_of(b)], (((1,), (1,)), ((), ())), preferred_element_type=F32)
        if isinstance(to, int) and to == TRASH:
            return
        left = a if isinstance(a, int) else jnp.maximum(a, 0)
        YT[to, :, cols_of(b)] += jnp.dot(vec[s, :, rows_of(left)], k, preferred_element_type=F32)

    def k_out(seq, place, half):
        kr = (kr0, kr1)[half]
        row = pl.multiple_of(place * STEP_ROWS + half * HALF_ROWS, STRIP)
        return pltpu.make_async_copy(kr.at[seq & 1], k_hbm.at[pl.ds(row, HALF_ROWS)], ko_sem.at[seq & 1, half])

    def half_step(prev, cur, kr_new, d_new, kr_old, d_old):
        gs = [gram(t) for t in cur]
        for u in range(UNITS):
            apply(prev[u], kr_old[d_old, u * STRIP : (u + 1) * STRIP, :], VT)
        for u in range(UNITS):
            kr_new[d_new, u * STRIP : (u + 1) * STRIP, :] = kern(cur[u], gs[u])

    def flat(tiles):
        return tuple(x for t in tiles for x in t)

    def unflat(xs):
        return [tuple(xs[5 * u : 5 * u + 5]) for u in range(UNITS)]

    def begin(seq, before, place):
        @pl.when(seq >= 2)
        def _():
            for h in range(2):
                k_out(seq, place, h).wait()

        @pl.when(seq >= 1)
        def _():
            for h in range(2):
                k_out(seq - 1, before, h).start()

        return seq & 1

    def step_of(state, place, tile):
        seq, before, prev = state[0], state[1], state[2:]
        d = begin(seq, before, place)
        first = [tile(u) for u in range(UNITS)]
        second = [tile(UNITS + u) for u in range(UNITS)]
        half_step(unflat(prev), first, kr0, d, kr1, 1 - d)
        half_step(first, second, kr1, d, kr0, d)
        return (seq + 1, place) + flat(second)

    none = flat([i32(OWN, -1, OWN, 0, TRASH)] * UNITS)

    def own_step(o, state):
        @pl.when(o == N_OWN)
        def _():
            p_copy.wait_recv()
            v_copies[2].wait_recv()
            n_copies[2].wait_recv()

        return step_of(state, table(OWN_PLACE, o), lambda j: own_tile(o, j, core))

    def remote_step(p, state):
        return step_of(state, table(REMOTE_PLACE, p), lambda j: remote_tile(p, j))

    def cross_step(q, state):
        return step_of(state, CROSS_PLACE + q, lambda j: cross_tile(q, j))

    with jax.named_scope("pre"):
        state = lax.fori_loop(0, N_PAIR, own_step, i32(0, 0) + none)

    with jax.named_scope("left_norm"):
        remote(VT.at[1:3], VT.at[1:3], sv_sem, rv_sem.at[0], tx).wait_recv()
        remote(NB.at[1:3, :, tail_cols], NB.at[1:3, :, tail_cols], sn_sem.at[0], rn_sem.at[0], tx).wait_recv()
        for j in range(2):
            left_norm(1 + j)

    def landed(i, state):
        with jax.named_scope("wait_strip"):

            @pl.when(i < 4)
            def _():
                wait_x(i, False)
                for s in range(1, 3):
                    norm_of(s, i)

            @pl.when(i >= 4)
            def _():
                wait_x(i, True)

            @pl.when(jnp.logical_or(i == 4, i == 5))
            def _():
                for s in range(1, 3):
                    norm_of(s, i + 4, STRIP)

        with jax.named_scope("strip"):
            state = lax.fori_loop(table(REMOTE_AT, i), table(REMOTE_AT, i + 1), remote_step, state)
            return lax.fori_loop(table(CROSS_AT, i), table(CROSS_AT, i + 1), cross_step, state)

    state = lax.fori_loop(0, 7, landed, state)

    homes = ((XNB, sx), (YNB, sy), (PAR, pt))

    def part_copy(j, c, send, recv, ss, rs):
        return remote(send.at[j, :, cols_of(c)], recv.at[j, :, cols_of(c)], ss, rs.at[c] if send is SB else rs, homes[j][1])

    def finish(j, c, send):
        s = homes[j][0]
        part = YT[s, :, cols_of(c)]
        if j < 2:
            part = part + jnp.transpose(YR[s, sums_of(c), :])
        send[j, :, cols_of(c)] = part
        if send is SB:
            YT[s, :, cols_of(c)] = jnp.zeros((32, CHUNK), F32)
            if j < 2:
                YR[s, sums_of(c), :] = jnp.zeros((CHUNK, 32), F32)

    def finish_range(lo, hi, send, recv, ss, rs, js=(0, 1)):
        for c in range(lo, hi):
            for j in js:
                finish(j, c, send)
            for j in js:
                part_copy(j, c, send, recv, ss, rs).start()

    def load_kb(d, slot):
        return pltpu.make_async_copy(k_hbm.at[pl.ds(pl.multiple_of(d * 2 * STEP_ROWS, STRIP), 2 * STEP_ROWS)], KB.at[slot], kb_sem.at[slot])

    def load_x(d, slot):
        src = k_hbm.at[pl.ds(pl.multiple_of(d * 2 * STEP_ROWS, STRIP), 2 * STEP_ROWS)]
        return pltpu.make_async_copy(src, X.at[slot, :, 0:CHUNK], kx_sem.at[slot])

    first_in = pltpu.make_async_copy(k_hbm.at[pl.ds(STEP_ROWS, STEP_ROWS)], KB.at[0, pl.ds(STEP_ROWS, STEP_ROWS)], kb_sem.at[0])
    first_in.start()
    for i in range(1, 4):
        load_kb(i, i).start()

    def y_copy(j, c):
        done = ryp_sem.at[(c >= 3) + (c >= 4)] if j == 2 else ry_sem.at[c]
        return remote(YV.at[OWN, :, cols_of(c)], YV.at[1 + j, :, cols_of(c)], sy_sem, done, (tx, ty, pt)[j])

    def middle(c):
        with jax.named_scope("wait_part"):
            three = RB.at[:, :, cols_of(c)]
            remote(three, three, s1_sem, r1_sem.at[c], pt).wait_recv()
        y = YT[OWN, :, cols_of(c)] + jnp.transpose(YR[OWN, sums_of(c), :])
        y = y + RB[0, :, cols_of(c)] + RB[1, :, cols_of(c)] + RB[2, :, cols_of(c)]
        YV[OWN, :, cols_of(c)] = y.astype(BF16)
        YT[OWN, :, cols_of(c)] = jnp.zeros((32, CHUNK), F32)
        YR[OWN, sums_of(c), :] = jnp.zeros((CHUNK, 32), F32)
        for j in range(3):
            y_copy(j, c).start()

    last = last_tiles()
    late = [remote_tile(jnp.int32(23), j) for j in range(6)]

    def rows_in(u, d):
        if d is None:
            return KL, (slice(u * STRIP, (u + 1) * STRIP), slice(None))
        return (kr0, kr1)[u % 6 // UNITS], (d, slice(u % UNITS * STRIP, (u % UNITS + 1) * STRIP), slice(None))

    def grams(tiles, first, d):
        gs = [gram(t) for t in tiles]

        def put():
            for u, (t, g) in enumerate(zip(tiles, gs), first):
                ref, at = rows_in(u, d)
                ref[at] = kern(t, g)

        return put

    def applies(tiles, first, d):
        for u, t in enumerate(tiles, first):
            ref, at = rows_in(u, d)
            apply(t, ref[at], VT)

    kl_out = pltpu.make_async_copy(KL, k_hbm.at[pl.ds(REMOTE_PLACE[23] * STEP_ROWS, STEP_ROWS)], loc_sem.at[0])
    seq, before, due = state[0], state[1], unflat(state[2:])
    d = begin(seq, before, before)
    put = grams(late[0:2], 0, None)
    applies(due, UNITS, 1 - d)
    put()
    put = grams(late[2:4], 2, None)
    applies(late[0:2], 0, None)
    put()
    applies(late[2:4], 2, None)
    finish_range(0, N_CHUNK, SB, RB, s1_sem, r1_sem, (2,))
    with jax.named_scope("wait_last"):
        wait_x(7, True)
    with jax.named_scope("last"):
        for c in range(N_CHUNK):
            if c == 3:
                d = begin(seq + 1, jnp.int32(CROSS_PLACE + 10), before)
            put = grams(last[2 * c : 2 * c + 2], 2 * c, d)
            if c > 1:
                applies(last[2 * c - 2 : 2 * c], 2 * c - 2, 1 - d if c == 3 else d)
            put()
            if c == 0:
                applies(last[0:2], 0, d)
            if c != 1:
                finish_range(max(c - 1, 0), max(c, 1), SB, RB, s1_sem, r1_sem)
        put = grams(late[4:6], 4, None)
        applies(last[10:12], 10, d)
        put()
        kl_out.start()
        load_x(4, 0).start()
        middle(0)
        applies(late[4:6], 4, None)
        finish_range(5, 6, SB, RB, s1_sem, r1_sem)

    for h in range(2):
        k_out(seq, 0, h).wait()
        k_out(seq + 1, CROSS_PLACE + 11, h).start()

    def use(k, slot, tile):
        for h in range(2):
            use_step(k, slot, h, functools.partial(tile, h))

    def use_step(k, slot, h, tile):
        for j in range(6):
            r = (6 * h + j) * STRIP
            apply(tile(j), k[slot, r : r + STRIP, 0:CHUNK], YV)

    def quad(t, tile):
        slot = t & 3
        load_x(0, slot).wait()
        load_kb(0, slot).wait()
        t = jnp.int32(t)

        @pl.when(jnp.logical_and(t >= 1, t <= 7))
        def _():
            load_x(10 + 2 * t, (t - 1) & 3).start()

        @pl.when(jnp.logical_and(t >= 1, t <= 6))
        def _():
            load_kb(11 + 2 * t, (t - 1) & 3).start()

        use(X, slot, lambda h, j: tile(0, h, j))
        use(KB, slot, lambda h, j: tile(1, h, j))

    def wait_y_one(c):
        two = YV.at[1:3, :, cols_of(c)]
        remote(two, two, sy_sem, ry_sem.at[c], tx).wait_recv()

    def wait_y(lo, hi):
        def one(c, _):
            wait_y_one(c)
            return 0

        lax.fori_loop(lo, hi, one, 0)

    def wait_y_par(late):
        part = YV.at[PAR, :, pl.ds((0, 3, 4)[late] * CHUNK, (3, 1, 2)[late] * CHUNK)]
        remote(part, part, sy_sem, ryp_sem.at[late], pt).wait_recv()

    with jax.named_scope("middle"):
        middle(1)
    with jax.named_scope("second_own"):
        first_in.wait()
        for j in range(6):
            apply(own_ints(0, j), KB[0, STEP_ROWS + j * STRIP : STEP_ROWS + (j + 1) * STRIP, :], YV)
        load_kb(5, 0).start()
        middle(2)
        load_kb(0, 1).wait()
        use_step(KB, 1, 0, lambda j: own_ints(1, j))
        wait_y_par(0)
        load_kb(0, 2).wait()
        use_step(KB, 2, 0, lambda j: own_ints(N_OWN, j))
        middle(3)
        use_step(KB, 1, 1, lambda j: own_ints(2, j))
        load_x(6, 1).start()
        load_kb(7, 1).start()
        wait_y_par(1)
        use_step(KB, 2, 1, lambda j: own_ints(N_OWN + 1, j))
        load_x(8, 2).start()
        load_kb(9, 2).start()
        kl_out.wait()
        for h in range(2):
            k_out(seq + 1, 0, h).wait()
        load_x(10, 3).start()
        middle(4)

    def remote_quad(step):
        ps = [step(i) for i in range(4)]
        return lambda d, h, j: remote_tile(ps[2 * d + h], j)

    with jax.named_scope("second_first"):

        wait_y_one(0)
        quad(0, remote_quad(jnp.int32))
        middle(5)
        load_kb(0, 3).wait()
        use(KB, 3, lambda h, j: own_ints(3 + h, j))
        load_kb(11, 3).start()
        wait_y_par(2)
        wait_y_one(1)
        quad(1, remote_quad(lambda i: jnp.int32(4 + i)))
    with jax.named_scope("second_cross"):

        def second_cross(t, _):
            with jax.named_scope("wait_y"):
                wait_y(table((2, 2, 2) + Y_NEED[:-1], t), table((2, 2) + Y_NEED, t))

            def tile(d, h, j):
                cross = cross_tile(4 * (t - 2) + 2 * d + h, j)
                return pick(t < 4, cross, last[6 * h + j]) if d else cross

            quad(t, tile)
            return 0

        lax.fori_loop(2, 5, second_cross, 0)

    for k, done in enumerate(((0,), (4, 5), (3,))):
        for c in done:
            finish_range(c, c + 1, SB2, RB2, s2_sem, r2_sem)
        with jax.named_scope("second_chunk"):
            ps = REMOTE_ORDER[4 * k : 4 * k + 4]
            quad(5 + k, remote_quad(lambda i: jnp.int32(ps[i])))

    def finish_strip(n):
        cols = pl.ds(n * STRIP, STRIP)
        for j in range(2):
            s = homes[j][0]
            SB2[j, :, cols] = YT[s, :, cols] + jnp.transpose(YR[s, pl.ds((n + 1) * STRIP, STRIP), :])
        for j in range(2):
            remote(SB2.at[j, :, cols], RB2.at[j, :, cols], s2_sem, r2_sem, homes[j][1]).start()

    with jax.named_scope("second_chunk"):
        finish_range(2, 3, SB2, RB2, s2_sem, r2_sem)
        load_x(0, 0).wait()
        load_kb(0, 0).wait()
        use(X, 0, lambda h, j: remote_tile(jnp.int32(REMOTE_ORDER[12 + h]), j))
        finish_strip(2)
        use(KB, 0, lambda h, j: remote_tile(jnp.int32(REMOTE_ORDER[14 + h]), j))
        finish_strip(3)

    with jax.named_scope("second_par"):
        quad(9, lambda d, h, j: own_tile(jnp.int32(N_PAIR - 1), j, core) if d and h else own_ints(N_OWN + 2 + 2 * d + h, j))
        remote(YT.at[PAR], RB2.at[2], s2_sem, r2_sem, pt).start()

    with jax.named_scope("sent"):
        p_copy.wait_send()
        for j in range(2):
            remote(x_hbm, X.at[1 + j], sx_sem.at[j], rx_sem.at[0], tx).wait_send()
        remote(NB.at[1:3, :, tail_cols], NB.at[1:3, :, tail_cols], sn_sem.at[0], rx_sem.at[0], tx).wait_send()
        n_copies[2].wait_send()
        for buf, sem in ((VT, sv_sem), (YV, sy_sem)):
            remote(buf.at[1:4], buf.at[1:4], sem, rx_sem.at[0], tx).wait_send()
        remote(SB, RB, s1_sem, rx_sem.at[0], tx).wait_send()

    with jax.named_scope("second_end"):
        load_x(0, 2).wait()
        use(X, 2, lambda h, j: own_ints(5 + h, j))

    with jax.named_scope("final"):
        for c in range(N_CHUNK):
            out_ref[:, cols_of(c)] = YT[OWN, :, cols_of(c)] + jnp.transpose(YR[OWN, sums_of(c), :])
        all_sums = remote(SB2, RB2, s2_sem, r2_sem, pt)
        all_sums.wait_send()
        all_sums.wait_recv()


def solution(mesh):
    def local_program(x_loc, v_loc, length_scale, out_scale):
        dma = pltpu.SemaphoreType.DMA
        hbm = pl.BlockSpec(memory_space=pltpu.HBM)
        vmem = pl.BlockSpec(memory_space=pltpu.VMEM)
        smem = pl.BlockSpec(memory_space=pltpu.SMEM)
        own, parts, _ = pl.pallas_call(
            body,
            out_shape=(
                pltpu.VMEM((32, ROWS), F32),
                pltpu.VMEM((3, 32, ROWS), F32),
                jax.ShapeDtypeStruct((N_PLACE * STEP_ROWS, CHUNK), BF16),
            ),
            in_specs=[hbm, hbm, smem, smem],
            out_specs=(vmem, vmem, hbm),
            scratch_shapes=[
                pltpu.VMEM((4, ROWS, 768), BF16),
                pltpu.VMEM((4, 32, ROWS), BF16),
                pltpu.VMEM((4, 32, ROWS), BF16),
                pltpu.VMEM((3, ROWS, 128), F32),
                pltpu.VMEM((4, 1, ROWS), F32),
                pltpu.VMEM((8, CHUNK), F32),
                pltpu.VMEM((3, STRIP + ROWS, 32), F32),
                pltpu.VMEM((5, 32, ROWS), F32),
                pltpu.VMEM((3, 32, ROWS), F32),
                pltpu.VMEM((3, 32, ROWS), F32),
                pltpu.VMEM((3, 32, ROWS), F32),
                pltpu.VMEM((2, HALF_ROWS, CHUNK), BF16),
                pltpu.VMEM((2, HALF_ROWS, CHUNK), BF16),
                pltpu.VMEM((STEP_ROWS, CHUNK), BF16),
                pltpu.VMEM((4, 2 * STEP_ROWS, CHUNK), BF16),
                dma((2,)), dma((8,)), dma, dma((2,)), dma((2,)), dma((2,)), dma, dma,
                dma((2,)), dma((2, 2)), dma((4,)), dma((4,)),
                dma, dma((N_CHUNK,)), dma, dma((N_CHUNK,)), dma((3,)), dma, dma,
            ],
            compiler_params=pltpu.CompilerParams(collective_id=0, has_side_effects=True, vmem_limit_bytes=58 * 2**20),
            name="products",
        )(x_loc, v_loc.T, length_scale, out_scale)
        return (own + parts[0] + parts[1] + parts[2]).T

    row_spec = P(("task", "row"), None)
    return jax.shard_map(local_program, mesh=mesh, in_specs=(row_spec, row_spec, P("task"), P("task")), out_specs=row_spec, check_vma=False)
```
